32 devices in a mesh: dp: 4 (over y, x), fsdp: 8 (over z, core).
Axes of the slice: x: 2, y: 2, z: 4, core: 2. Of those that a mesh axis runs over, the one named last changes fastest.
Arguments:
- inputs: bfloat16 [65536, 512], P(('dp', 'fsdp')), may hold values from -6 to 6
- cotangent: bfloat16 [65536, 512], P(('dp', 'fsdp')), may hold values from -6 to 6
- feature_omega: bfloat16 [8, 64, 256], replicated, may hold values from -6 to 6
- seg_start: int32 [64], P(('dp', 'fsdp')), may hold values from 0 to 1, as said below
- seg_len: int32 [64], P(('dp', 'fsdp')), may hold values from 0 to 1024, as said below
- step_count: int32 [], replicated, may hold values from 1 to 20
- w_qkv: float32 [512, 1536], P(('dp', 'fsdp')), may hold values from -0.25 to 0.25
- w_out: float32 [512, 512], P(('dp', 'fsdp')), may hold values from -1 to 1
- w_up: float32 [512, 2048], P(('dp', 'fsdp')), may hold values from -0.26516504 to 0.26516504
- w_down: float32 [2048, 512], P(('dp', 'fsdp')), may hold values from -0.125 to 0.125
- gains: float32 [2, 512], P(None, ('dp', 'fsdp')), may hold values from 0.3 to 3.1
- m_qkv: float32 [512, 1536], P(('dp', 'fsdp')), may hold values from -0.0009765625 to 0.0009765625
- m_out: float32 [512, 512], P(('dp', 'fsdp')), may hold values from -0.0009765625 to 0.0009765625
- m_up: float32 [512, 2048], P(('dp', 'fsdp')), may hold values from -0.0009765625 to 0.0009765625
- m_down: float32 [2048, 512], P(('dp', 'fsdp')), may hold values from -0.0009765625 to 0.0009765625
- m_gains: float32 [2, 512], P(None, ('dp', 'fsdp')), may hold values from -0.0029296875 to 0.0029296875
- v_qkv: float32 [512, 1536], P(('dp', 'fsdp')), may hold values from 1.58894e-08 to 1.271152e-07
- v_out: float32 [512, 512], P(('dp', 'fsdp')), may hold values from 1.58894e-09 to 1.271152e-08
- v_up: float32 [512, 2048], P(('dp', 'fsdp')), may hold values from 2.224516e-09 to 1.7796127e-08
- v_down: float32 [2048, 512], P(('dp', 'fsdp')), may hold values from 3.17788e-09 to 2.542304e-08
- v_gains: float32 [2, 512], P(None, ('dp', 'fsdp')), may hold values from 1.430046e-07 to 1.1440368e-06
Outputs:
- out_rows: bfloat16 [65536, 512], P(('dp', 'fsdp'))
- grad_inputs: float32 [65536, 512], P(('dp', 'fsdp'))
- grad_norm: float32 [], replicated
- grad_qkv: float32 [512, 1536], P(('dp', 'fsdp'))
- var_qkv: float32 [512, 1536], P(('dp', 'fsdp'))
- new_qkv: float32 [512, 1536], P(('dp', 'fsdp'))
- grad_out: float32 [512, 512], P(('dp', 'fsdp'))
- var_out: float32 [512, 512], P(('dp', 'fsdp'))
- new_out: float32 [512, 512], P(('dp', 'fsdp'))
- grad_up: float32 [512, 2048], P(('dp', 'fsdp'))
- var_up: float32 [512, 2048], P(('dp', 'fsdp'))
- new_up: float32 [512, 2048], P(('dp', 'fsdp'))
- grad_down: float32 [2048, 512], P(('dp', 'fsdp'))
- var_down: float32 [2048, 512], P(('dp', 'fsdp'))
- new_down: float32 [2048, 512], P(('dp', 'fsdp'))
- grad_gains: float32 [2, 512], P(None, ('dp', 'fsdp'))
- var_gains: float32 [2, 512], P(None, ('dp', 'fsdp'))
- new_gains: float32 [2, 512], P(None, ('dp', 'fsdp'))
The draws below stay inside these ranges and needn't reach their ends.
Inputs may be any that keep to these rules, and one draw needn't show every extreme that they name: Each device holds 2 consecutive segments; its first segment has seg_start 1, so no protein crosses devices; a protein is 1 to 2 segments. Residues fill a segment from its start; all segments of a protein but its last are full, and a protein of one segment is full; after a device's last protein come empty segments (seg_len 0, seg_start 0); a segment with seg_start 1 is never empty; in every draw some device is full.
All inputs are finite; a program needn't handle non-finite values.
Results may differ from the reference program's by a relative error of at most 0.025.
The reference program's roundings to bfloat16 on the way count: a program that leaves them out, or rounds other values in their place, can miss the bound.
Values may be sent and summed in bfloat16 or wider, within the bound.
A program may use at most 256 MiB of HBM per device.

```python
import math
import jax
import jax.numpy as jnp
from jax import lax

D = 512
HEADS = 8
HD = 64
FEAT = 256
FF = 2048
SEG = 1024
TILE = 256
SEGS_DEV = 2
TOK_DEV = 2048
NSEGS = 64
TOKENS = 65536


def protein_layout(key):
    keys = jax.random.split(key, 4)
    devices_all = NSEGS // SEGS_DEV
    used = jax.random.randint(keys[0], (devices_all,), 1, SEGS_DEV + 1)
    full_device = jax.random.randint(keys[1], (), 0, devices_all)
    device_index = jnp.arange(devices_all, dtype=jnp.int32)
    is_full = device_index == full_device
    used = jnp.where(is_full, SEGS_DEV, used)
    flips = jax.random.randint(keys[2], (devices_all, SEGS_DEV), 0, 2)
    segment = jnp.arange(SEGS_DEV, dtype=jnp.int32)[None, :]
    inside = segment < used[:, None]
    starts = jnp.where(segment == 0, 1, flips)
    starts = jnp.where(inside, starts, 0)
    next_start = jnp.concatenate([starts[:, 1:], jnp.ones((devices_all, 1), jnp.int32)], axis=1)
    last_used = segment == used[:, None] - 1
    ends = (next_start == 1) | last_used
    single = ends & (starts == 1)
    tail = jax.random.randint(keys[3], (devices_all, SEGS_DEV), 1, SEG + 1)
    partial_value = ends & jnp.logical_not(single) & jnp.logical_not(is_full)[:, None]
    lengths = jnp.where(partial_value, tail, SEG)
    lengths = jnp.where(inside, lengths, 0)
    return (starts.reshape(-1).astype(jnp.int32), lengths.reshape(-1).astype(jnp.int32))


def draw_seg_start(key, part):
    return protein_layout(key)[0]


def draw_seg_len(key, part):
    return protein_layout(key)[1]


def draw_gains(key, part):
    rough_key = jax.random.fold_in(key, 17)
    place = jnp.arange(D, dtype=jnp.float32) / float(max(D - 1, 1))
    lowest = 0.6
    ratio = 3.0
    base = lowest * jnp.exp(place * jnp.log(ratio))
    rough = jnp.exp(jax.random.uniform(rough_key, (2, D), jnp.float32, jnp.log(0.8), jnp.log(1.25)))
    return (base[None, :] * rough).astype(jnp.float32)


def draw_w_up(key, part):
    base_key = jax.random.fold_in(key, 23)
    column_key = jax.random.fold_in(key, 29)
    base = jax.random.truncated_normal(base_key, -4.0, 4.0, (D, FF), jnp.float32)
    column = 0.5 * jax.random.truncated_normal(column_key, -4.0, 4.0, (1, FF), jnp.float32)
    return ((base + column) * float(D) ** (-0.5)).astype(jnp.float32)


def steps_of(key, shape, cuts, smallest, high):
    level = 1.0
    for axis_at, blocks in cuts:
        heights = jax.random.uniform(jax.random.fold_in(jax.random.fold_in(key, 6), axis_at), (blocks,), jnp.float32, smallest / len(cuts), high / len(cuts))
        level = level * jnp.repeat(jnp.exp(heights), shape[axis_at] // blocks).reshape((-1,) + (1,) * (len(shape) - 1 - axis_at))
    return level


def noise(stream_key, dims, deviation, most, cuts=(), kind=jnp.bfloat16):
    factor_of = steps_of(stream_key, dims, cuts, -0.22, 0.18) if cuts else 1.0
    entries = jax.random.normal(stream_key, dims, jnp.float32) * deviation * factor_of
    return jnp.minimum(jnp.maximum(entries, -most), most).astype(kind)


def setup_inputs(seed: int = 0) -> dict:
    key_list = jax.random.split(jax.random.key(seed), 22)
    return {
        "inputs": noise(key_list[0], (TOKENS, D), 1.0, 6.0, ((0, 32),)),
        "cotangent": noise(key_list[1], (TOKENS, D), 1.0, 6.0, ((0, 32),)),
        "feature_omega": noise(key_list[2], (HEADS, HD, FEAT), 1.0, 6.0),
        "seg_start": draw_seg_start(jax.random.fold_in(key_list[21], 71), 0),
        "seg_len": draw_seg_len(jax.random.fold_in(key_list[21], 71), 0),
        "step_count": jax.random.randint(key_list[5], (), 1, 21).astype(jnp.int32),
        "w_qkv": noise(key_list[6], (D, 3 * D), D ** -0.5, 0.25, ((0, 32),), jnp.float32),
        "w_out": noise(key_list[7], (D, D), (D // 16) ** -0.5, 1.0, ((0, 32),), jnp.float32),
        "w_up": draw_w_up(jax.random.fold_in(key_list[21], 71), 0),
        "w_down": noise(key_list[9], (FF, D), FF ** -0.5, 0.125, ((0, 32),), jnp.float32),
        "gains": draw_gains(jax.random.fold_in(key_list[21], 71), 0),
        "m_qkv": noise(key_list[11], (D, 3 * D), (0.11 / (4 * D * D + 2 * D * FF + 2 * D) ** 0.5), 0.0009765625, ((0, 32),), jnp.float32),
        "m_out": noise(key_list[12], (D, D), (0.11 / (4 * D * D + 2 * D * FF + 2 * D) ** 0.5), 0.0009765625, ((0, 32),), jnp.float32),
        "m_up": noise(key_list[13], (D, FF), (0.11 / (4 * D * D + 2 * D * FF + 2 * D) ** 0.5), 0.0009765625, ((0, 32),), jnp.float32),
        "m_down": noise(key_list[14], (FF, D), (0.11 / (4 * D * D + 2 * D * FF + 2 * D) ** 0.5), 0.0009765625, ((0, 32),), jnp.float32),
        "m_gains": noise(key_list[15], (2, D), (0.33 / (4 * D * D + 2 * D * FF + 2 * D) ** 0.5), 0.0029296875, ((1, 32),), jnp.float32),
        "v_qkv": jnp.clip(jnp.exp(math.log(1.2711520014363487e-07) - 2.0794415 * jax.random.uniform(key_list[16], (D, 3 * D), jnp.float32) ** steps_of(key_list[16], (D, 3 * D), ((0, 32),), -0.2, 0.2)), 1.5889400017954358e-08, 1.2711520014363487e-07),
        "v_out": jnp.clip(jnp.exp(math.log(1.2711519836727803e-08) - 2.0794415 * jax.random.uniform(key_list[17], (D, D), jnp.float32) ** steps_of(key_list[17], (D, D), ((0, 32),), -0.2, 0.2)), 1.5889399795909753e-09, 1.2711519836727803e-08),
        "v_up": jnp.clip(jnp.exp(math.log(1.7796127238511872e-08) - 2.0794415 * jax.random.uniform(key_list[18], (D, FF), jnp.float32) ** steps_of(key_list[18], (D, FF), ((0, 32),), -0.2, 0.2)), 2.224515904813984e-09, 1.7796127238511872e-08),
        "v_down": jnp.clip(jnp.exp(math.log(2.5423039673455605e-08) - 2.0794415 * jax.random.uniform(key_list[19], (FF, D), jnp.float32) ** steps_of(key_list[19], (FF, D), ((0, 32),), -0.2, 0.2)), 3.1778799591819507e-09, 2.5423039673455605e-08),
        "v_gains": jnp.clip(jnp.exp(math.log(1.144036787081859e-06) - 2.0794415 * jax.random.uniform(key_list[20], (2, D), jnp.float32) ** steps_of(key_list[20], (2, D), ((1, 32),), -0.2, 0.2)), 1.4300459838523238e-07, 1.144036787081859e-06),
    }


@jax.custom_vjp
def low(v):
    return lax.optimization_barrier(v.astype(jnp.bfloat16)).astype(jnp.float32)

@jax.custom_vjp
def low_back(v):
    return v

def low_keep(v):
    return (low(v), None)

def low_pass(kept, grad):
    return (grad,)

def back_keep(v):
    return (v, None)

def back_low(kept, grad):
    return (low(grad),)
low.defvjp(low_keep, low_pass)
low_back.defvjp(back_keep, back_low)
norm_eps = 1e-05
clip_level = 1.0
rate_matrix = 0.03
rate_gain = 0.4
beta_first = 0.9
beta_second = 0.95
adam_eps = 1e-08
decay_weight = 0.1
highest = lax.Precision.HIGHEST

def product(left, right):
    return jnp.dot(left, right, precision=highest, preferred_element_type=jnp.float32)

def layer_norm(input_rows, gain_row):
    centred = input_rows - lax.optimization_barrier(jnp.mean(input_rows, axis=-1, keepdims=True))
    spread = lax.optimization_barrier(jnp.mean(centred * centred, axis=-1, keepdims=True))
    return centred * lax.rsqrt(spread + norm_eps) * gain_row

def feature_map(projected, values):
    feat_scale = HD ** (-0.25)
    square = lax.optimization_barrier(jnp.sum(values * values, axis=-1, keepdims=True)) * (0.5 * feat_scale * feat_scale)
    return jnp.exp(projected * feat_scale - square)

def token_mask(lengths):
    position = jnp.arange(SEG, dtype=jnp.int32)[None, :]
    return (position < lengths[:, None]).astype(jnp.float32).reshape(lengths.shape[0] * SEG)

def tile_links(starts):
    protein_id = jnp.cumsum(starts.astype(jnp.int32)).astype(jnp.int32)
    per_tile = jnp.repeat(protein_id, SEG // TILE)
    tile_index = jnp.arange(per_tile.shape[0], dtype=jnp.int32)
    same_protein = per_tile[:, None] == per_tile[None, :]
    earlier = tile_index[None, :] < tile_index[:, None]
    return (same_protein & earlier).astype(jnp.float32)

def block_forward(input_rows, w_qkv, w_out, w_up, w_down, gains, omega_full, valid_mask, links):
    tokens = input_rows.shape[0]
    tiles = tokens // TILE
    qkv_w = low(w_qkv)
    out_w = low(w_out)
    up_w = low(w_up)
    down_w = low(w_down)
    gain_w = low(gains)
    normed = low(layer_norm(input_rows, gain_w[0]))
    qkv_all = low(low_back(product(normed, qkv_w))).reshape(tokens, 3, HEADS, HD)
    queries = qkv_all[:, 0]
    key_rows = qkv_all[:, 1]
    value_rows = qkv_all[:, 2]
    proj_query = low_back(jnp.einsum('thd,hdm->thm', queries, omega_full, precision=highest))
    proj_key = low_back(jnp.einsum('thd,hdm->thm', key_rows, omega_full, precision=highest))
    query_feat = low(feature_map(proj_query, queries)).reshape(tiles, TILE, HEADS, FEAT)
    key_feat = (low(feature_map(proj_key, key_rows)) * valid_mask[:, None, None]).reshape(tiles, TILE, HEADS, FEAT)
    value_tiles = value_rows.reshape(tiles, TILE, HEADS, HD)
    causal = (jnp.arange(TILE)[:, None] >= jnp.arange(TILE)[None, :]).astype(jnp.float32)
    scores = jnp.einsum('cihm,cjhm->chij', query_feat, key_feat, precision=highest)
    weights = low(low_back(scores * causal))
    tile_kv = low_back(jnp.einsum('cjhm,cjhd->chmd', key_feat, value_tiles, precision=highest))
    key_sums = lax.optimization_barrier(jnp.sum(key_feat, axis=1))
    prefix_state = low(jnp.einsum('cd,dhme->chme', links, tile_kv, precision=highest))
    totals = low(jnp.einsum('cd,dhm->chm', links, key_sums, precision=highest))
    numerator = low_back(jnp.einsum('chij,cjhd->cihd', weights, value_tiles, precision=highest) + jnp.einsum('cihm,chmd->cihd', query_feat, prefix_state, precision=highest))
    denominator = low_back(jnp.transpose(lax.optimization_barrier(jnp.sum(weights, axis=-1)), (0, 2, 1)) + jnp.einsum('cihm,chm->cih', query_feat, totals, precision=highest))
    attended = low((numerator / denominator[..., None]).reshape(tokens, HEADS * HD))
    middle = input_rows + low_back(product(attended, out_w))
    normed_two = low(layer_norm(middle, gain_w[1]))
    hidden = low_back(product(normed_two, up_w))
    active = low(jax.nn.gelu(hidden, approximate=False))
    return middle + product(active, down_w)

def reference(inputs, cotangent, feature_omega, seg_start, seg_len, step_count, w_qkv, w_out, w_up, w_down, gains, m_qkv, m_out, m_up, m_down, m_gains, v_qkv, v_out, v_up, v_down, v_gains):
    params = (w_qkv, w_out, w_up, w_down, gains)
    omega_full = feature_omega.astype(jnp.float32)
    devices_all = NSEGS // SEGS_DEV
    rows_all = inputs.astype(jnp.float32).reshape(devices_all, TOK_DEV, D)
    cot_all = cotangent.astype(jnp.float32).reshape(devices_all, TOK_DEV, D)
    start_all = seg_start.reshape(devices_all, SEGS_DEV)
    length_all = seg_len.reshape(devices_all, SEGS_DEV)

    def one_device(summed, pieces):
        device_rows, device_cot, device_starts, device_lengths = pieces
        valid_mask = token_mask(device_lengths)
        links = tile_links(device_starts)

        def forward(rows_in, *weights_in):
            return block_forward(rows_in, *weights_in, omega_full, valid_mask, links)
        result, pullback = jax.vjp(forward, device_rows, *params)
        gradients = pullback(device_cot * valid_mask[:, None])
        summed = tuple((total + grad_piece for total, grad_piece in zip(summed, gradients[1:])))
        return (summed, (result.astype(jnp.bfloat16), gradients[0]))
    zero_start = tuple((jnp.zeros(weight.shape, jnp.float32) for weight in params))
    summed, (out_all, grad_all) = lax.scan(one_device, zero_start, (rows_all, cot_all, start_all, length_all))
    out_rows = out_all.reshape(TOKENS, D)
    grad_inputs = grad_all.reshape(TOKENS, D)
    square_sum = sum((jnp.sum(piece * piece) for piece in summed))
    grad_norm = jnp.sqrt(square_sum)
    factor = jnp.minimum(1.0, clip_level / grad_norm)
    count = step_count.astype(jnp.float32)
    first_fix = 1.0 - jnp.power(beta_first, count)
    second_fix = 1.0 - jnp.power(beta_second, count)

    def update(weight, first, second, gradient, rate):
        clipped = gradient * factor
        first_new = beta_first * first + (1.0 - beta_first) * clipped
        second_new = beta_second * second + (1.0 - beta_second) * clipped * clipped
        direction = first_new / first_fix / (jnp.sqrt(second_new / second_fix) + adam_eps)
        return (clipped, second_new, weight - rate * (direction + decay_weight * weight))
    grad_qkv, var_qkv, new_qkv = update(w_qkv, m_qkv, v_qkv, summed[0], rate_matrix)
    grad_out, var_out, new_out = update(w_out, m_out, v_out, summed[1], rate_matrix)
    grad_up, var_up, new_up = update(w_up, m_up, v_up, summed[2], rate_matrix)
    grad_down, var_down, new_down = update(w_down, m_down, v_down, summed[3], rate_matrix)
    grad_gains, var_gains, new_gains = update(gains, m_gains, v_gains, summed[4], rate_gain)
    return (out_rows, grad_inputs, grad_norm, grad_qkv, var_qkv, new_qkv, grad_out, var_out, new_out, grad_up, var_up, new_up, grad_down, var_down, new_down, grad_gains, var_gains, new_gains)
```

```python
import functools
import math

import jax
import jax.numpy as jnp
from jax import lax
from jax.experimental import pallas as pl
from jax.experimental.pallas import tpu as pltpu
from jax.sharding import PartitionSpec as P

D = 512
HEADS = 8
HD = 64
FEAT = 256
FF = 2048
SEG = 1024
TILE = 256
PAIRS = HEADS // 2
WIDE = 3 * D

norm_eps = 1e-05
clip_level = 1.0
rate_matrix = 0.03
rate_gain = 0.4
beta_first = 0.9
beta_second = 0.95
adam_eps = 1e-08
decay_weight = 0.1

feat_scale = HD ** (-0.25)
log2_e = math.log2(math.e)
f32 = jnp.float32
bf16 = jnp.bfloat16
MESH = pl.DeviceIdType.MESH


def dot_nn(a, b):
    return lax.dot_general(a, b, (((1,), (0,)), ((), ())), preferred_element_type=f32)


def dot_nt(a, b):
    return lax.dot_general(a, b, (((1,), (1,)), ((), ())), preferred_element_type=f32)


def dot_tn(a, b):
    return lax.dot_general(a, b, (((0,), (0,)), ((), ())), preferred_element_type=f32)


def normalise(rows):
    centred = rows - jnp.mean(rows, axis=-1, keepdims=True)
    spread = jnp.mean(centred * centred, axis=-1, keepdims=True)
    inverse = lax.rsqrt(spread + norm_eps)
    return centred * inverse, inverse


def normalise_back(grad, gain, unit, inverse):
    scaled = grad * gain
    first = jnp.mean(scaled, axis=-1, keepdims=True)
    second = jnp.mean(scaled * unit, axis=-1, keepdims=True)
    return inverse * (scaled - first - unit * second)


def lane_masks(rows):
    lane = lax.broadcasted_iota(jnp.int32, (rows, 2 * HD), 1)
    return lane, lane < HD


def with_ones(value_pair, low):
    wide = value_pair.astype(f32)
    return (
        jnp.where(low, wide, 1.0).astype(bf16),
        jnp.where(low, 1.0, wide).astype(bf16),
    )


def valid_rows(tile, lens_ref):
    per_seg = SEG // TILE
    place = lax.broadcasted_iota(jnp.int32, (TILE, 1), 0) + (tile % per_seg) * TILE
    return (place < lens_ref[tile // per_seg]).astype(f32)


AXES = ("dp", "fsdp")
EXTRA = 128
FULL = WIDE + EXTRA
ROWS = {"qkv": 16, "out": 16, "up": 16, "down": 64}
COLS = {"qkv": FULL, "out": D, "up": FF, "down": D}
LATE = ("out", "up", "down")


def place():
    dp, inner = lax.axis_index("dp"), lax.axis_index("fsdp")
    z, core = inner // 2, inner % 2
    y, x = dp // 2, dp % 2
    across = y * 2 + (1 - x)
    along = (1 - y) * 2 + x
    return {
        "dp": dp, "z": z, "core": core,
        "first": core * along + (1 - core) * across,
        "second": core * across + (1 - core) * along,
        "diag": (1 - y) * 2 + (1 - x),
    }


def greet(devices):
    barrier = pltpu.get_barrier_semaphore()
    for device in devices:
        pl.semaphore_signal(barrier, inc=1, device_id=device, device_id_type=MESH)
    pl.semaphore_wait(barrier, len(devices))


def near_devices(at):
    devices = [{"fsdp": (at["z"] + i) % 4 * 2 + at["core"]} for i in range(1, 4)]
    devices += [{"fsdp": at["z"] * 2 + 1 - at["core"]}]
    devices += [{"dp": at["first"]}, {"dp": at["second"]}]
    return devices


def gather_copy(at, own, full, send, recv, k):
    dp, z, core = at["dp"], at["z"], at["core"]
    sibling = {"fsdp": z * 2 + 1 - core}
    if k < 3:
        src, dst, device = own, full.at[dp, z, core], {"fsdp": (z + 1 + k) % 4 * 2 + core}
    else:
        which = {3: "dp", 4: "dp", 5: "dp", 6: "first", 7: "first", 8: "second", 9: "diag"}[k]
        src = dst = full.at[at[which], :, core]
        device = {4: {"dp": at["first"]}, 5: {"dp": at["second"]}, 6: {"dp": at["second"]}}.get(k, sibling)
    return pltpu.make_async_remote_copy(
        src_ref=src, dst_ref=dst, send_sem=send.at[k], recv_sem=recv.at[k],
        device_id=device, device_id_type=MESH,
    )


def attention_forward_tile(
    tile, starts_ref, lens_ref, x_ref, weight, gain_row, omega_ref,
    qkv_ref, fq_ref, fk_ref, o_ref, rden_ref, prefix_ref, state_ref,
):
    per_seg = SEG // TILE

    @pl.when(tile % per_seg == 0)
    def _():
        begins = jnp.logical_or(tile == 0, starts_ref[tile // per_seg] != 0)
        state_ref[...] = jnp.where(begins, 0.0, state_ref[...])

    unit, _ = normalise(x_ref[...].astype(f32))
    normed = (unit * gain_row).astype(bf16)
    qkv_ref[...] = dot_nn(normed, weight()).astype(bf16)
    valid = valid_rows(tile, lens_ref)
    _, low = lane_masks(TILE)
    causal = lax.broadcasted_iota(jnp.int32, (TILE, TILE), 0) >= lax.broadcasted_iota(
        jnp.int32, (TILE, TILE), 1
    )
    for pair in range(PAIRS):
        lanes = slice(pair * 2 * HD, (pair + 1) * 2 * HD)
        feats = []
        for part in range(2):
            rows = qkv_ref[:, part * D + pair * 2 * HD : part * D + (pair + 1) * 2 * HD]
            wide = rows.astype(f32)
            square = wide * wide
            proj = dot_nn(rows, omega_ref[pair])
            for odd in range(2):
                total = jnp.sum(
                    jnp.where(low, 0.0, square) if odd else jnp.where(low, square, 0.0),
                    axis=-1, keepdims=True,
                )
                value = jnp.exp2(
                    proj[:, odd * FEAT : (odd + 1) * FEAT] * (feat_scale * log2_e)
                    - total * (0.5 * feat_scale * feat_scale * log2_e)
                )
                if part:
                    value = value * valid
                feats.append(value.astype(bf16))
        value_pair = qkv_ref[:, 2 * D + pair * 2 * HD : 2 * D + (pair + 1) * 2 * HD]
        ones = with_ones(value_pair, low)
        mixed = []
        for odd in range(2):
            head = 2 * pair + odd
            query_feat, key_feat = feats[odd], feats[2 + odd]
            fq_ref[:, head * FEAT : (head + 1) * FEAT] = query_feat
            fk_ref[:, head * FEAT : (head + 1) * FEAT] = key_feat
            weights = jnp.where(causal, dot_nt(query_feat, key_feat), 0.0).astype(bf16)
            before = state_ref[head]
            before_low = before.astype(bf16)
            prefix_ref[0, head] = before_low
            mixed.append(dot_nn(weights, ones[odd]) + dot_nt(query_feat, before_low))
            state_ref[head] = before + dot_tn(ones[odd], key_feat)
        top = jnp.where(low, mixed[0], mixed[1])
        bottom = pltpu.roll(jnp.where(low, mixed[1], mixed[0]), HD, 1)
        o_ref[:, lanes] = (top / bottom).astype(bf16)
        rden_ref[:, lanes] = 1.0 / bottom


def spread_projection(omega_ref, wide_ref):
    wide_ref[...] = jnp.zeros_like(wide_ref)
    for pair in range(PAIRS):
        wide_ref[pair, :HD, :FEAT] = omega_ref[2 * pair]
        wide_ref[pair, HD:, FEAT:] = omega_ref[2 * pair + 1]


def ones_projection(omega_ref, wide_ref):
    wide_ref[...] = jnp.ones_like(wide_ref)
    for head in range(HEADS):
        odd = head % 2
        wide_ref[head, odd * HD : (odd + 1) * HD, :] = omega_ref[head]


def attention_forward_local_kernel(
    starts_ref, lens_ref, x_ref, w_ref, gain_ref, omega_ref,
    qkv_ref, fq_ref, fk_ref, o_ref, rden_ref, prefix_ref, state_ref, wide_ref,
):
    tile = pl.program_id(0)

    @pl.when(tile == 0)
    def _():
        spread_projection(omega_ref, wide_ref)

    attention_forward_tile(
        tile, starts_ref, lens_ref, x_ref, lambda: w_ref[...], gain_ref[0:1, :], wide_ref,
        qkv_ref, fq_ref, fk_ref, o_ref, rden_ref, prefix_ref, state_ref,
    )


def attention_forward_kernel(
    starts_ref, lens_ref, x_ref, omega_ref, wq_ref, wo_ref, wu_ref, wd_ref, gains_ref,
    qkv_ref, fq_ref, fk_ref, o_ref, rden_ref, prefix_ref, gain_ref, fullq_ref, fullo_ref, fullu_ref, fulld_ref,
    state_ref, wide_ref, held_ref, so_ref, su_ref, sd_ref, pad_ref, send, recv, local,
):
    tile = pl.program_id(0)
    last = pl.num_programs(0) - 1
    at = place()
    dp, z, core = at["dp"], at["z"], at["core"]
    own = [held_ref.at[dp, z, core], so_ref, su_ref, sd_ref]
    full = [held_ref, fullo_ref, fullu_ref, fulld_ref]

    def copy(w, k):
        return gather_copy(at, own[w], full[w], send.at[w], recv.at[w], k)

    def keep(w):
        if w == 0:
            return pltpu.make_async_copy(held_ref, fullq_ref, local.at[0])
        return pltpu.make_async_copy(own[w], full[w].at[dp, z, core], local.at[w])

    @pl.when(tile == 0)
    def _():
        pad_ref[...] = jnp.zeros_like(pad_ref)
        pad_ref[0:2, 0:16] = gains_ref[...]
        flat = pad_ref[...]
        shift = inner_lane(at)
        turned = flat
        for i in range(1, 8):
            turned = jnp.where(shift == i, pltpu.roll(flat, 16 * i, 1), turned)
        row = lax.broadcasted_iota(jnp.int32, (16, 128), 0)
        band = flat_index(at) // 8
        placed = jnp.where(row == band, turned[0:1, :], 0.0) + jnp.where(
            row == band + 4, turned[1:2, :], 0.0
        )
        held_ref[dp, z, core, :, :WIDE] = wq_ref[...].astype(bf16)
        held_ref[dp, z, core, :, WIDE:] = placed.astype(bf16)
        greet(near_devices(at))
        for k in range(3):
            copy(0, k).start()
        so_ref[...] = wo_ref[...].astype(bf16)
        su_ref[...] = wu_ref[...].astype(bf16)
        sd_ref[...] = wd_ref[...].astype(bf16)
        spread_projection(omega_ref, wide_ref)
        for w in range(1, 4):
            keep(w).start()
        for k in range(3):
            copy(0, k).wait_recv()
        for k in (4, 5, 3):
            copy(0, k).start()
        for w in range(1, 4):
            for k in range(3):
                copy(w, k).start()
        copy(0, 4).wait_recv()
        copy(0, 6).start()
        copy(0, 7).start()
        copy(0, 5).wait_recv()
        copy(0, 8).start()
        copy(0, 6).wait_recv()
        copy(0, 9).start()
        for k in (3, 7, 8, 9):
            copy(0, k).wait_recv()
        keep(0).start()
        packed = held_ref[..., WIDE:].astype(f32)
        total = jnp.sum(packed.reshape(32, 16, 128), axis=0)
        gain_ref[...] = jnp.zeros_like(gain_ref)
        for i in range(2):
            for j in range(4):
                gain_ref[i : i + 1, 128 * j : 128 * (j + 1)] = total[4 * i + j : 4 * i + j + 1, :]

    for w in range(1, 4):

        @pl.when(tile == 1)
        def _(w=w):
            keep(w).wait()
            for k in range(3):
                copy(w, k).wait_recv()
            for k in (4, 5, 3):
                copy(w, k).start()

        @pl.when(tile == 2 + (w > 1))
        def _(w=w):
            copy(w, 4).wait_recv()
            copy(w, 6).start()
            copy(w, 7).start()
            copy(w, 5).wait_recv()
            copy(w, 8).start()

        @pl.when(tile == 5)
        def _(w=w):
            copy(w, 6).wait_recv()
            copy(w, 9).start()

    attention_forward_tile(
        tile, starts_ref, lens_ref, x_ref, lambda: held_ref[..., :WIDE].reshape(D, WIDE), gain_ref[0:1, :], wide_ref,
        qkv_ref, fq_ref, fk_ref, o_ref, rden_ref, prefix_ref, state_ref,
    )

    @pl.when(tile == last)
    def _():
        keep(0).wait()
        for w in range(4):
            if w:
                for k in (3, 7, 8, 9):
                    copy(w, k).wait_recv()
            for k in range(10):
                copy(w, k).wait_send()


def inner_lane(at):
    return flat_index(at) % 8


def flat_index(at):
    return at["dp"] * 8 + at["z"] * 2 + at["core"]


def attention_backward_tile(
    tile, tiles, starts_ref, x_ref, qkv_ref, fq_ref, fk_ref, o_ref, rden_ref, do_ref, dmid_ref,
    prefix_ref, weight, gain, omega_ref, gin_ref, acc_ref, suffix_ref, dqkv_ref, dgain_ref,
):
    per_seg = SEG // TILE

    @pl.when(tile == tiles - 1)
    def _():
        acc_ref[...] = jnp.zeros_like(acc_ref)
        dgain_ref[...] = jnp.zeros_like(dgain_ref)

    @pl.when(tile % per_seg == per_seg - 1)
    def _():
        after = jnp.minimum(tile // per_seg + 1, tiles // per_seg - 1)
        ends = jnp.logical_or(tile == tiles - 1, starts_ref[after] != 0)
        suffix_ref[...] = jnp.where(ends, 0.0, suffix_ref[...])

    lane, low = lane_masks(TILE)
    row_at = lax.broadcasted_iota(jnp.int32, (TILE, TILE), 0)
    col_at = lax.broadcasted_iota(jnp.int32, (TILE, TILE), 1)
    causal = row_at >= col_at
    anti = row_at <= col_at
    state_row = lax.broadcasted_iota(jnp.int32, (2 * HD, FEAT), 0)
    for pair in range(PAIRS):
        lanes = slice(pair * 2 * HD, (pair + 1) * 2 * HD)
        scaled = do_ref[:, lanes] * rden_ref[:, lanes]
        product = scaled * o_ref[:, lanes].astype(f32)
        scaled = scaled.astype(bf16).astype(f32)
        ones = with_ones(qkv_ref[:, 2 * D + pair * 2 * HD : 2 * D + (pair + 1) * 2 * HD], low)
        back_q, back_k, back_v = [], [], []
        for odd in range(2):
            head = 2 * pair + odd
            free = 0 if odd else HD
            mine = jnp.logical_not(low) if odd else low
            grad_den = -jnp.sum(jnp.where(mine, product, 0.0), axis=-1, keepdims=True)
            grad_one = jnp.where(
                mine, scaled, jnp.where(lane == free, grad_den, 0.0)
            ).astype(bf16)
            query_feat = fq_ref[:, head * FEAT : (head + 1) * FEAT]
            key_feat = fk_ref[:, head * FEAT : (head + 1) * FEAT]
            one = ones[odd]
            after = suffix_ref[head]
            edge = after[free : free + 1, :]
            rest = edge - edge.astype(bf16).astype(f32)
            after_low = jnp.where(state_row == free + 1, rest, after).astype(bf16)
            before_low = prefix_ref[0, head]
            weights_t = jnp.where(anti, dot_nt(key_feat, query_feat), 0.0).astype(bf16)
            grad_w = jnp.where(causal, dot_nt(grad_one, one), 0.0).astype(bf16)
            grad_wt = jnp.where(anti, dot_nt(one, grad_one), 0.0).astype(bf16)
            grad_fq = dot_nn(grad_w, key_feat) + dot_nn(grad_one, before_low)
            grad_fk = dot_nn(grad_wt, query_feat) + dot_nn(one, after_low)
            back_v.append(dot_nn(weights_t, grad_one) + dot_nt(key_feat, after_low))
            suffix_ref[head] = after + dot_tn(grad_one, query_feat)
            grad_pq = (grad_fq * query_feat.astype(f32) * feat_scale).astype(bf16)
            grad_pk = (grad_fk * key_feat.astype(f32) * feat_scale).astype(bf16)
            back_q.append(dot_nt(grad_pq, omega_ref[head]))
            back_k.append(dot_nt(grad_pk, omega_ref[head]))
        for part, back in enumerate((back_q, back_k)):
            at = slice(part * D + pair * 2 * HD, part * D + (pair + 1) * 2 * HD)
            top = jnp.where(low, back[0], back[1])
            bottom = pltpu.roll(jnp.where(low, back[1], back[0]), HD, 1)
            dqkv_ref[:, at] = (
                top - bottom * feat_scale * qkv_ref[:, at].astype(f32)
            ).astype(bf16)
        dqkv_ref[:, 2 * D + pair * 2 * HD : 2 * D + (pair + 1) * 2 * HD] = jnp.where(
            low, back_v[0], back_v[1]
        ).astype(bf16)

    unit, inverse = normalise(x_ref[...].astype(f32))
    normed_t = (unit * gain).astype(bf16).T
    acc_ref[...] += dot_nn(normed_t, dqkv_ref[...])
    grad_normed = dot_nt(dqkv_ref[...], weight())
    dgain_ref[0:1, :] += jnp.sum(grad_normed * unit, axis=0, keepdims=True)
    gin_ref[...] = dmid_ref[...] + normalise_back(grad_normed, gain, unit, inverse)


def gain_block(dgain_ref, dgain2_ref):
    first = dgain_ref[0:1, :]
    second = dgain2_ref[0:1, :]
    rows = [first[:, i * 128 : (i + 1) * 128] for i in range(4)]
    rows += [second[:, i * 128 : (i + 1) * 128] for i in range(4)]
    rows += [jnp.zeros((8, 128), f32)]
    return jnp.concatenate(rows, axis=0).astype(bf16)


def attention_backward_local_kernel(
    tiles,
    starts_ref, x_ref, qkv_ref, fq_ref, fk_ref, o_ref, rden_ref, do_ref, dmid_ref,
    prefix_ref, w_ref, gain_ref, omega_ref,
    gin_ref, gw_ref, dgain_ref, acc_ref, suffix_ref, dqkv_ref, wide_ref,
):
    step = pl.program_id(0)

    @pl.when(step == 0)
    def _():
        ones_projection(omega_ref, wide_ref)

    attention_backward_tile(
        tiles - 1 - step, tiles, starts_ref, x_ref, qkv_ref, fq_ref, fk_ref, o_ref, rden_ref, do_ref, dmid_ref,
        prefix_ref, lambda: w_ref[...], gain_ref[0:1, :], wide_ref, gin_ref, acc_ref, suffix_ref, dqkv_ref, dgain_ref,
    )

    @pl.when(step == tiles - 1)
    def _():
        gw_ref[...] = acc_ref[...].astype(bf16)


def scatter_copy(at, grad, part, sums, boxes, send, recv, k):
    z, core = at["z"], at["core"]
    if k == 0:
        src, dst, device = grad.at[:, :, 1 - core], sums, {"fsdp": z * 2 + 1 - core}
    elif k == 1:
        src, dst, device = part.at[at["diag"]], boxes.at[0], {"dp": at["second"]}
    elif k == 2:
        src, dst, device = part.at[at["second"]], boxes.at[1], {"dp": at["second"]}
    elif k == 3:
        src, dst, device = part.at[at["first"]], boxes.at[2], {"dp": at["first"]}
    else:
        there = (z + k - 3) % 4
        src, dst, device = part.at[at["dp"], there], boxes.at[3, k - 4], {"fsdp": there * 2 + core}
    return pltpu.make_async_remote_copy(
        src_ref=src, dst_ref=dst, send_sem=send.at[k], recv_sem=recv.at[k],
        device_id=device, device_id_type=MESH,
    )


def add_low(left, right):
    return (left.astype(f32) + right.astype(f32)).astype(bf16)


def scatter_last(at, part, boxes):
    total = part[at["dp"], at["z"]].astype(f32)
    for i in range(3):
        total = total + boxes[3, i].astype(f32)
    return total


def attention_backward_kernel(
    tiles,
    starts_ref, x_ref, qkv_ref, fq_ref, fk_ref, o_ref, rden_ref, do_ref, dmid_ref,
    prefix_ref, w_ref, gain_ref, omega_ref, dgain2_ref, go_ref, gu_ref, gd_ref,
    gin_ref, gw_ref, ro_ref, ru_ref, rd_ref,
    acc_ref, suffix_ref, dqkv_ref, dgain_ref, wide_ref,
    po_ref, pu_ref, pd_ref, so_ref, su_ref, sd_ref, bo_ref, bu_ref, bd_ref, send, recv, local,
):
    step = pl.program_id(0)
    at = place()
    dp, core = at["dp"], at["core"]
    grads, parts, sums, boxes, results = (
        (go_ref, gu_ref, gd_ref), (po_ref, pu_ref, pd_ref), (so_ref, su_ref, sd_ref),
        (bo_ref, bu_ref, bd_ref), (ro_ref, ru_ref, rd_ref),
    )

    def copy(w, k):
        return scatter_copy(at, grads[w], parts[w], sums[w], boxes[w], send.at[w], recv.at[w], k)

    def keep(w):
        return pltpu.make_async_copy(grads[w].at[:, :, core], parts[w], local.at[w])

    @pl.when(step == 0)
    def _():
        greet(near_devices(at))
        for w in range(3):
            copy(w, 0).start()
            keep(w).start()
        ones_projection(omega_ref, wide_ref)

    @pl.when(step == 1)
    def _():
        for w in range(3):
            keep(w).wait()
            copy(w, 0).wait_recv()
            parts[w][at["diag"]] = add_low(parts[w][at["diag"]], sums[w][at["diag"]])
            copy(w, 1).start()
        for w in range(3):
            for name in ("second", "first", "dp"):
                parts[w][at[name]] = add_low(parts[w][at[name]], sums[w][at[name]])
                if name == "second":
                    copy(w, 2).start()

    @pl.when(step == 3)
    def _():
        for w in range(3):
            copy(w, 1).wait_recv()
            parts[w][at["first"]] = add_low(parts[w][at["first"]], boxes[w][0])
            copy(w, 3).start()

    @pl.when(step == 5)
    def _():
        for w in range(3):
            copy(w, 2).wait_recv()
            copy(w, 3).wait_recv()
            parts[w][dp] = add_low(add_low(parts[w][dp], boxes[w][1]), boxes[w][2])
            for k in (4, 5, 6):
                copy(w, k).start()

    attention_backward_tile(
        tiles - 1 - step, tiles, starts_ref, x_ref, qkv_ref, fq_ref, fk_ref, o_ref, rden_ref, do_ref, dmid_ref,
        prefix_ref, lambda: w_ref[...], gain_ref[0:1, :], wide_ref, gin_ref, acc_ref, suffix_ref, dqkv_ref, dgain_ref,
    )

    @pl.when(step == tiles - 1)
    def _():
        gw_ref[:, :WIDE] = acc_ref[...].astype(bf16)
        stacked = gain_block(dgain_ref, dgain2_ref)
        for i in range(D // 16):
            gw_ref[16 * i : 16 * (i + 1), WIDE:] = stacked
        for w in range(3):
            for k in (4, 5, 6):
                copy(w, k).wait_recv()
            results[w][...] = scatter_last(at, parts[w], boxes[w])
            for k in range(7):
                copy(w, k).wait_send()


def finish_kernel(
    gq_ref, ro_ref, ru_ref, rd_ref,
    rq_ref, norm_ref,
    part_ref, sums_ref, boxes_ref, near_ref, far_ref, send, recv, near_send, near_recv, far_send, far_recv,
):
    at = place()
    dp, z, core = at["dp"], at["z"], at["core"]
    inner = z * 2 + core

    def copy(k):
        return scatter_copy(at, gq_ref, part_ref, sums_ref, boxes_ref, send, recv, k)

    others = [{"fsdp": (z + i // 2) % 4 * 2 + (core + i) % 2} for i in range(1, 8)]
    far = [{"dp": (dp + i) % 4} for i in range(1, 4)]
    greet(others + far)
    copy(0).start()
    row = lax.broadcasted_iota(jnp.int32, (16, EXTRA), 0)
    lane = lax.broadcasted_iota(jnp.int32, (16, EXTRA), 1)
    index = flat_index(at)
    mine = jnp.logical_and(row % 4 == index // 8, lane // 16 == index % 8)
    mine = jnp.logical_and(mine, row < 8)

    def squares(value):
        return jnp.sum((value * value).reshape(-1, 8, value.shape[-1]), axis=0)

    def narrow(value):
        return sum(value[:, 128 * i : 128 * (i + 1)] for i in range(value.shape[1] // 128))

    local = narrow(squares(ro_ref[...])) + narrow(squares(ru_ref[...])) + narrow(squares(rd_ref[...]))
    copy(0).wait_recv()
    for name in ("diag", "second", "first", "dp"):
        part_ref[at[name]] = add_low(gq_ref[at[name], :, core], sums_ref[at[name]])
        if name == "diag":
            copy(1).start()
        if name == "second":
            copy(2).start()
    copy(1).wait_recv()
    part_ref[at["first"]] = add_low(part_ref[at["first"]], boxes_ref[0])
    copy(3).start()
    copy(2).wait_recv()
    part_ref[dp] = add_low(part_ref[dp], boxes_ref[1])
    copy(3).wait_recv()
    part_ref[dp] = add_low(part_ref[dp], boxes_ref[2])
    for k in (4, 5, 6):
        copy(k).start()
    for k in (4, 5, 6):
        copy(k).wait_recv()
    total = scatter_last(at, part_ref, boxes_ref)
    rq_ref[...] = total
    local = local + narrow(squares(total[:, :WIDE])) + squares(jnp.where(mine, total[:, WIDE:], 0.0))
    near_ref[inner] = local

    def near(i):
        return pltpu.make_async_remote_copy(
            src_ref=near_ref.at[inner], dst_ref=near_ref.at[inner], send_sem=near_send.at[i],
            recv_sem=near_recv.at[i], device_id=others[i], device_id_type=MESH,
        )

    def across(i):
        return pltpu.make_async_remote_copy(
            src_ref=far_ref.at[dp], dst_ref=far_ref.at[dp], send_sem=far_send.at[i],
            recv_sem=far_recv.at[i], device_id=far[i], device_id_type=MESH,
        )

    for i in range(7):
        near(i).start()
    for i in range(7):
        near(i).wait_recv()
    group = near_ref[0]
    for i in range(1, 8):
        group = group + near_ref[i]
    far_ref[dp] = group
    for i in range(3):
        across(i).start()
    for i in range(3):
        across(i).wait_recv()
    norm_ref[...] = far_ref[0] + far_ref[1] + far_ref[2] + far_ref[3]
    for i in range(7):
        near(i).wait_send()
    for i in range(3):
        across(i).wait_send()
    for k in range(7):
        copy(k).wait_send()


def update_kernel(
    index_ref, count_ref, rq_ref, ro_ref, ru_ref, rd_ref, total_ref,
    wq_ref, wo_ref, wu_ref, wd_ref, wg_ref, mq_ref, mo_ref, mu_ref, md_ref, mg_ref,
    vq_ref, vo_ref, vu_ref, vd_ref, vg_ref,
    norm_ref, gq_ref, nvq_ref, nwq_ref, go_ref, nvo_ref, nwo_ref, gu_ref, nvu_ref, nwu_ref,
    gd_ref, nvd_ref, nwd_ref, gg_ref, nvg_ref, nwg_ref,
):
    total = jnp.sum(jnp.sum(total_ref[...], axis=0, keepdims=True), axis=1, keepdims=True)
    norm = jnp.sqrt(total)
    norm_ref[...] = norm
    factor = jnp.minimum(1.0, clip_level / norm)
    count = jnp.full((1, 1), count_ref[0], jnp.int32).astype(f32)
    first_fix = 1.0 - jnp.exp2(count * math.log2(beta_first))
    second_fix = 1.0 - jnp.exp2(count * math.log2(beta_second))

    def update(grad, weight, first, second, rate, outs):
        clipped = grad * factor
        first_new = beta_first * first + (1.0 - beta_first) * clipped
        second_new = beta_second * second + (1.0 - beta_second) * clipped * clipped
        direction = first_new / first_fix / (jnp.sqrt(second_new / second_fix) + adam_eps)
        outs[0][...] = clipped
        outs[1][...] = second_new
        outs[2][...] = weight - rate * (direction + decay_weight * weight)

    update(rq_ref[:, :WIDE], wq_ref[...], mq_ref[...], vq_ref[...], rate_matrix, (gq_ref, nvq_ref, nwq_ref))
    update(ro_ref[...], wo_ref[...], mo_ref[...], vo_ref[...], rate_matrix, (go_ref, nvo_ref, nwo_ref))
    update(ru_ref[...], wu_ref[...], mu_ref[...], vu_ref[...], rate_matrix, (gu_ref, nvu_ref, nwu_ref))
    update(rd_ref[...], wd_ref[...], md_ref[...], vd_ref[...], rate_matrix, (gd_ref, nvd_ref, nwd_ref))
    index = index_ref[0]
    packed = rq_ref[:8, WIDE:]
    row = lax.broadcasted_iota(jnp.int32, (8, EXTRA), 0)
    packed = jnp.where(row % 4 == index // 8, packed, 0.0)
    turned = packed
    for i in range(1, 8):
        turned = jnp.where(index % 8 == i, pltpu.roll(packed, EXTRA - 16 * i, 1), turned)
    grad = jnp.concatenate(
        [jnp.sum(turned[:4], axis=0, keepdims=True), jnp.sum(turned[4:], axis=0, keepdims=True)], axis=0
    )[:, :16]
    update(grad, wg_ref[...], mg_ref[...], vg_ref[...], rate_gain, (gg_ref, nvg_ref, nwg_ref))


def feed_forward_kernel(
    block, chunk,
    lens_ref, x_ref, o_ref, cot_ref, wo_ref, wu_ref, wd_ref, gain_ref,
    out_ref, dmid_ref, do_ref, gwo_ref, gwu_ref, gwd_ref, dgain_ref,
    awo_ref, awu_ref, awd_ref, norm_ref, normt_ref, dyt_ref, dy_ref, y_ref, dn_ref,
):
    step = pl.program_id(0)
    steps = pl.num_programs(0)

    @pl.when(step == 0)
    def _():
        awo_ref[...] = jnp.zeros_like(awo_ref)
        awu_ref[...] = jnp.zeros_like(awu_ref)
        awd_ref[...] = jnp.zeros_like(awd_ref)
        dgain_ref[...] = jnp.zeros_like(dgain_ref)

    per_seg = SEG // block
    place = lax.broadcasted_iota(jnp.int32, (block, 1), 0) + (step % per_seg) * block
    valid = (place < lens_ref[step // per_seg]).astype(f32)
    dy = (cot_ref[...].astype(f32) * valid).astype(bf16)
    dy_ref[...] = dy
    dyt_ref[...] = dy.T
    gain = gain_ref[1:2, :]
    attended = o_ref[...]
    middle = x_ref[...].astype(f32) + dot_nn(attended, wo_ref[...])
    unit, inverse = normalise(middle)
    normed = (unit * gain).astype(bf16)
    norm_ref[...] = normed
    normt_ref[...] = normed.T
    y_ref[...] = middle
    dn_ref[...] = jnp.zeros_like(dn_ref)

    @pl.loop(0, FF // chunk)
    def _(index):
        at = pl.ds(pl.multiple_of(index * chunk, chunk), chunk)
        hidden = dot_nn(norm_ref[...], wu_ref[:, at])
        inner = 0.5 + 0.5 * lax.erf(hidden * (0.5**0.5))
        bell = jnp.exp2(hidden * hidden * (-0.5 * log2_e)) * (1.0 / math.sqrt(2.0 * math.pi))
        active = (hidden * inner).astype(bf16)
        slope = inner + hidden * bell
        y_ref[...] += dot_nn(active, wd_ref[at, :])
        grad_hidden = (slope * dot_nt(dy_ref[...], wd_ref[at, :])).astype(bf16)
        awd_ref[:, at] += dot_nn(dyt_ref[...], active)
        awu_ref[:, at] += dot_nn(normt_ref[...], grad_hidden)
        dn_ref[...] += dot_nt(grad_hidden, wu_ref[:, at])

    out_ref[...] = y_ref[...].astype(bf16)
    grad_normed = dn_ref[...]
    dgain_ref[0:1, :] += jnp.sum(grad_normed * unit, axis=0, keepdims=True)
    grad_middle = dy_ref[...].astype(f32) + normalise_back(grad_normed, gain, unit, inverse)
    dmid_ref[...] = grad_middle
    branch = grad_middle.astype(bf16)
    awo_ref[...] += dot_tn(attended, branch)
    do_ref[...] = dot_nt(branch, wo_ref[...])

    @pl.when(step == steps - 1)
    def _():
        gwo_ref[...] = awo_ref[...].astype(bf16)
        gwu_ref[...] = awu_ref[...].astype(bf16)
        gwd_ref[...] = awd_ref[...].astype(bf16).T


def whole(shape):
    return pl.BlockSpec(shape, lambda i: (0,) * len(shape), pipeline_mode=pl.Buffered(1))


def whole_out(shape):
    return pl.BlockSpec(shape, lambda i: (0,) * len(shape))


smem = pl.BlockSpec(memory_space=pltpu.SMEM)


def feed_forward(lens, x, o, cot, wo, wu, wd, gains, block=512, chunk=512):
    tokens = x.shape[0]

    def rows(width):
        return pl.BlockSpec((block, width), lambda i: (i, 0))

    return pl.pallas_call(
        functools.partial(feed_forward_kernel, block, chunk),
        grid=(tokens // block,),
        in_specs=[smem, rows(D), rows(D), rows(D), whole((D, D)), whole((D, FF)), whole((FF, D)), whole((8, D))],
        out_specs=[rows(D), rows(D), rows(D), whole_out((D, D)), whole_out((D, FF)), whole_out((FF, D)), whole_out((8, D))],
        out_shape=[
            jax.ShapeDtypeStruct((tokens, D), bf16),
            jax.ShapeDtypeStruct((tokens, D), f32),
            jax.ShapeDtypeStruct((tokens, D), f32),
            jax.ShapeDtypeStruct((D, D), bf16),
            jax.ShapeDtypeStruct((D, FF), bf16),
            jax.ShapeDtypeStruct((FF, D), bf16),
            jax.ShapeDtypeStruct((8, D), f32),
        ],
        scratch_shapes=[
            pltpu.VMEM((D, D), f32), pltpu.VMEM((D, FF), f32), pltpu.VMEM((D, FF), f32),
            pltpu.VMEM((block, D), bf16), pltpu.VMEM((D, block), bf16), pltpu.VMEM((D, block), bf16),
            pltpu.VMEM((block, D), bf16), pltpu.VMEM((block, D), f32), pltpu.VMEM((block, D), f32),
        ],
        compiler_params=pltpu.CompilerParams(vmem_limit_bytes=60 << 20),
    )(lens, x, o, cot, wo, wu, wd, gains)


def tile_rows(width, tiles=None):
    if tiles is None:
        return pl.BlockSpec((TILE, width), lambda i: (i, 0))
    return pl.BlockSpec((TILE, width), lambda i: (tiles - 1 - i, 0))


hbm = pl.BlockSpec(memory_space=pl.ANY)
vmem = pl.BlockSpec(memory_space=pltpu.VMEM)


def five(name, dtype=bf16):
    return (4, 4, 2, ROWS[name], COLS[name])


def forward_outs(tokens):
    tiles = tokens // TILE
    specs = [tile_rows(WIDE), tile_rows(HEADS * FEAT), tile_rows(HEADS * FEAT), tile_rows(D), tile_rows(D),
             pl.BlockSpec((1, HEADS, 2 * HD, FEAT), lambda i: (i, 0, 0, 0))]
    shapes = [
        jax.ShapeDtypeStruct((tokens, WIDE), bf16),
        jax.ShapeDtypeStruct((tokens, HEADS * FEAT), bf16),
        jax.ShapeDtypeStruct((tokens, HEADS * FEAT), bf16),
        jax.ShapeDtypeStruct((tokens, D), bf16),
        jax.ShapeDtypeStruct((tokens, D), f32),
        jax.ShapeDtypeStruct((tiles, HEADS, 2 * HD, FEAT), bf16),
    ]
    scratch = [pltpu.VMEM((HEADS, 2 * HD, FEAT), f32), pltpu.VMEM((PAIRS, 2 * HD, 2 * FEAT), bf16)]
    return specs, shapes, scratch


def attention_forward_local(starts, lens, x, w_qkv, gains, omega):
    tokens = x.shape[0]
    specs, shapes, scratch = forward_outs(tokens)
    return pl.pallas_call(
        attention_forward_local_kernel,
        grid=(tokens // TILE,),
        in_specs=[smem, smem, tile_rows(D), whole((D, WIDE)), whole((8, D)), whole((HEADS, HD, FEAT))],
        out_specs=specs,
        out_shape=shapes,
        scratch_shapes=scratch,
        compiler_params=pltpu.CompilerParams(vmem_limit_bytes=48 << 20),
    )(starts, lens, x, w_qkv, gains, omega)


def attention_forward(starts, lens, x, omega, wq, wo, wu, wd, gains):
    tokens = x.shape[0]
    specs, shapes, scratch = forward_outs(tokens)
    return pl.pallas_call(
        attention_forward_kernel,
        grid=(tokens // TILE,),
        in_specs=[smem, smem, tile_rows(D), whole((HEADS, HD, FEAT)), whole(wq.shape), whole(wo.shape), whole(wu.shape),
                  whole(wd.shape), whole(gains.shape)],
        out_specs=specs + [whole_out((8, D)), hbm, hbm, hbm, hbm],
        out_shape=shapes + [jax.ShapeDtypeStruct((8, D), f32)]
        + [jax.ShapeDtypeStruct(five(name), bf16) for name in ("qkv",) + LATE],
        scratch_shapes=scratch + [pltpu.VMEM(five("qkv"), bf16)]
        + [pltpu.VMEM((ROWS[name], COLS[name]), bf16) for name in LATE]
        + [pltpu.VMEM((8, 128), f32), pltpu.SemaphoreType.DMA((4, 10)), pltpu.SemaphoreType.DMA((4, 10)),
           pltpu.SemaphoreType.DMA((4,))],
        compiler_params=pltpu.CompilerParams(vmem_limit_bytes=48 << 20, collective_id=0, has_side_effects=True),
    )(starts, lens, x, omega, wq, wo, wu, wd, gains)


def backward_specs(tokens):
    tiles = tokens // TILE
    rows = functools.partial(tile_rows, tiles=tiles)
    ins = [smem, rows(D), rows(WIDE), rows(HEADS * FEAT), rows(HEADS * FEAT), rows(D), rows(D), rows(D), rows(D),
           pl.BlockSpec((1, HEADS, 2 * HD, FEAT), lambda i: (tiles - 1 - i, 0, 0, 0)),
           whole((D, WIDE)), whole((8, D)), whole((HEADS, HD, FEAT))]
    scratch = [pltpu.VMEM((D, WIDE), f32), pltpu.VMEM((HEADS, 2 * HD, FEAT), f32), pltpu.VMEM((TILE, WIDE), bf16)]
    wide = pltpu.VMEM((HEADS, 2 * HD, FEAT), bf16)
    return tiles, rows(D), ins, scratch, wide


def attention_backward_local(args):
    tokens = args[1].shape[0]
    tiles, rows, ins, scratch, wide = backward_specs(tokens)
    return pl.pallas_call(
        functools.partial(attention_backward_local_kernel, tiles),
        grid=(tiles,),
        in_specs=ins,
        out_specs=[rows, whole_out((D, WIDE)), whole_out((8, D))],
        out_shape=[
            jax.ShapeDtypeStruct((tokens, D), f32),
            jax.ShapeDtypeStruct((D, WIDE), bf16),
            jax.ShapeDtypeStruct((8, D), f32),
        ],
        scratch_shapes=scratch + [wide],
        compiler_params=pltpu.CompilerParams(vmem_limit_bytes=56 << 20),
    )(*args)


def attention_backward(args, dgain2, grads):
    tokens = args[1].shape[0]
    tiles, rows, ins, scratch, wide = backward_specs(tokens)
    half = [(4, 4, ROWS[name], COLS[name]) for name in LATE]
    grads = [grad.reshape(five(name)) for grad, name in zip(grads, LATE)]
    return pl.pallas_call(
        functools.partial(attention_backward_kernel, tiles),
        grid=(tiles,),
        in_specs=ins + [whole((8, D)), hbm, hbm, hbm],
        out_specs=[rows, whole_out((D, FULL))] + [whole_out((ROWS[name], COLS[name])) for name in LATE],
        out_shape=[
            jax.ShapeDtypeStruct((tokens, D), f32),
            jax.ShapeDtypeStruct((D, FULL), bf16),
        ]
        + [jax.ShapeDtypeStruct((ROWS[name], COLS[name]), f32) for name in LATE],
        scratch_shapes=scratch
        + [pltpu.VMEM((8, D), f32), wide]
        + [pltpu.VMEM(shape, bf16) for shape in half]
        + [pltpu.VMEM(shape, bf16) for shape in half]
        + [pltpu.VMEM(shape, bf16) for shape in half]
        + [pltpu.SemaphoreType.DMA((3, 7)), pltpu.SemaphoreType.DMA((3, 7)), pltpu.SemaphoreType.DMA((3,))],
        compiler_params=pltpu.CompilerParams(vmem_limit_bytes=60 << 20, collective_id=1, has_side_effects=True),
    )(*args, dgain2, *grads)


def finish(grad_wide, reduced):
    grad_wide = grad_wide.reshape(five("qkv"))
    half = (4, 4, 16, FULL)
    return pl.pallas_call(
        finish_kernel,
        in_specs=[vmem] * 4,
        out_specs=[vmem] * 2,
        out_shape=[jax.ShapeDtypeStruct((16, FULL), f32), jax.ShapeDtypeStruct((8, 128), f32)],
        scratch_shapes=[pltpu.VMEM(half, bf16)] * 3
        + [pltpu.VMEM((8, 8, 128), f32), pltpu.VMEM((4, 8, 128), f32)]
        + [pltpu.SemaphoreType.DMA((7,))] * 4
        + [pltpu.SemaphoreType.DMA((3,))] * 2,
        compiler_params=pltpu.CompilerParams(vmem_limit_bytes=48 << 20, collective_id=2, has_side_effects=True),
    )(grad_wide, *reduced)


def update_all(index, count, grads, total, weights, firsts, seconds):
    shapes = [jax.ShapeDtypeStruct((1, 1), f32)]
    for weight in weights:
        shapes += [jax.ShapeDtypeStruct(weight.shape, f32)] * 3
    return pl.pallas_call(
        update_kernel,
        in_specs=[smem, smem] + [vmem] * 20,
        out_specs=[vmem] * 16,
        out_shape=shapes,
    )(index.reshape(1), count.reshape(1), *grads, total, *weights, *firsts, *seconds)


def on_device(
    sizes, inputs, cotangent, feature_omega, seg_start, seg_len, step_count,
    w_qkv, w_out, w_up, w_down, gains,
    m_qkv, m_out, m_up, m_down, m_gains,
    v_qkv, v_out, v_up, v_down, v_gains,
):
    weights = (w_qkv, w_out, w_up, w_down, gains)
    firsts = (m_qkv, m_out, m_up, m_down, m_gains)
    seconds = (v_qkv, v_out, v_up, v_down, v_gains)
    if sizes == (4, 8):
        (qkv, fq, fk, attended, rden, prefix, gain_full, qkv_full, out_full, up_full, down_full) = attention_forward(
            seg_start, seg_len, inputs, feature_omega, *weights
        )
        qkv_full = qkv_full.reshape(D, FULL)
        out_rows, dmid, grad_attended, grad_out, grad_up, grad_down, dgain2 = feed_forward(
            seg_len, inputs, attended, cotangent, out_full.reshape(D, D), up_full.reshape(D, FF),
            down_full.reshape(FF, D), gain_full,
        )
        grad_inputs, grad_wide, *late = attention_backward(
            (seg_start, inputs, qkv, fq, fk, attended, rden, grad_attended, dmid, prefix, qkv_full, gain_full,
             feature_omega),
            dgain2, (grad_out, grad_up, grad_down),
        )
        reduced, total = finish(grad_wide, late)
        index = lax.axis_index("dp") * 8 + lax.axis_index("fsdp")
        norm, *updated = update_all(index, step_count, (reduced, *late), total, weights, firsts, seconds)
        return (out_rows, grad_inputs, norm.reshape(()), *updated)

    def gather(piece, axis=0):
        return lax.all_gather(piece.astype(bf16), AXES, axis=axis, tiled=True)

    qkv_full, out_full, up_full, down_full = (gather(piece) for piece in weights[:4])
    gain_full = jnp.pad(gather(gains, 1).astype(f32), ((0, 6), (0, 0)))
    qkv, fq, fk, attended, rden, prefix = attention_forward_local(
        seg_start, seg_len, inputs, qkv_full, gain_full, feature_omega
    )
    out_rows, dmid, grad_attended, grad_out, grad_up, grad_down, dgain2 = feed_forward(
        seg_len, inputs, attended, cotangent, out_full, up_full, down_full, gain_full
    )
    grad_inputs, grad_qkv, dgain = attention_backward_local(
        (seg_start, inputs, qkv, fq, fk, attended, rden, grad_attended, dmid, prefix, qkv_full, gain_full,
         feature_omega)
    )

    def scatter(piece, axis=0):
        return lax.psum_scatter(piece.astype(f32), AXES, scatter_dimension=axis, tiled=True)

    reduced = [scatter(piece) for piece in (grad_qkv, grad_out, grad_up, grad_down)]
    reduced.append(scatter(jnp.concatenate([dgain[:1], dgain2[:1]], axis=0), 1))
    grad_norm = jnp.sqrt(lax.psum(sum(jnp.sum(piece * piece) for piece in reduced), AXES))
    factor = jnp.minimum(1.0, clip_level / grad_norm)
    count = step_count.astype(f32)
    first_fix = 1.0 - jnp.power(beta_first, count)
    second_fix = 1.0 - jnp.power(beta_second, count)
    updated = []
    rates = (rate_matrix,) * 4 + (rate_gain,)
    for weight, first, second, gradient, rate in zip(weights, firsts, seconds, reduced, rates):
        clipped = gradient * factor
        first_new = beta_first * first + (1.0 - beta_first) * clipped
        second_new = beta_second * second + (1.0 - beta_second) * clipped * clipped
        direction = first_new / first_fix / (jnp.sqrt(second_new / second_fix) + adam_eps)
        updated += [clipped, second_new, weight - rate * (direction + decay_weight * weight)]
    return (out_rows, grad_inputs, grad_norm, *updated)


def solution(mesh):
    return jax.shard_map(
        functools.partial(on_device, tuple(mesh.shape[name] for name in AXES)),
        mesh=mesh,
        in_specs=(
            P(("dp", "fsdp"), None),
            P(("dp", "fsdp"), None),
            P(),
            P(("dp", "fsdp")),
            P(("dp", "fsdp")),
            P(),
            P(("dp", "fsdp"), None),
            P(("dp", "fsdp"), None),
            P(("dp", "fsdp"), None),
            P(("dp", "fsdp"), None),
            P(None, ("dp", "fsdp")),
            P(("dp", "fsdp"), None),
            P(("dp", "fsdp"), None),
            P(("dp", "fsdp"), None),
            P(("dp", "fsdp"), None),
            P(None, ("dp", "fsdp")),
            P(("dp", "fsdp"), None),
            P(("dp", "fsdp"), None),
            P(("dp", "fsdp"), None),
            P(("dp", "fsdp"), None),
            P(None, ("dp", "fsdp")),
        ),
        out_specs=(
            P(("dp", "fsdp"), None),
            P(("dp", "fsdp"), None),
            P(),
            P(("dp", "fsdp"), None),
            P(("dp", "fsdp"), None),
            P(("dp", "fsdp"), None),
            P(("dp", "fsdp"), None),
            P(("dp", "fsdp"), None),
            P(("dp", "fsdp"), None),
            P(("dp", "fsdp"), None),
            P(("dp", "fsdp"), None),
            P(("dp", "fsdp"), None),
            P(("dp", "fsdp"), None),
            P(("dp", "fsdp"), None),
            P(("dp", "fsdp"), None),
            P(None, ("dp", "fsdp")),
            P(None, ("dp", "fsdp")),
            P(None, ("dp", "fsdp")),
        ),
        check_vma=False,
    )
```

```python
import functools
import math

import jax
import jax.numpy as jnp
from jax import lax
from jax.experimental import pallas as pl
from jax.experimental.pallas import tpu as pltpu
from jax.sharding import PartitionSpec as P

D = 512
HEADS = 8
HD = 64
FEAT = 256
FF = 2048
SEG = 1024
TILE = 256
PAIRS = HEADS // 2
DUO = 2 * HD
BLOCK = 1024
TILES_BLOCK = BLOCK // TILE
UPDATE_ROWS = 512
WIDE = 3 * D
CHUNK = 3 * DUO
EXTRA = 128
AXES = ("dp", "fsdp")

norm_eps = 1e-05
clip_level = 1.0
rate_matrix = 0.03
rate_gain = 0.4
beta_first = 0.9
beta_second = 0.95
adam_eps = 1e-08
decay_weight = 0.1

feat_scale = HD ** (-0.25)
log2_e = math.log2(math.e)
f32 = jnp.float32
bf16 = jnp.bfloat16
MESH = pl.DeviceIdType.MESH
VMEM_LIMIT = 63 << 20


def dot_nn(a, b):
    return lax.dot_general(a, b, (((1,), (0,)), ((), ())), preferred_element_type=f32)


def dot_nt(a, b):
    return lax.dot_general(a, b, (((1,), (1,)), ((), ())), preferred_element_type=f32)


def dot_tn(a, b):
    return lax.dot_general(a, b, (((0,), (0,)), ((), ())), preferred_element_type=f32)


def normalise(rows):
    centred = rows - jnp.mean(rows, axis=-1, keepdims=True)
    spread = jnp.mean(centred * centred, axis=-1, keepdims=True)
    inverse = lax.rsqrt(spread + norm_eps)
    return centred * inverse, inverse


def normalise_back(grad, gain, unit, inverse):
    scaled = grad * gain
    first = jnp.mean(scaled, axis=-1, keepdims=True)
    second = jnp.mean(scaled * unit, axis=-1, keepdims=True)
    return inverse * (scaled - first - unit * second)


def lane_masks(rows):
    lane = lax.broadcasted_iota(jnp.int32, (rows, DUO), 1)
    return lane, lane < HD


def causal_masks():
    row = lax.broadcasted_iota(jnp.int32, (TILE, TILE), 0)
    col = lax.broadcasted_iota(jnp.int32, (TILE, TILE), 1)
    return row >= col, row <= col


def with_ones(value_pair, low):
    wide = value_pair.astype(f32)
    return (
        jnp.where(low, wide, 1.0).astype(bf16),
        jnp.where(low, 1.0, wide).astype(bf16),
    )


def place():
    dp, inner = lax.axis_index("dp"), lax.axis_index("fsdp")
    z, core = inner // 2, inner % 2
    y, x = dp // 2, dp % 2
    across = y * 2 + (1 - x)
    along = (1 - y) * 2 + x
    return {
        "dp": dp, "z": z, "core": core, "flat": dp * 8 + inner,
        "first": core * along + (1 - core) * across,
        "second": core * across + (1 - core) * along,
        "diag": (1 - y) * 2 + (1 - x),
    }


def greet(devices):
    barrier = pltpu.get_barrier_semaphore()
    for device in devices:
        pl.semaphore_signal(barrier, inc=1, device_id=device, device_id_type=MESH)


def greeted(devices):
    pl.semaphore_wait(pltpu.get_barrier_semaphore(), len(devices))


def near_devices(at):
    devices = [{"fsdp": (at["z"] + i) % 4 * 2 + at["core"]} for i in range(1, 4)]
    devices += [{"fsdp": at["z"] * 2 + 1 - at["core"]}]
    devices += [{"dp": at["first"]}, {"dp": at["second"]}]
    return devices


def halves(up, down):
    return [up.at[..., i * (FF // 2) : (i + 1) * (FF // 2)] for i in range(2)] + [
        down.at[:, :, :, i * 32 : (i + 1) * 32, :] for i in range(2)
    ]


def gather_copy(at, own, full, send, recv, k):
    dp, z, core = at["dp"], at["z"], at["core"]
    sibling = {"fsdp": z * 2 + 1 - core}
    if k < 3:
        src, dst, device = own, full.at[dp, z, core], {"fsdp": (z + 1 + k) % 4 * 2 + core}
    else:
        which = {3: "dp", 4: "dp", 5: "dp", 6: "first", 7: "first", 8: "second", 9: "diag"}[k]
        src = dst = full.at[at[which], :, core]
        device = {4: {"dp": at["first"]}, 5: {"dp": at["second"]}, 6: {"dp": at["second"]}}.get(k, sibling)
    return pltpu.make_async_remote_copy(
        src_ref=src, dst_ref=dst, send_sem=send.at[k], recv_sem=recv.at[k],
        device_id=device, device_id_type=MESH,
    )


def gather_stage(copy, stage):
    if stage == 0:
        for k in range(3):
            copy(k).start()
    elif stage == 1:
        for k in range(3):
            copy(k).wait_recv()
        for k in (4, 5, 3):
            copy(k).start()
    elif stage == 2:
        copy(4).wait_recv()
        copy(6).start()
        copy(7).start()
        copy(5).wait_recv()
        copy(8).start()
    elif stage == 3:
        copy(6).wait_recv()
        copy(9).start()
    else:
        for k in (3, 7, 8, 9):
            copy(k).wait_recv()


GATHER_PLAN = {
    0: [(0, 0), (1, 0), (2, 0), (3, 0), (0, 1), (4, 0), (5, 0), (6, 0), (7, 0), (8, 0),
        (0, 2), (1, 1), (2, 1), (3, 1), (0, 3), (0, 4), (1, 2), (4, 1), (5, 1)],
    1: [(1, 3), (2, 2), (3, 2), (6, 1)],
    2: [(1, 4), (4, 2), (5, 2), (7, 1), (2, 3), (3, 3)],
    3: [(6, 2), (8, 1), (4, 3)],
    4: [(2, 4), (5, 3)],
    5: [(7, 2), (6, 3)],
    6: [(3, 4), (8, 2), (4, 4), (5, 4)],
    7: [(7, 3), (8, 3), (6, 4)],
    8: [(7, 4), (8, 4)],
}


def scatter_copy(at, grad, part, sums, boxes, send, recv, k):
    z, core = at["z"], at["core"]
    if k == 0:
        src, dst, device = grad.at[:, :, 1 - core], sums, {"fsdp": z * 2 + 1 - core}
    elif k == 1:
        src, dst, device = part.at[at["diag"]], boxes.at[0], {"dp": at["second"]}
    elif k == 2:
        src, dst, device = part.at[at["second"]], boxes.at[1], {"dp": at["second"]}
    elif k == 3:
        src, dst, device = part.at[at["first"]], boxes.at[2], {"dp": at["first"]}
    else:
        there = (z + k - 3) % 4
        src, dst, device = part.at[at["dp"], there], boxes.at[3, k - 4], {"fsdp": there * 2 + core}
    return pltpu.make_async_remote_copy(
        src_ref=src, dst_ref=dst, send_sem=send.at[k], recv_sem=recv.at[k],
        device_id=device, device_id_type=MESH,
    )


def direct_copy(at, part, boxes, send, recv, i):
    dp, z = (at["dp"] + i // 4) % 4, (at["z"] + i % 4) % 4
    return pltpu.make_async_remote_copy(
        src_ref=part.at[dp, z], dst_ref=boxes.at[i - 1], send_sem=send.at[i - 1], recv_sem=recv.at[i - 1],
        device_id={"dp": dp, "fsdp": z * 2 + at["core"]}, device_id_type=MESH,
    )


def all_devices(at):
    inner = at["z"] * 2 + at["core"]
    return [{"dp": (at["dp"] + i // 8) % 4, "fsdp": (inner + i % 8) % 8} for i in range(1, 32)]


def add_low(left, right):
    return left + right


def scatter_stage(at, copy, mine, part, sums, boxes, stage):
    dp = at["dp"]
    if stage == 0:
        copy(0).start()
    elif stage == 1:
        copy(0).wait_recv()
        for name in ("diag", "second", "first", "dp"):
            part[at[name]] = add_low(mine(at[name]), sums[at[name]])
            if name == "diag":
                copy(1).start()
            if name == "second":
                copy(2).start()
    elif stage == 2:
        copy(1).wait_recv()
        part[at["first"]] = add_low(part[at["first"]], boxes[0])
        copy(3).start()
    elif stage == 3:
        copy(2).wait_recv()
        part[dp] = add_low(part[dp], boxes[1])
        copy(3).wait_recv()
        part[dp] = add_low(part[dp], boxes[2])
        for k in (4, 5, 6):
            copy(k).start()
    else:
        for k in (4, 5, 6):
            copy(k).wait_recv()


def scatter_total(at, part, boxes):
    total = part[at["dp"], at["z"]].astype(f32)
    for i in range(3):
        total = total + boxes[3, i].astype(f32)
    return total


SCATTER_PLAN = {
    1: [(0, 0), (1, 0), (2, 0), (3, 0), (4, 0)],
    2: [(0, 1), (1, 1), (2, 1)],
    3: [(5, 1), (3, 1), (0, 2)],
    4: [(1, 2), (2, 2), (4, 1)],
    5: [(5, 2), (6, 1), (3, 2), (0, 3)],
    6: [(4, 2), (7, 1), (1, 3), (2, 3)],
    7: [(6, 2), (5, 3), (3, 3), (7, 2), (0, 4)],
}


def spread_projection(omega_ref, wide_ref):
    wide_ref[...] = jnp.zeros_like(wide_ref)
    wide_ref[:HD, :FEAT] = omega_ref[0]
    wide_ref[HD:, FEAT:] = omega_ref[1]


def ones_projection(omega_ref, wide_ref):
    wide_ref[...] = jnp.ones_like(wide_ref)
    for odd in range(2):
        wide_ref[odd, odd * HD : (odd + 1) * HD, :] = omega_ref[odd]


def forward_step(
    block, starts_ref, lens_ref, normed, weight, wide_ref,
    qkv_ref, fq_ref, fk_ref, o_ref, rden_ref, prefix_ref, state_ref,
):
    per_seg = SEG // BLOCK

    @pl.when(block % per_seg == 0)
    def _():
        begins = jnp.logical_or(block == 0, starts_ref[block // per_seg] != 0)
        state_ref[...] = jnp.where(begins, 0.0, state_ref[...])

    qkv_ref[0] = dot_nn(normed, weight).astype(bf16)
    position = lax.broadcasted_iota(jnp.int32, (BLOCK, 1), 0) + (block % per_seg) * BLOCK
    valid = (position < lens_ref[block // per_seg]).astype(f32)
    _, low = lane_masks(BLOCK)
    feats = []
    for part, feat_ref in enumerate((fq_ref, fk_ref)):
        rows = qkv_ref[0, :, part * DUO : (part + 1) * DUO]
        wide = rows.astype(f32)
        square = wide * wide
        proj = dot_nn(rows, wide_ref[...])
        for odd in range(2):
            total = jnp.sum(
                jnp.where(low, 0.0, square) if odd else jnp.where(low, square, 0.0), axis=-1, keepdims=True
            )
            value = jnp.exp2(
                proj[:, odd * FEAT : (odd + 1) * FEAT] * (feat_scale * log2_e)
                - total * (0.5 * feat_scale * feat_scale * log2_e)
            )
            if part:
                value = value * valid
            value = value.astype(bf16)
            feat_ref[0, :, odd * FEAT : (odd + 1) * FEAT] = value
            feats.append(value)
    _, low = lane_masks(TILE)
    causal, _ = causal_masks()
    cuts = [slice(tile * TILE, (tile + 1) * TILE) for tile in range(TILES_BLOCK)]
    values = qkv_ref[0, :, 2 * DUO :]
    ones = [with_ones(values[at], low) for at in cuts]
    turned = [[one.T for one in pair] for pair in ones]
    weights = [
        [
            jnp.where(causal, dot_nt(feats[odd][at], feats[2 + odd][at]), 0.0).astype(bf16)
            for odd in range(2)
        ]
        for at in cuts
    ]
    sums = [[dot_nn(turned[i][odd], feats[2 + odd][at]) for odd in range(2)] for i, at in enumerate(cuts)]
    states = [state_ref[odd] for odd in range(2)]
    for i, at in enumerate(cuts):
        mixed = []
        for odd in range(2):
            before_low = states[odd].astype(bf16)
            prefix_ref[0, i, odd] = before_low
            mixed.append(dot_nn(weights[i][odd], ones[i][odd]) + dot_nt(feats[odd][at], before_low))
            states[odd] = states[odd] + sums[i][odd]
        top = jnp.where(low, mixed[0], mixed[1])
        bottom = pltpu.roll(jnp.where(low, mixed[1], mixed[0]), HD, 1)
        o_ref[at, :] = (top / bottom).astype(bf16)
        rden_ref[0, at, :] = 1.0 / bottom
    for odd in range(2):
        state_ref[odd] = states[odd]


def block_rows(block):
    return pl.ds(pl.multiple_of(block * BLOCK, BLOCK), BLOCK)


def forward_local_kernel(
    starts_ref, lens_ref, x_ref, w_ref, gain_ref, omega_ref,
    qkv_ref, fq_ref, fk_ref, o_ref, rden_ref, prefix_ref, normed_ref, state_ref, wide_ref,
):
    pair, block = pl.program_id(0), pl.program_id(1)
    rows = block_rows(block)

    @pl.when(pair == 0)
    def _():
        unit, _ = normalise(x_ref[rows, :].astype(f32))
        normed_ref[rows, :] = (unit * gain_ref[0:1, :]).astype(bf16)

    @pl.when(block == 0)
    def _():
        spread_projection(omega_ref, wide_ref)

    forward_step(
        block, starts_ref, lens_ref, normed_ref[rows, :], w_ref[...], wide_ref,
        qkv_ref, fq_ref, fk_ref, o_ref, rden_ref, prefix_ref, state_ref,
    )


def forward_kernel(
    starts_ref, lens_ref, x_ref, omega_ref, wq_ref, wo_ref, wu_ref, wd_ref, gains_ref,
    qkv_ref, fq_ref, fk_ref, o_ref, rden_ref, prefix_ref, normed_ref, wpair_ref, gain_ref,
    fullo_ref, fullu_ref, fulld_ref,
    state_ref, wide_ref, rows_ref, unit_ref, head_ref, held_ref, heldo_ref, heldu_ref, heldd_ref, pad_ref,
    send, recv, local,
):
    pair, block = pl.program_id(0), pl.program_id(1)
    blocks = pl.num_programs(1)
    step = pair * blocks + block
    at = place()
    dp, z, core = at["dp"], at["z"], at["core"]
    full = [head_ref, held_ref.at[0], held_ref.at[1], held_ref.at[2], heldo_ref]
    full += [heldu_ref.at[0], heldu_ref.at[1], heldd_ref.at[0], heldd_ref.at[1]]
    own = [array.at[dp, z, core] for array in full]
    leave = [fullo_ref] + halves(fullu_ref, fulld_ref)
    partners = near_devices(at)

    def copy(w, k):
        return gather_copy(at, own[w], full[w], send.at[w], recv.at[w], k)

    def keep(w):
        return pltpu.make_async_copy(full[w], leave[w - 4], local.at[w])

    def fetch():
        return pltpu.make_async_copy(x_ref, rows_ref, local.at[0])

    def stages(plan):
        for w, stage in plan:
            gather_stage(functools.partial(copy, w), stage)
            if stage == 4 and w > 3:
                keep(w).start()

    @pl.when(step == 0)
    def _():
        greet(partners)
        fetch().start()
        pad_ref[...] = jnp.zeros_like(pad_ref)
        pad_ref[0:2, 0:16] = gains_ref[...]
        flat = pad_ref[...]
        turned = flat
        for i in range(1, 8):
            turned = jnp.where(at["flat"] % 8 == i, pltpu.roll(flat, 16 * i, 1), turned)
        row = lax.broadcasted_iota(jnp.int32, (16, EXTRA), 0)
        band = at["flat"] // 8
        placed = jnp.where(row == band, turned[0:1, :], 0.0) + jnp.where(row == band + 4, turned[1:2, :], 0.0)
        for part in range(3):
            for i in range(PAIRS):
                piece = wq_ref[:, part * D + i * DUO : part * D + (i + 1) * DUO].astype(bf16)
                if i == 0:
                    head_ref[dp, z, core, :, part * DUO : (part + 1) * DUO] = piece
                else:
                    held_ref[i - 1, dp, z, core, :, part * DUO : (part + 1) * DUO] = piece
        head_ref[dp, z, core, :, CHUNK:] = placed.astype(bf16)
        greeted(partners)
        stages(GATHER_PLAN[0][:4])
        heldo_ref[dp, z, core] = wo_ref[...].astype(bf16)
        for i in range(2):
            heldu_ref[i, dp, z, core] = wu_ref[:, i * (FF // 2) : (i + 1) * (FF // 2)].astype(bf16)
            heldd_ref[i, dp, z, core] = wd_ref[i * 32 : (i + 1) * 32, :].astype(bf16)
        stages(GATHER_PLAN[0][4:10])
        fetch().wait()

        @pl.loop(0, blocks)
        def _(i):
            unit_ref[block_rows(i), :] = normalise(rows_ref[block_rows(i), :].astype(f32))[0]

        stages(GATHER_PLAN[0][10:])
        packed = head_ref[..., CHUNK:].astype(f32)
        total = jnp.sum(packed.reshape(32, 16, EXTRA), axis=0)
        gain_ref[...] = jnp.zeros_like(gain_ref)
        for i in range(2):
            for j in range(4):
                gain_ref[i : i + 1, EXTRA * j : EXTRA * (j + 1)] = total[4 * i + j : 4 * i + j + 1, :]

    for when, plan in GATHER_PLAN.items():
        if 0 < when < 8:

            @pl.when(step == when)
            def _(plan=plan):
                stages(plan)

    rows = block_rows(block)

    @pl.when(pair == 0)
    def _():
        normed_ref[rows, :] = (unit_ref[rows, :] * gain_ref[0:1, :]).astype(bf16)

    for i in range(PAIRS):

        @pl.when(jnp.logical_and(block == 0, pair == i))
        def _(i=i):
            piece = held_ref[i - 1] if i else head_ref[..., :CHUNK]
            wpair_ref[...] = piece.reshape(D, CHUNK)

    @pl.when(block == 0)
    def _():
        spread_projection(omega_ref, wide_ref)

    forward_step(
        block, starts_ref, lens_ref, normed_ref[rows, :], wpair_ref[...], wide_ref,
        qkv_ref, fq_ref, fk_ref, o_ref, rden_ref, prefix_ref, state_ref,
    )

    @pl.when(step == PAIRS * blocks - 1)
    def _():
        stages(GATHER_PLAN[8])
        for w in range(4, 9):
            keep(w).wait()
        for w in range(9):
            for k in range(10):
                copy(w, k).wait_send()


def normal_parts(hidden):
    inner = 0.5 + 0.5 * lax.erf(hidden * (0.5**0.5))
    return inner, jnp.exp2(hidden * hidden * (-0.5 * log2_e)) * (1.0 / math.sqrt(2.0 * math.pi))


def feed_forward_kernel(
    block, chunk,
    lens_ref, x_ref, o_ref, cot_ref, wo_ref, wu_ref, wd_ref, gain_ref,
    out_ref, dmid_ref, do_ref, gwo_ref, gwu_ref, gwd_ref,
    awo_ref, awu_ref, awd_ref, norm_ref, normt_ref, dyt_ref, dy_ref, y_ref, dn_ref,
):
    step = pl.program_id(0)
    steps = pl.num_programs(0)

    @pl.when(step == 0)
    def _():
        awo_ref[...] = jnp.zeros_like(awo_ref)
        awu_ref[...] = jnp.zeros_like(awu_ref)
        awd_ref[...] = jnp.zeros_like(awd_ref)

    per_seg = SEG // block
    position = lax.broadcasted_iota(jnp.int32, (block, 1), 0) + (step % per_seg) * block
    valid = (position < lens_ref[step // per_seg]).astype(f32)
    dy = (cot_ref[...].astype(f32) * valid).astype(bf16)
    dy_ref[...] = dy
    dyt_ref[...] = dy.T
    gain = gain_ref[1:2, :]
    attended = o_ref[...]
    middle = x_ref[...].astype(f32) + dot_nn(attended, wo_ref[...])
    unit, inverse = normalise(middle)
    normed = (unit * gain).astype(bf16)
    norm_ref[...] = normed
    normt_ref[...] = normed.T
    y_ref[...] = middle
    dn_ref[...] = jnp.zeros_like(dn_ref)

    for index in range(FF // chunk):
        at = slice(index * chunk, (index + 1) * chunk)
        hidden = dot_nn(norm_ref[...], wu_ref[:, at])
        inner, bell = normal_parts(hidden)
        active = (hidden * inner).astype(bf16)
        slope = inner + hidden * bell
        y_ref[...] += dot_nn(active, wd_ref[at, :])
        grad_hidden = (slope * dot_nt(dy_ref[...], wd_ref[at, :])).astype(bf16)
        awd_ref[:, at] += dot_nn(dyt_ref[...], active)
        awu_ref[:, at] += dot_nn(normt_ref[...], grad_hidden)
        dn_ref[...] += dot_nt(grad_hidden, wu_ref[:, at])

    out_ref[...] = y_ref[...].astype(bf16)
    grad_middle = dy_ref[...].astype(f32) + normalise_back(dn_ref[...], gain, unit, inverse)
    dmid_ref[...] = grad_middle
    branch = grad_middle.astype(bf16)
    awo_ref[...] += dot_tn(attended, branch)
    do_ref[...] = dot_nt(branch, wo_ref[...])

    @pl.when(step == steps - 1)
    def _():
        gwo_ref[...] = awo_ref[...].astype(bf16)
        gwu_ref[...] = awu_ref[...].astype(bf16)
        gwd_ref[...] = awd_ref[...].astype(bf16).T


def backward_step(
    block, blocks, starts_ref, qkv_ref, fq_ref, fk_ref, o_ref, rden_ref, do_ref, prefix_ref, wide_ref,
    suffix_ref, store,
):
    per_seg = SEG // BLOCK

    @pl.when(block % per_seg == per_seg - 1)
    def _():
        after = jnp.minimum(block // per_seg + 1, blocks // per_seg - 1)
        ends = jnp.logical_or(block == blocks - 1, starts_ref[after] != 0)
        suffix_ref[...] = jnp.where(ends, 0.0, suffix_ref[...])

    lane, low = lane_masks(TILE)
    causal, anti = causal_masks()
    state_row = lax.broadcasted_iota(jnp.int32, (DUO, FEAT), 0)
    for tile in reversed(range(TILES_BLOCK)):
        at = slice(tile * TILE, (tile + 1) * TILE)
        scaled = do_ref[at, :] * rden_ref[0, at, :]
        product = scaled * o_ref[at, :].astype(f32)
        scaled = scaled.astype(bf16).astype(f32)
        ones = with_ones(qkv_ref[0, at, 2 * DUO :], low)
        back = [[], [], []]
        for odd in range(2):
            free = 0 if odd else HD
            mine = jnp.logical_not(low) if odd else low
            grad_den = -jnp.sum(jnp.where(mine, product, 0.0), axis=-1, keepdims=True)
            grad_one = jnp.where(mine, scaled, jnp.where(lane == free, grad_den, 0.0)).astype(bf16)
            query_feat = fq_ref[0, at, odd * FEAT : (odd + 1) * FEAT]
            key_feat = fk_ref[0, at, odd * FEAT : (odd + 1) * FEAT]
            one = ones[odd]
            after = suffix_ref[odd]
            edge = after[free : free + 1, :]
            rest = edge - edge.astype(bf16).astype(f32)
            after_low = jnp.where(state_row == free + 1, rest, after).astype(bf16)
            before_low = prefix_ref[0, tile, odd]
            weights_t = jnp.where(anti, dot_nt(key_feat, query_feat), 0.0).astype(bf16)
            grad_w = jnp.where(causal, dot_nt(grad_one, one), 0.0).astype(bf16)
            grad_wt = jnp.where(anti, dot_nt(one, grad_one), 0.0).astype(bf16)
            grad_fq = dot_nn(grad_w, key_feat) + dot_nn(grad_one, before_low)
            grad_fk = dot_nn(grad_wt, query_feat) + dot_nn(one, after_low)
            back[2].append(dot_nn(weights_t, grad_one) + dot_nt(key_feat, after_low))
            suffix_ref[odd] = after + dot_tn(grad_one, query_feat)
            grad_pq = (grad_fq * query_feat.astype(f32)).astype(bf16)
            grad_pk = (grad_fk * key_feat.astype(f32)).astype(bf16)
            back[0].append(dot_nt(grad_pq, wide_ref[odd]))
            back[1].append(dot_nt(grad_pk, wide_ref[odd]))
        for part in range(2):
            top = jnp.where(low, back[part][0], back[part][1])
            bottom = pltpu.roll(jnp.where(low, back[part][1], back[part][0]), HD, 1)
            values = qkv_ref[0, at, part * DUO : (part + 1) * DUO].astype(f32)
            store(tile, part, top * feat_scale - bottom * (feat_scale * feat_scale) * values)
        store(tile, 2, jnp.where(low, back[2][0], back[2][1]))


def pair_lanes(pair):
    return pl.ds(pl.multiple_of(pair * CHUNK, CHUNK), CHUNK)


def store_into(dqkv_ref, pair, block):
    def store(tile, part, value):
        rows = pl.ds(pl.multiple_of(block * BLOCK + tile * TILE, TILE), TILE)
        lanes = pl.ds(pl.multiple_of(pair * CHUNK + part * DUO, DUO), DUO)
        dqkv_ref[rows, lanes] = value.astype(bf16)

    return store


def input_gradient(i, x_ref, dqkv_ref, weight_ref, gain, dmid_ref):
    rows = pl.ds(pl.multiple_of(i * TILE, TILE), TILE)
    grad_normed = dot_nt(dqkv_ref[rows, :], weight_ref[...])
    unit, inverse = normalise(x_ref[rows, :].astype(f32))
    dmid_ref[rows, :] = dmid_ref[rows, :] + normalise_back(grad_normed, gain, unit, inverse)
    return rows


def backward_local_kernel(
    starts_ref, normed_ref, qkv_ref, fq_ref, fk_ref, o_ref, rden_ref, do_ref, prefix_ref, omega_ref, gain_ref,
    x_ref, dmid_in_ref, weight_ref,
    gin_ref, gw_ref,
    suffix_ref, wide_ref, dqkv_ref, turned_ref,
):
    pair, step = pl.program_id(0), pl.program_id(1)
    blocks = pl.num_programs(1)
    block = blocks - 1 - step

    @pl.when(step == 0)
    def _():
        ones_projection(omega_ref, wide_ref)

    @pl.when(pair == 0)
    def _():
        turned_ref[:, block_rows(block)] = normed_ref[...].T

    backward_step(
        block, blocks, starts_ref, qkv_ref, fq_ref, fk_ref, o_ref, rden_ref, do_ref, prefix_ref, wide_ref,
        suffix_ref, store_into(dqkv_ref, pair, block),
    )

    @pl.when(step == blocks - 1)
    def _():
        gw_ref[...] = dot_nn(turned_ref[...], dqkv_ref[:, pair_lanes(pair)]).astype(bf16)

    @pl.when(jnp.logical_and(step == blocks - 1, pair == PAIRS - 1))
    def _():
        gin_ref[...] = dmid_in_ref[...]

        @pl.loop(0, blocks * TILES_BLOCK)
        def _(i):
            input_gradient(i, x_ref, dqkv_ref, weight_ref, gain_ref[0:1, :], gin_ref)


def eye_row(column):
    row = lax.broadcasted_iota(jnp.int32, (16, 16), 0)
    lane = lax.broadcasted_iota(jnp.int32, (16, 16), 1)
    return jnp.sum(jnp.where(row == lane, column, 0.0), axis=0, keepdims=True)


def row_squares(value):
    return jnp.sum(value * value, axis=-1, keepdims=True).sum(axis=0, keepdims=True)


def backward_kernel(
    starts_ref, normed_ref, qkv_ref, fq_ref, fk_ref, o_ref, rden_ref, do_ref, prefix_ref, omega_ref, gain_ref,
    wq_ref, wu_ref, own_gain_ref, x_ref, dmid_ref, weight_ref, go_ref, gu_ref, gd_ref,
    gin_ref, ro_ref, ru_ref, rd_ref, rq_ref, rg_ref, norm_ref,
    suffix_ref, wide_ref, dqkv_ref, turned_ref, gq_ref,
    rows_ref, mid_ref, held_ref,
    po_ref, pu_ref, pd_ref, pq_ref, so_ref, su_ref, sd_ref, sq_ref, bo_ref, bu_ref, bd_ref, bq_ref,
    last_ref, near_ref, send, recv, local, out_sem, last_send, last_recv, near_send, near_recv,
):
    pair, inner_step = pl.program_id(0), pl.program_id(1)
    blocks = pl.num_programs(1)
    block = blocks - 1 - inner_step
    step = pair * blocks + inner_step
    at = place()
    dp, z, core = at["dp"], at["z"], at["core"]
    grads = [go_ref] + halves(gu_ref, gd_ref) + [gq_ref.at[i] for i in range(PAIRS)]

    def each(out, up, down, pairs):
        return [out, up.at[0], up.at[1], down.at[0], down.at[1]] + [pairs.at[i] for i in range(PAIRS)]

    parts = each(po_ref, pu_ref, pd_ref, pq_ref)
    sums = each(so_ref, su_ref, sd_ref, sq_ref)
    boxes = each(bo_ref, bu_ref, bd_ref, bq_ref)
    results = [ro_ref, ru_ref.at[:, : FF // 2], ru_ref.at[:, FF // 2 :], rd_ref.at[:32], rd_ref.at[32:]]
    results += [rq_ref.at[i] for i in range(PAIRS)]
    others = all_devices(at)

    def copy(w, k):
        return scatter_copy(at, grads[w], parts[w], sums[w], boxes[w], send.at[w], recv.at[w], k)

    def keep(w):
        return pltpu.make_async_copy(grads[w].at[:, :, core], parts[w], local.at[w])

    def late(i):
        src = (x_ref, dmid_ref, weight_ref)[i]
        dst = (rows_ref, mid_ref, held_ref)[i]
        return pltpu.make_async_copy(src, dst, local.at[5 + i])

    def stages(plan):
        for w, stage in plan:
            if w < 5:
                if stage == 0:
                    keep(w).start()
                if stage == 1:
                    keep(w).wait()
                mine = lambda index, w=w: parts[w][index]
            else:
                mine = lambda index, w=w: gq_ref[w - 5, index, :, core]
            scatter_stage(at, functools.partial(copy, w), mine, parts[w], sums[w], boxes[w], stage)
            if stage == 4:
                results[w][...] = scatter_total(at, parts[w], boxes[w])

    @pl.when(step == 0)
    def _():
        greet(others)
        for i in range(3):
            late(i).start()

    @pl.when(step == 1)
    def _():
        greeted(others)

    for when, plan in SCATTER_PLAN.items():

        @pl.when(step == when)
        def _(plan=plan):
            stages(plan)

    @pl.when(inner_step == 0)
    def _():
        ones_projection(omega_ref, wide_ref)

    @pl.when(pair == 0)
    def _():
        turned_ref[:, block_rows(block)] = normed_ref[...].T

    backward_step(
        block, blocks, starts_ref, qkv_ref, fq_ref, fk_ref, o_ref, rden_ref, do_ref, prefix_ref, wide_ref,
        suffix_ref, store_into(dqkv_ref, pair, block),
    )

    for i in range(PAIRS):

        @pl.when(step == (i + 1) * blocks - 1)
        def _(i=i):
            grad = dot_nn(turned_ref[...], dqkv_ref[:, i * CHUNK : (i + 1) * CHUNK]).astype(bf16)
            gq_ref[i] = grad.reshape(4, 4, 2, 16, CHUNK)
            stages([(5 + i, 0)])

    @pl.when(step == PAIRS * blocks - 1)
    def _():
        for i in range(3):
            late(i).wait()
        tiles = blocks * TILES_BLOCK

        def inputs_part(first, last):
            @pl.loop(first * tiles // 8, last * tiles // 8)
            def _(i):
                rows = input_gradient(i, rows_ref, dqkv_ref, held_ref, gain_ref[0:1, :], mid_ref)
                pltpu.make_async_copy(mid_ref.at[rows], gin_ref.at[rows], out_sem.at[i]).start()

        def last(i):
            return direct_copy(at, parts[8], last_ref, last_send, last_recv, i)

        stages([(4, 3), (6, 3), (7, 3)])
        inputs_part(0, 1)
        copy(8, 0).wait_recv()
        for i in range(4):
            index = (dp + i) % 4
            parts[8][index] = add_low(gq_ref[3, index, :, core], sums[8][index])
            for j in range(4):
                if i + j:
                    last(4 * i + j).start()
        inputs_part(1, 5)
        stages([(1, 4), (2, 4), (3, 4), (5, 4), (4, 4), (6, 4), (7, 4)])
        inputs_part(5, 8)
        early = row_squares(ro_ref[...]) + row_squares(ru_ref[...]) + row_squares(rd_ref[...])
        for i in range(PAIRS - 1):
            early = early + row_squares(rq_ref[i])
        up_low = wu_ref[...].astype(bf16).astype(f32)
        gain_low = own_gain_ref[...].astype(bf16).astype(f32)
        second = eye_row(jnp.sum(ru_ref[...] * up_low, axis=-1, keepdims=True)) / gain_low[1:2, :]
        total = parts[8][dp, z].astype(f32)
        for i in range(1, 16):
            last(i).wait_recv()
            total = total + last_ref[i - 1].astype(f32)
        rq_ref[3] = total
        first = jnp.zeros((16, 1), f32)
        for i in range(PAIRS):
            for part in range(3):
                low_w = wq_ref[:, part * D + i * DUO : part * D + (i + 1) * DUO].astype(bf16).astype(f32)
                first = first + jnp.sum(
                    rq_ref[i, :, part * DUO : (part + 1) * DUO] * low_w, axis=-1, keepdims=True
                )
        first = eye_row(first) / gain_low[0:1, :]
        rg_ref[0:1, :] = first
        rg_ref[1:2, :] = second
        squares = early + row_squares(rq_ref[PAIRS - 1]) + row_squares(first) + row_squares(second)
        mine = near_ref.at[at["flat"]]
        mine[...] = jnp.broadcast_to(squares, (8, 128))

        def near(i):
            return pltpu.make_async_remote_copy(
                src_ref=mine, dst_ref=mine, send_sem=near_send.at[i], recv_sem=near_recv.at[i],
                device_id=others[i], device_id_type=MESH,
            )

        for i in range(31):
            near(i).start()
        for i in range(31):
            near(i).wait_recv()
        group = near_ref[0]
        for i in range(1, 32):
            group = group + near_ref[i]
        norm_ref[...] = group

        @pl.loop(0, tiles)
        def _(i):
            rows = pl.ds(pl.multiple_of(i * TILE, TILE), TILE)
            pltpu.make_async_copy(mid_ref.at[rows], gin_ref.at[rows], out_sem.at[i]).wait()

        for i in range(31):
            near(i).wait_send()
        for i in range(1, 16):
            last(i).wait_send()
        copy(8, 0).wait_send()
        for w in range(8):
            for k in range(7):
                copy(w, k).wait_send()


def update_kernel(
    count_ref, total_ref, rq_ref, ro_ref, ru_ref, rd_ref, rg_ref,
    wq_ref, wo_ref, wu_ref, wd_ref, wg_ref, mq_ref, mo_ref, mu_ref, md_ref, mg_ref,
    vq_ref, vo_ref, vu_ref, vd_ref, vg_ref, gin_ref,
    norm_ref, gq_ref, nvq_ref, nwq_ref, go_ref, nvo_ref, nwo_ref, gu_ref, nvu_ref, nwu_ref,
    gd_ref, nvd_ref, nwd_ref, gg_ref, nvg_ref, nwg_ref, gin_out_ref,
):
    gin_out_ref[...] = gin_ref[...]

    @pl.when(pl.program_id(0) == 0)
    def _():
        update_weights(
            count_ref, total_ref, rq_ref, ro_ref, ru_ref, rd_ref, rg_ref,
            wq_ref, wo_ref, wu_ref, wd_ref, wg_ref, mq_ref, mo_ref, mu_ref, md_ref, mg_ref,
            vq_ref, vo_ref, vu_ref, vd_ref, vg_ref,
            norm_ref, gq_ref, nvq_ref, nwq_ref, go_ref, nvo_ref, nwo_ref, gu_ref, nvu_ref, nwu_ref,
            gd_ref, nvd_ref, nwd_ref, gg_ref, nvg_ref, nwg_ref,
        )


def update_weights(
    count_ref, total_ref, rq_ref, ro_ref, ru_ref, rd_ref, rg_ref,
    wq_ref, wo_ref, wu_ref, wd_ref, wg_ref, mq_ref, mo_ref, mu_ref, md_ref, mg_ref,
    vq_ref, vo_ref, vu_ref, vd_ref, vg_ref,
    norm_ref, gq_ref, nvq_ref, nwq_ref, go_ref, nvo_ref, nwo_ref, gu_ref, nvu_ref, nwu_ref,
    gd_ref, nvd_ref, nwd_ref, gg_ref, nvg_ref, nwg_ref,
):
    norm = jnp.sqrt(total_ref[0:1, 0:1])
    norm_ref[...] = norm
    factor = jnp.minimum(1.0, clip_level / norm)
    count = jnp.full((1, 1), count_ref[0], jnp.int32).astype(f32)
    first_fix = 1.0 - jnp.exp2(count * math.log2(beta_first))
    second_fix = 1.0 - jnp.exp2(count * math.log2(beta_second))

    def update(grad, at, weight, first, second, rate, outs):
        clipped = grad * factor
        first_new = beta_first * first[at] + (1.0 - beta_first) * clipped
        second_new = beta_second * second[at] + (1.0 - beta_second) * clipped * clipped
        direction = first_new / first_fix / (jnp.sqrt(second_new / second_fix) + adam_eps)
        outs[0][at] = clipped
        outs[1][at] = second_new
        outs[2][at] = weight[at] - rate * (direction + decay_weight * weight[at])

    for part in range(3):
        for i in range(PAIRS):
            at = (slice(None), slice(part * D + i * DUO, part * D + (i + 1) * DUO))
            grad = rq_ref[i, :, part * DUO : (part + 1) * DUO]
            update(grad, at, wq_ref, mq_ref, vq_ref, rate_matrix, (gq_ref, nvq_ref, nwq_ref))
    update(ro_ref[...], ..., wo_ref, mo_ref, vo_ref, rate_matrix, (go_ref, nvo_ref, nwo_ref))
    update(ru_ref[...], ..., wu_ref, mu_ref, vu_ref, rate_matrix, (gu_ref, nvu_ref, nwu_ref))
    update(rd_ref[...], ..., wd_ref, md_ref, vd_ref, rate_matrix, (gd_ref, nvd_ref, nwd_ref))
    update(rg_ref[...], ..., wg_ref, mg_ref, vg_ref, rate_gain, (gg_ref, nvg_ref, nwg_ref))


ROWS = {"pair": 16, "out": 16, "up": 16, "down": 64}
COLS = {"pair": CHUNK, "out": D, "up": FF, "down": D}
LATE = ("out", "up", "down")
smem = pl.BlockSpec(memory_space=pltpu.SMEM)
hbm = pl.BlockSpec(memory_space=pl.ANY)
vmem = pl.BlockSpec(memory_space=pltpu.VMEM)


def shaped(shape, dtype):
    return jax.ShapeDtypeStruct(shape, dtype)


def params(collective_id=None):
    if collective_id is None:
        return pltpu.CompilerParams(vmem_limit_bytes=VMEM_LIMIT)
    return pltpu.CompilerParams(vmem_limit_bytes=VMEM_LIMIT, collective_id=collective_id, has_side_effects=True)


def whole(shape):
    return pl.BlockSpec(shape, lambda *_: (0,) * len(shape), pipeline_mode=pl.Buffered(1))


def whole_out(shape):
    return pl.BlockSpec(shape, lambda *_: (0,) * len(shape))


def five(name):
    return (4, 4, 2, ROWS[name], COLS[name])


def forward_outs(tokens):
    tiles = tokens // TILE
    specs = [
        pl.BlockSpec((1, BLOCK, CHUNK), lambda p, b: (p, b, 0)),
        pl.BlockSpec((1, BLOCK, 2 * FEAT), lambda p, b: (p, b, 0)),
        pl.BlockSpec((1, BLOCK, 2 * FEAT), lambda p, b: (p, b, 0)),
        pl.BlockSpec((BLOCK, DUO), lambda p, b: (b, p)),
        pl.BlockSpec((1, BLOCK, DUO), lambda p, b: (p, b, 0)),
        pl.BlockSpec((1, TILES_BLOCK, 2, DUO, FEAT), lambda p, b: (p, b, 0, 0, 0)),
        whole_out((tokens, D)),
    ]
    shapes = [
        shaped((PAIRS, tokens, CHUNK), bf16),
        shaped((PAIRS, tokens, 2 * FEAT), bf16),
        shaped((PAIRS, tokens, 2 * FEAT), bf16),
        shaped((tokens, D), bf16),
        shaped((PAIRS, tokens, DUO), f32),
        shaped((PAIRS, tiles, 2, DUO, FEAT), bf16),
        shaped((tokens, D), bf16),
    ]
    scratch = [pltpu.VMEM((2, DUO, FEAT), f32), pltpu.VMEM((DUO, 2 * FEAT), bf16)]
    return specs, shapes, scratch


pair_omega = pl.BlockSpec((2, HD, FEAT), lambda p, b: (p, 0, 0))
pair_weight = pl.BlockSpec((D, CHUNK), lambda p, b: (0, p))


def forward_local(starts, lens, x, weight, gains, omega):
    tokens = x.shape[0]
    specs, shapes, scratch = forward_outs(tokens)
    return pl.pallas_call(
        forward_local_kernel,
        grid=(PAIRS, tokens // BLOCK),
        in_specs=[smem, smem, whole((tokens, D)), pair_weight, whole((8, D)), pair_omega],
        out_specs=specs,
        out_shape=shapes,
        scratch_shapes=scratch,
        compiler_params=params(),
    )(starts, lens, x, weight, gains, omega)


def forward(starts, lens, x, omega, wq, wo, wu, wd, gains):
    tokens = x.shape[0]
    specs, shapes, scratch = forward_outs(tokens)
    return pl.pallas_call(
        forward_kernel,
        grid=(PAIRS, tokens // BLOCK),
        in_specs=[smem, smem, hbm, pair_omega] + [whole(array.shape) for array in (wq, wo, wu, wd, gains)],
        out_specs=specs + [pair_weight, whole_out((8, D)), hbm, hbm, hbm],
        out_shape=shapes + [shaped((D, WIDE), bf16), shaped((8, D), f32)]
        + [shaped(five(name), bf16) for name in LATE],
        scratch_shapes=scratch
        + [
            pltpu.VMEM((tokens, D), bf16),
            pltpu.VMEM((tokens, D), f32),
            pltpu.VMEM((4, 4, 2, 16, CHUNK + EXTRA), bf16),
            pltpu.VMEM((PAIRS - 1, *five("pair")), bf16),
        ]
        + [
            pltpu.VMEM(five("out"), bf16),
            pltpu.VMEM((2, 4, 4, 2, 16, FF // 2), bf16),
            pltpu.VMEM((2, 4, 4, 2, 32, D), bf16),
            pltpu.VMEM((8, EXTRA), f32),
            pltpu.SemaphoreType.DMA((9, 10)),
            pltpu.SemaphoreType.DMA((9, 10)),
            pltpu.SemaphoreType.DMA((9,)),
        ],
        compiler_params=params(0),
    )(starts, lens, x, omega, wq, wo, wu, wd, gains)


def feed_forward(lens, x, o, cot, wo, wu, wd, gains, block=512, chunk=512):
    tokens = x.shape[0]
    rows = pl.BlockSpec((block, D), lambda i: (i, 0))
    return pl.pallas_call(
        functools.partial(feed_forward_kernel, block, chunk),
        grid=(tokens // block,),
        in_specs=[smem, rows, rows, rows, whole((D, D)), whole((D, FF)), whole((FF, D)), whole((8, D))],
        out_specs=[rows, rows, rows, whole_out((D, D)), whole_out((D, FF)), whole_out((FF, D))],
        out_shape=[
            shaped((tokens, D), bf16),
            shaped((tokens, D), f32),
            shaped((tokens, D), f32),
            shaped((D, D), bf16),
            shaped((D, FF), bf16),
            shaped((FF, D), bf16),
        ],
        scratch_shapes=[
            pltpu.VMEM((D, D), f32), pltpu.VMEM((D, FF), f32), pltpu.VMEM((D, FF), f32),
            pltpu.VMEM((block, D), bf16), pltpu.VMEM((D, block), bf16), pltpu.VMEM((D, block), bf16),
            pltpu.VMEM((block, D), bf16), pltpu.VMEM((block, D), f32), pltpu.VMEM((block, D), f32),
        ],
        compiler_params=params(),
    )(lens, x, o, cot, wo, wu, wd, gains)


def backward_ins(blocks):
    last = blocks - 1
    return [
        smem,
        pl.BlockSpec((BLOCK, D), lambda p, b: (jnp.where(p == 0, last - b, 0), 0)),
        pl.BlockSpec((1, BLOCK, CHUNK), lambda p, b: (p, last - b, 0)),
        pl.BlockSpec((1, BLOCK, 2 * FEAT), lambda p, b: (p, last - b, 0)),
        pl.BlockSpec((1, BLOCK, 2 * FEAT), lambda p, b: (p, last - b, 0)),
        pl.BlockSpec((BLOCK, DUO), lambda p, b: (last - b, p)),
        pl.BlockSpec((1, BLOCK, DUO), lambda p, b: (p, last - b, 0)),
        pl.BlockSpec((BLOCK, DUO), lambda p, b: (last - b, p)),
        pl.BlockSpec((1, TILES_BLOCK, 2, DUO, FEAT), lambda p, b: (p, last - b, 0, 0, 0)),
        pair_omega,
        whole((8, D)),
    ]


def backward_scratch(tokens):
    return [
        pltpu.VMEM((2, DUO, FEAT), f32),
        pltpu.VMEM((2, DUO, FEAT), bf16),
        pltpu.VMEM((tokens, WIDE), bf16),
        pltpu.VMEM((D, tokens), bf16),
    ]


def backward_local(args, x, dmid, weight):
    tokens = x.shape[0]
    return pl.pallas_call(
        backward_local_kernel,
        grid=(PAIRS, tokens // BLOCK),
        in_specs=backward_ins(tokens // BLOCK) + [whole((tokens, D)), whole((tokens, D)), whole((D, WIDE))],
        out_specs=[whole_out((tokens, D)), pair_weight],
        out_shape=[shaped((tokens, D), f32), shaped((D, WIDE), bf16)],
        scratch_shapes=backward_scratch(tokens),
        compiler_params=params(),
    )(*args, x, dmid, weight)


def backward(args, wq, wu, gains, x, dmid, weight, grads):
    tokens = x.shape[0]
    half = [(4, 4, 16, D), (2, 4, 4, 16, FF // 2), (2, 4, 4, 32, D), (PAIRS, 4, 4, 16, CHUNK)]
    grads = [grad.reshape(five(name)) for grad, name in zip(grads, LATE)]
    dma = pltpu.SemaphoreType.DMA
    return pl.pallas_call(
        backward_kernel,
        grid=(PAIRS, tokens // BLOCK),
        in_specs=backward_ins(tokens // BLOCK) + [whole(wq.shape), whole(wu.shape), whole(gains.shape)] + [hbm] * 6,
        out_specs=[hbm]
        + [whole_out((ROWS[name], COLS[name])) for name in LATE]
        + [whole_out((PAIRS, 16, CHUNK)), whole_out((2, 16)), whole_out((8, 128))],
        out_shape=[shaped((tokens, D), f32)]
        + [shaped((ROWS[name], COLS[name]), f32) for name in LATE]
        + [shaped((PAIRS, 16, CHUNK), f32), shaped((2, 16), f32), shaped((8, 128), f32)],
        scratch_shapes=backward_scratch(tokens)
        + [pltpu.VMEM((PAIRS, *five("pair")), bf16)]
        + [pltpu.VMEM((tokens, D), bf16), pltpu.VMEM((tokens, D), f32), pltpu.VMEM((D, WIDE), bf16)]
        + [pltpu.VMEM(shape, bf16) for shape in half] * 3
        + [pltpu.VMEM((15, 16, CHUNK), bf16), pltpu.VMEM((32, 8, 128), f32)]
        + [dma((9, 7)), dma((9, 7)), dma((8,)), dma((tokens // TILE,)), dma((15,)), dma((15,)), dma((31,)), dma((31,))],
        compiler_params=params(1),
    )(*args, wq, wu, gains, x, dmid, weight, *grads)


def update_all(count, total, grads, weights, firsts, seconds, grad_inputs):
    shapes = [shaped((1, 1), f32)]
    for weight in weights:
        shapes += [shaped(weight.shape, f32)] * 3
    arrays = (total, *grads, *weights, *firsts, *seconds)
    rows = pl.BlockSpec((UPDATE_ROWS, D), lambda i: (i, 0))
    return pl.pallas_call(
        update_kernel,
        grid=(grad_inputs.shape[0] // UPDATE_ROWS,),
        in_specs=[smem] + [whole(array.shape) for array in arrays] + [rows],
        out_specs=[whole_out(shape.shape) for shape in shapes] + [rows],
        out_shape=shapes + [shaped(grad_inputs.shape, f32)],
        compiler_params=params(),
    )(count.reshape(1), *arrays, grad_inputs)


def to_pairs(weight):
    split = weight.reshape(weight.shape[0], 3, PAIRS, DUO)
    return jnp.swapaxes(split, 1, 2).reshape(weight.shape)


def from_pairs(weight):
    split = weight.reshape(weight.shape[0], PAIRS, 3, DUO)
    return jnp.swapaxes(split, 1, 2).reshape(weight.shape)


def on_device(
    sizes, inputs, cotangent, feature_omega, seg_start, seg_len, step_count,
    w_qkv, w_out, w_up, w_down, gains,
    m_qkv, m_out, m_up, m_down, m_gains,
    v_qkv, v_out, v_up, v_down, v_gains,
):
    weights = (w_qkv, w_out, w_up, w_down, gains)
    firsts = (m_qkv, m_out, m_up, m_down, m_gains)
    seconds = (v_qkv, v_out, v_up, v_down, v_gains)
    if sizes == (4, 8):
        (qkv, fq, fk, attended, rden, prefix, normed, qkv_full, gain_full, out_full, up_full, down_full) = forward(
            seg_start, seg_len, inputs, feature_omega, *weights
        )
        out_rows, dmid, grad_attended, grad_out, grad_up, grad_down = feed_forward(
            seg_len, inputs, attended, cotangent, out_full.reshape(D, D), up_full.reshape(D, FF),
            down_full.reshape(FF, D), gain_full,
        )
        grad_inputs, r_out, r_up, r_down, r_qkv, r_gains, total = backward(
            (seg_start, normed, qkv, fq, fk, attended, rden, grad_attended, prefix, feature_omega, gain_full),
            w_qkv, w_up, gains, inputs, dmid, qkv_full, (grad_out, grad_up, grad_down),
        )
        norm, *updated, grad_inputs = update_all(
            step_count, total, (r_qkv, r_out, r_up, r_down, r_gains), weights, firsts, seconds, grad_inputs
        )
        return (out_rows, grad_inputs, norm.reshape(()), *updated)

    def gather(piece, axis=0):
        return lax.all_gather(piece.astype(bf16), AXES, axis=axis, tiled=True)

    qkv_full, out_full, up_full, down_full = (gather(piece) for piece in weights[:4])
    qkv_full = to_pairs(qkv_full)
    gain_full = jnp.pad(gather(gains, 1).astype(f32), ((0, 6), (0, 0)))
    qkv, fq, fk, attended, rden, prefix, normed = forward_local(
        seg_start, seg_len, inputs, qkv_full, gain_full, feature_omega
    )
    out_rows, dmid, grad_attended, grad_out, grad_up, grad_down = feed_forward(
        seg_len, inputs, attended, cotangent, out_full, up_full, down_full, gain_full
    )
    grad_inputs, grad_qkv = backward_local(
        (seg_start, normed, qkv, fq, fk, attended, rden, grad_attended, prefix, feature_omega, gain_full),
        inputs, dmid, qkv_full,
    )

    def scatter(piece):
        return lax.psum_scatter(piece.astype(f32), AXES, scatter_dimension=0, tiled=True)

    reduced = [scatter(piece) for piece in (from_pairs(grad_qkv), grad_out, grad_up, grad_down)]
    low = [weight.astype(bf16).astype(f32) for weight in weights]
    first = jnp.sum(reduced[0] * low[0], axis=1) / low[4][0]
    second = jnp.sum(reduced[2] * low[2], axis=1) / low[4][1]
    reduced.append(jnp.stack([first, second], axis=0))
    grad_norm = jnp.sqrt(lax.psum(sum(jnp.sum(piece * piece) for piece in reduced), AXES))
    factor = jnp.minimum(1.0, clip_level / grad_norm)
    count = step_count.astype(f32)
    first_fix = 1.0 - jnp.power(beta_first, count)
    second_fix = 1.0 - jnp.power(beta_second, count)
    updated = []
    rates = (rate_matrix,) * 4 + (rate_gain,)
    for weight, first, second, gradient, rate in zip(weights, firsts, seconds, reduced, rates):
        clipped = gradient * factor
        first_new = beta_first * first + (1.0 - beta_first) * clipped
        second_new = beta_second * second + (1.0 - beta_second) * clipped * clipped
        direction = first_new / first_fix / (jnp.sqrt(second_new / second_fix) + adam_eps)
        updated += [clipped, second_new, weight - rate * (direction + decay_weight * weight)]
    return (out_rows, grad_inputs, grad_norm, *updated)


def solution(mesh):
    return jax.shard_map(
        functools.partial(on_device, tuple(mesh.shape[name] for name in AXES)),
        mesh=mesh,
        in_specs=(
            P(("dp", "fsdp"), None),
            P(("dp", "fsdp"), None),
            P(),
            P(("dp", "fsdp")),
            P(("dp", "fsdp")),
            P(),
            P(("dp", "fsdp"), None),
            P(("dp", "fsdp"), None),
            P(("dp", "fsdp"), None),
            P(("dp", "fsdp"), None),
            P(None, ("dp", "fsdp")),
            P(("dp", "fsdp"), None),
            P(("dp", "fsdp"), None),
            P(("dp", "fsdp"), None),
            P(("dp", "fsdp"), None),
            P(None, ("dp", "fsdp")),
            P(("dp", "fsdp"), None),
            P(("dp", "fsdp"), None),
            P(("dp", "fsdp"), None),
            P(("dp", "fsdp"), None),
            P(None, ("dp", "fsdp")),
        ),
        out_specs=(
            P(("dp", "fsdp"), None),
            P(("dp", "fsdp"), None),
            P(),
            P(("dp", "fsdp"), None),
            P(("dp", "fsdp"), None),
            P(("dp", "fsdp"), None),
            P(("dp", "fsdp"), None),
            P(("dp", "fsdp"), None),
            P(("dp", "fsdp"), None),
            P(("dp", "fsdp"), None),
            P(("dp", "fsdp"), None),
            P(("dp", "fsdp"), None),
            P(("dp", "fsdp"), None),
            P(("dp", "fsdp"), None),
            P(("dp", "fsdp"), None),
            P(None, ("dp", "fsdp")),
            P(None, ("dp", "fsdp")),
            P(None, ("dp", "fsdp")),
        ),
        check_vma=False,
    )
```

```python
import functools
import math

import jax
import jax.numpy as jnp
from jax import lax
from jax.experimental import pallas as pl
from jax.experimental.pallas import tpu as pltpu
from jax.sharding import PartitionSpec as P

D = 512
HEADS = 8
HD = 64
FEAT = 256
FF = 2048
SEG = 1024
TILE = 256
PAIRS = HEADS // 2
DUO = 2 * HD
BLOCK = 1024
TILES_BLOCK = BLOCK // TILE
FORWARD_MIB = 60
BACKWARD_MIB = 52
UPDATE_MIB = 20
FF_BLOCK = 512
FF_CHUNK = 512
WIDE = 3 * D
CHUNK = 3 * DUO
EXTRA = 128
AXES = ("dp", "fsdp")

norm_eps = 1e-05
clip_level = 1.0
rate_matrix = 0.03
rate_gain = 0.4
beta_first = 0.9
beta_second = 0.95
adam_eps = 1e-08
decay_weight = 0.1

feat_scale = HD ** (-0.25)
log2_e = math.log2(math.e)
f32 = jnp.float32
bf16 = jnp.bfloat16
MESH = pl.DeviceIdType.MESH


def dot_nn(a, b):
    return lax.dot_general(a, b, (((1,), (0,)), ((), ())), preferred_element_type=f32)


def dot_nt(a, b):
    return lax.dot_general(a, b, (((1,), (1,)), ((), ())), preferred_element_type=f32)


def dot_tn(a, b):
    return lax.dot_general(a, b, (((0,), (0,)), ((), ())), preferred_element_type=f32)


def normalise(rows):
    centred = rows - jnp.mean(rows, axis=-1, keepdims=True)
    spread = jnp.mean(centred * centred, axis=-1, keepdims=True)
    inverse = lax.rsqrt(spread + norm_eps)
    return centred * inverse, inverse


def normalise_back(grad, gain, unit, inverse):
    scaled = grad * gain
    first = jnp.mean(scaled, axis=-1, keepdims=True)
    second = jnp.mean(scaled * unit, axis=-1, keepdims=True)
    return inverse * (scaled - first - unit * second)


def lane_masks(rows):
    lane = lax.broadcasted_iota(jnp.int32, (rows, DUO), 1)
    return lane, lane < HD


def causal_masks():
    row = lax.broadcasted_iota(jnp.int32, (TILE, TILE), 0)
    col = lax.broadcasted_iota(jnp.int32, (TILE, TILE), 1)
    return row >= col, row <= col


def with_ones(value_pair, low):
    wide = value_pair.astype(f32)
    return (
        jnp.where(low, wide, 1.0).astype(bf16),
        jnp.where(low, 1.0, wide).astype(bf16),
    )


def place():
    dp, inner = lax.axis_index("dp"), lax.axis_index("fsdp")
    z, core = inner // 2, inner % 2
    y, x = dp // 2, dp % 2
    across = y * 2 + (1 - x)
    along = (1 - y) * 2 + x
    return {
        "dp": dp, "z": z, "core": core, "flat": dp * 8 + inner,
        "first": core * along + (1 - core) * across,
        "second": core * across + (1 - core) * along,
        "diag": (1 - y) * 2 + (1 - x),
    }


def greet(devices):
    barrier = pltpu.get_barrier_semaphore()
    for device in devices:
        pl.semaphore_signal(barrier, inc=1, device_id=device, device_id_type=MESH)


def greeted(devices):
    pl.semaphore_wait(pltpu.get_barrier_semaphore(), len(devices))


def near_devices(at):
    devices = [{"fsdp": (at["z"] + i) % 4 * 2 + at["core"]} for i in range(1, 4)]
    devices += [{"fsdp": at["z"] * 2 + 1 - at["core"]}]
    devices += [{"dp": at["first"]}, {"dp": at["second"]}]
    return devices


def halves(up, down):
    return [up.at[..., i * (FF // 2) : (i + 1) * (FF // 2)] for i in range(2)] + [
        down.at[:, :, :, i * 32 : (i + 1) * 32, :] for i in range(2)
    ]


def gather_copy(at, own, full, send, recv, k):
    dp, z, core = at["dp"], at["z"], at["core"]
    sibling = {"fsdp": z * 2 + 1 - core}
    if k < 3:
        src, dst, device = own, full.at[dp, z, core], {"fsdp": (z + 1 + k) % 4 * 2 + core}
    else:
        which = {3: "dp", 4: "dp", 5: "dp", 6: "first", 7: "first", 8: "second", 9: "diag"}[k]
        src = dst = full.at[at[which], :, core]
        device = {4: {"dp": at["first"]}, 5: {"dp": at["second"]}, 6: {"dp": at["second"]}}.get(k, sibling)
    return pltpu.make_async_remote_copy(
        src_ref=src, dst_ref=dst, send_sem=send.at[k], recv_sem=recv.at[k],
        device_id=device, device_id_type=MESH,
    )


def gather_stage(copy, stage):
    if stage == 0:
        for k in range(3):
            copy(k).start()
    elif stage == 1:
        for k in range(3):
            copy(k).wait_recv()
        for k in (4, 5, 3):
            copy(k).start()
    elif stage == 2:
        copy(4).wait_recv()
        copy(6).start()
        copy(7).start()
        copy(5).wait_recv()
        copy(8).start()
    elif stage == 3:
        copy(6).wait_recv()
        copy(9).start()
    else:
        for k in (3, 7, 8, 9):
            copy(k).wait_recv()


GATHER_PLAN = {
    0: [(0, 0), (1, 0), (2, 0), (3, 0), (0, 1), (5, 0), (6, 0), (7, 0), (8, 0), (4, 0),
        (0, 2), (1, 1), (2, 1), (3, 1), (0, 3), (0, 4), (1, 2), (5, 1)],
    1: [(6, 1), (1, 3), (2, 2), (3, 2)],
    2: [(1, 4), (7, 1), (5, 2), (8, 1)],
    3: [(6, 2), (4, 1), (2, 3), (3, 3)],
    4: [(2, 4), (7, 2)],
    5: [(8, 2), (5, 3)],
    6: [(3, 4), (4, 2), (6, 3), (5, 4)],
    7: [(7, 3), (8, 3), (4, 3), (6, 4)],
    8: [(4, 4), (7, 4), (8, 4)],
}
GATHER_END = [(7, 4), (8, 4)]


def scatter_copy(at, grad, part, sums, boxes, send, recv, k):
    z, core = at["z"], at["core"]
    if k == 0:
        src, dst, device = grad.at[:, :, 1 - core], sums, {"fsdp": z * 2 + 1 - core}
    elif k == 1:
        src, dst, device = part.at[at["diag"]], boxes.at[0], {"dp": at["second"]}
    elif k == 2:
        src, dst, device = part.at[at["second"]], boxes.at[1], {"dp": at["second"]}
    elif k == 3:
        src, dst, device = part.at[at["first"]], boxes.at[2], {"dp": at["first"]}
    else:
        there = (z + k - 3) % 4
        src, dst, device = part.at[at["dp"], there], boxes.at[3, k - 4], {"fsdp": there * 2 + core}
    return pltpu.make_async_remote_copy(
        src_ref=src, dst_ref=dst, send_sem=send.at[k], recv_sem=recv.at[k],
        device_id=device, device_id_type=MESH,
    )


def direct_copy(at, part, boxes, send, recv, i):
    dp, z = (at["dp"] + i // 4) % 4, (at["z"] + i % 4) % 4
    return pltpu.make_async_remote_copy(
        src_ref=part.at[dp, z], dst_ref=boxes.at[i - 1], send_sem=send.at[i - 1], recv_sem=recv.at[i - 1],
        device_id={"dp": dp, "fsdp": z * 2 + at["core"]}, device_id_type=MESH,
    )


def all_devices(at):
    inner = at["z"] * 2 + at["core"]
    return [{"dp": (at["dp"] + i // 8) % 4, "fsdp": (inner + i % 8) % 8} for i in range(1, 32)]


def add_low(left, right):
    return left + right


def scatter_stage(at, copy, mine, part, sums, boxes, stage):
    dp = at["dp"]
    if stage == 0:
        copy(0).start()
    elif stage == 1:
        copy(0).wait_recv()
        for name in ("diag", "second", "first", "dp"):
            part[at[name]] = add_low(mine(at[name]), sums[at[name]])
            if name == "diag":
                copy(1).start()
            if name == "second":
                copy(2).start()
    elif stage == 2:
        copy(1).wait_recv()
        part[at["first"]] = add_low(part[at["first"]], boxes[0])
        copy(3).start()
    elif stage == 3:
        copy(2).wait_recv()
        part[dp] = add_low(part[dp], boxes[1])
        copy(3).wait_recv()
        part[dp] = add_low(part[dp], boxes[2])
        for k in (4, 5, 6):
            copy(k).start()
    else:
        for k in (4, 5, 6):
            copy(k).wait_recv()


def scatter_total(at, part, boxes):
    total = part[at["dp"], at["z"]].astype(f32)
    for i in range(3):
        total = total + boxes[3, i].astype(f32)
    return total


SCATTER_PLAN = {
    1: [(0, 0), (1, 0), (2, 0), (3, 0), (4, 0)],
    2: [(0, 1), (1, 1), (2, 1)],
    3: [(5, 1), (3, 1), (0, 2)],
    4: [(1, 2), (2, 2), (4, 1)],
    5: [(5, 2), (6, 1), (3, 2), (0, 3)],
    6: [(4, 2), (7, 1), (1, 3), (2, 3)],
    7: [(6, 2), (5, 3), (3, 3), (7, 2), (0, 4)],
}


def spread_projection(omega_ref, wide_ref):
    wide_ref[...] = jnp.zeros_like(wide_ref)
    wide_ref[:HD, :FEAT] = omega_ref[0]
    wide_ref[HD:, FEAT:] = omega_ref[1]


def ones_projection(omega_ref, wide_ref):
    wide_ref[...] = jnp.ones_like(wide_ref)
    for odd in range(2):
        wide_ref[odd, odd * HD : (odd + 1) * HD, :] = omega_ref[odd]


def forward_step(
    block, starts_ref, lens_ref, normed, weight, wide_ref,
    qkv_ref, fq_ref, fk_ref, o_ref, rden_ref, prefix_ref, state_ref,
):
    per_seg = SEG // BLOCK

    @pl.when(block % per_seg == 0)
    def _():
        begins = jnp.logical_or(block == 0, starts_ref[block // per_seg] != 0)
        state_ref[...] = jnp.where(begins, 0.0, state_ref[...])

    qkv_ref[0] = dot_nn(normed, weight).astype(bf16)
    position = lax.broadcasted_iota(jnp.int32, (BLOCK, 1), 0) + (block % per_seg) * BLOCK
    valid = (position < lens_ref[block // per_seg]).astype(f32)
    _, low = lane_masks(TILE)
    causal, _ = causal_masks()
    states = [state_ref[odd] for odd in range(2)]
    cuts = [slice(tile * TILE, (tile + 1) * TILE) for tile in range(TILES_BLOCK)]
    made, mixed = {}, {}

    def features(tile):
        at = cuts[tile]
        feats = []
        for part, feat_ref in enumerate((fq_ref, fk_ref)):
            rows = qkv_ref[0, at, part * DUO : (part + 1) * DUO]
            wide = rows.astype(f32)
            square = wide * wide
            proj = dot_nn(rows, wide_ref[...])
            for odd in range(2):
                total = jnp.sum(
                    jnp.where(low, 0.0, square) if odd else jnp.where(low, square, 0.0), axis=-1, keepdims=True
                )
                value = jnp.exp2(
                    proj[:, odd * FEAT : (odd + 1) * FEAT] * (feat_scale * log2_e)
                    - total * (0.5 * feat_scale * feat_scale * log2_e)
                )
                if part:
                    value = value * valid[at]
                value = value.astype(bf16)
                feat_ref[0, at, odd * FEAT : (odd + 1) * FEAT] = value
                feats.append(value)
        made[tile] = feats, with_ones(qkv_ref[0, at, 2 * DUO :], low)

    def scores(tile):
        feats, ones = made[tile]
        weights = [
            jnp.where(causal, dot_nt(feats[odd], feats[2 + odd]), 0.0).astype(bf16) for odd in range(2)
        ]
        sums = [dot_nn(ones[odd].T, feats[2 + odd]) for odd in range(2)]
        mixed[tile] = weights, sums

    def finish(tile):
        at = cuts[tile]
        (feats, ones), (weights, sums) = made[tile], mixed[tile]
        both = []
        for odd in range(2):
            before_low = states[odd].astype(bf16)
            prefix_ref[0, tile, odd] = before_low
            both.append(dot_nn(weights[odd], ones[odd]) + dot_nt(feats[odd], before_low))
            states[odd] = states[odd] + sums[odd]
        top = jnp.where(low, both[0], both[1])
        bottom = pltpu.roll(jnp.where(low, both[1], both[0]), HD, 1)
        o_ref[at, :] = (top / bottom).astype(bf16)
        rden_ref[0, at, :] = 1.0 / bottom

    for step in range(TILES_BLOCK + 2):
        if step < TILES_BLOCK:
            features(step)
        if 1 <= step <= TILES_BLOCK:
            scores(step - 1)
        if step >= 2:
            finish(step - 2)
    for odd in range(2):
        state_ref[odd] = states[odd]


def block_rows(block):
    return pl.ds(pl.multiple_of(block * BLOCK, BLOCK), BLOCK)


ATTENTION_STEPS = 8


def forward_local_kernel(
    starts_ref, lens_ref, x_ref, w_ref, gain_ref, omega_ref,
    qkv_ref, fq_ref, fk_ref, o_ref, rden_ref, prefix_ref, normed_ref, state_ref, wide_ref,
):
    pair, block = pl.program_id(0), pl.program_id(1)
    rows = block_rows(block)

    @pl.when(pair == 0)
    def _():
        unit, _ = normalise(x_ref[rows, :].astype(f32))
        normed_ref[rows, :] = (unit * gain_ref[0:1, :]).astype(bf16)

    @pl.when(block == 0)
    def _():
        spread_projection(omega_ref, wide_ref)

    forward_step(
        block, starts_ref, lens_ref, normed_ref[rows, :], w_ref[...], wide_ref,
        qkv_ref, fq_ref, fk_ref, o_ref, rden_ref, prefix_ref, state_ref,
    )


def forward_kernel(
    count_ref, starts_ref, lens_ref, x_ref, omega_ref, wq_ref, wo_ref, wu_ref, wd_ref, gains_ref, cot_ref,
    qkv_ref, fq_ref, fk_ref, o_ref, rden_ref, prefix_ref, normed_ref, wpair_ref, gain_ref,
    out_ref, dmid_ref, do_ref, gwo_ref, gwu_ref, gwd_ref,
    state_ref, wide_ref, rows_ref, unit_ref, attended_ref,
    head_ref, held_ref, heldo_ref, heldu_ref, heldd_ref, pad_ref,
    awo_ref, awu_ref, awd_ref, norm_ref, normt_ref, dy_ref, send, recv, local,
):
    step = pl.program_id(0)
    blocks = ATTENTION_STEPS // PAIRS
    pair, block = step // blocks, step % blocks
    at = place()
    dp, z, core = at["dp"], at["z"], at["core"]
    full = [head_ref, held_ref.at[0], held_ref.at[1], held_ref.at[2], heldo_ref] + halves(heldu_ref, heldd_ref)
    own = [array.at[dp, z, core] for array in full]
    partners = near_devices(at)

    def copy(w, k):
        return gather_copy(at, own[w], full[w], send.at[w], recv.at[w], k)

    def leave(w):
        src = (heldo_ref, heldu_ref, heldd_ref)[w]
        return pltpu.make_async_copy(src, (gwo_ref, gwu_ref, gwd_ref)[w], local.at[w])

    def fetch():
        return pltpu.make_async_copy(x_ref, rows_ref, local.at[0])

    def stages(plan):
        for w, stage in plan:
            gather_stage(functools.partial(copy, w), stage)

    @pl.when(step == 0)
    def _():
        greet(partners)
        fetch().start()
        pad_ref[...] = jnp.zeros_like(pad_ref)
        pad_ref[0:2, 0:16] = gains_ref[...]
        flat = pad_ref[...]
        turned = flat
        for i in range(1, 8):
            turned = jnp.where(at["flat"] % 8 == i, pltpu.roll(flat, 16 * i, 1), turned)
        row = lax.broadcasted_iota(jnp.int32, (16, EXTRA), 0)
        band = at["flat"] // 8
        placed = jnp.where(row == band, turned[0:1, :], 0.0) + jnp.where(row == band + 4, turned[1:2, :], 0.0)
        for part in range(3):
            for i in range(PAIRS):
                piece = wq_ref[:, part * D + i * DUO : part * D + (i + 1) * DUO].astype(bf16)
                if i == 0:
                    head_ref[dp, z, core, :, part * DUO : (part + 1) * DUO] = piece
                else:
                    held_ref[i - 1, dp, z, core, :, part * DUO : (part + 1) * DUO] = piece
        head_ref[dp, z, core, :, CHUNK:] = placed.astype(bf16)
        greeted(partners)
        stages(GATHER_PLAN[0][:4])
        heldo_ref[dp, z, core] = wo_ref[...].astype(bf16)
        heldu_ref[dp, z, core] = wu_ref[...].astype(bf16)
        heldd_ref[dp, z, core] = wd_ref[...].astype(bf16)
        stages(GATHER_PLAN[0][4:10])
        fetch().wait()

        @pl.loop(0, blocks)
        def _(i):
            unit_ref[block_rows(i), :] = normalise(rows_ref[block_rows(i), :].astype(f32))[0]

        stages(GATHER_PLAN[0][10:])
        packed = head_ref[..., CHUNK:].astype(f32)
        total = jnp.sum(packed.reshape(32, 16, EXTRA), axis=0)
        gain_ref[...] = jnp.zeros_like(gain_ref)
        for i in range(2):
            for j in range(4):
                gain_ref[i : i + 1, EXTRA * j : EXTRA * (j + 1)] = total[4 * i + j : 4 * i + j + 1, :]

    for when, plan in GATHER_PLAN.items():
        if when:

            @pl.when(step == when)
            def _(plan=plan):
                stages(plan)

    for i in range(PAIRS):

        @pl.when(step == i * blocks)
        def _(i=i):
            piece = held_ref[i - 1] if i else head_ref[..., :CHUNK]
            wpair_ref[...] = piece.reshape(D, CHUNK)
            spread_projection(omega_ref, wide_ref)

    @pl.when(step < ATTENTION_STEPS)
    def _():
        rows = block_rows(block)

        @pl.when(pair == 0)
        def _():
            normed_ref[rows, :] = (unit_ref[rows, :] * gain_ref[0:1, :]).astype(bf16)

        forward_step(
            block, starts_ref, lens_ref, normed_ref[rows, :], wpair_ref[...], wide_ref,
            qkv_ref, fq_ref, fk_ref, o_ref, rden_ref, prefix_ref, state_ref,
        )
        attended_ref[rows, pl.ds(pl.multiple_of(pair * DUO, DUO), DUO)] = o_ref[...]

    @pl.when(step >= ATTENTION_STEPS)
    def _():
        late = step - ATTENTION_STEPS
        rows = pl.ds(pl.multiple_of(late * FF_BLOCK, FF_BLOCK), FF_BLOCK)

        def arrive():
            @pl.when(late == 0)
            def _():
                stages(GATHER_END)

        feed_forward_step(
            late, lens_ref, rows_ref[rows, :], attended_ref[rows, :], cot_ref[...],
            lambda: heldo_ref[...].reshape(D, D),
            lambda c: heldu_ref[..., c * FF_CHUNK : (c + 1) * FF_CHUNK].reshape(D, FF_CHUNK),
            lambda c: heldd_ref[c].reshape(FF_CHUNK, D), gain_ref[1:2, :],
            out_ref.at[rows], dmid_ref, do_ref, awo_ref, awu_ref, awd_ref, norm_ref, normt_ref, dy_ref, arrive,
        )

    @pl.when(step == pl.num_programs(0) - 1)
    def _():
        for w in range(9):
            for k in range(10):
                copy(w, k).wait_send()
        heldo_ref[...] = awo_ref[...].astype(bf16).reshape(heldo_ref.shape)
        leave(0).start()
        heldu_ref[...] = awu_ref[...].astype(bf16).reshape(heldu_ref.shape)
        leave(1).start()
        heldd_ref[...] = awd_ref[...].astype(bf16).reshape(heldd_ref.shape)
        leave(2).start()
        for w in range(3):
            leave(w).wait()


def normal_parts(hidden):
    inner = 0.5 + 0.5 * lax.erf(hidden * (0.5**0.5))
    return inner, jnp.exp2(hidden * hidden * (-0.5 * log2_e)) * (1.0 / math.sqrt(2.0 * math.pi))


def feed_forward_step(
    step, lens_ref, x, attended, cot, wo, wu, wd, gain,
    out_ref, dmid_ref, do_ref, awo_ref, awu_ref, awd_ref, norm_ref, normt_ref, dy_ref, arrive=lambda: None,
):
    @pl.when(step == 0)
    def _():
        awo_ref[...] = jnp.zeros_like(awo_ref)
        awu_ref[...] = jnp.zeros_like(awu_ref)
        awd_ref[...] = jnp.zeros_like(awd_ref)

    per_seg = SEG // FF_BLOCK
    position = lax.broadcasted_iota(jnp.int32, (FF_BLOCK, 1), 0) + (step % per_seg) * FF_BLOCK
    valid = (position < lens_ref[step // per_seg]).astype(f32)
    dy_ref[...] = (cot.astype(f32) * valid).astype(bf16)
    middle = x.astype(f32) + dot_nn(attended, wo())
    unit, inverse = normalise(middle)
    normed = (unit * gain).astype(bf16)
    norm_ref[...] = normed
    normt_ref[...] = normed.T
    total = middle
    back = 0.0
    for index in range(FF // FF_CHUNK):
        at = slice(index * FF_CHUNK, (index + 1) * FF_CHUNK)
        up, down = wu(index), wd(index)
        hidden = dot_nn(norm_ref[...], up)
        inner, bell = normal_parts(hidden)
        active = (hidden * inner).astype(bf16)
        slope = inner + hidden * bell
        total = total + dot_nn(active, down)
        grad_hidden = (slope * dot_nt(dy_ref[...], down)).astype(bf16)
        awd_ref[at, :] += dot_tn(active, dy_ref[...])
        awu_ref[:, at] += dot_nn(normt_ref[...], grad_hidden)
        back = back + dot_nt(grad_hidden, up)
    out_ref[...] = total.astype(bf16)
    grad_middle = dy_ref[...].astype(f32) + normalise_back(back, gain, unit, inverse)
    dmid_ref[...] = grad_middle
    branch = grad_middle.astype(bf16)
    awo_ref[...] += dot_tn(attended, branch)
    do_ref[...] = dot_nt(branch, wo())


def feed_forward_local_kernel(
    lens_ref, x_ref, o_ref, cot_ref, wo_ref, wu_ref, wd_ref, gain_ref,
    out_ref, dmid_ref, do_ref, gwo_ref, gwu_ref, gwd_ref,
    awo_ref, awu_ref, awd_ref, norm_ref, normt_ref, dy_ref,
):
    def chunk(index):
        return slice(index * FF_CHUNK, (index + 1) * FF_CHUNK)

    step = pl.program_id(0)
    feed_forward_step(
        step, lens_ref, x_ref[...], o_ref[...], cot_ref[...],
        lambda: wo_ref[...], lambda c: wu_ref[:, chunk(c)], lambda c: wd_ref[chunk(c), :], gain_ref[1:2, :],
        out_ref, dmid_ref, do_ref, awo_ref, awu_ref, awd_ref, norm_ref, normt_ref, dy_ref,
    )

    @pl.when(step == pl.num_programs(0) - 1)
    def _():
        gwo_ref[...] = awo_ref[...].astype(bf16)
        gwu_ref[...] = awu_ref[...].astype(bf16)
        gwd_ref[...] = awd_ref[...].astype(bf16)


def backward_step(
    block, blocks, starts_ref, qkv_ref, fq_ref, fk_ref, o_ref, rden_ref, do_ref, prefix_ref, wide_ref,
    suffix_ref, store,
):
    per_seg = SEG // BLOCK

    @pl.when(block % per_seg == per_seg - 1)
    def _():
        after = jnp.minimum(block // per_seg + 1, blocks // per_seg - 1)
        ends = jnp.logical_or(block == blocks - 1, starts_ref[after] != 0)
        suffix_ref[...] = jnp.where(ends, 0.0, suffix_ref[...])

    lane, low = lane_masks(TILE)
    causal, anti = causal_masks()
    state_row = lax.broadcasted_iota(jnp.int32, (DUO, FEAT), 0)
    for tile in reversed(range(TILES_BLOCK)):
        at = slice(tile * TILE, (tile + 1) * TILE)
        scaled = do_ref[at, :] * rden_ref[0, at, :]
        product = scaled * o_ref[at, :].astype(f32)
        scaled = scaled.astype(bf16).astype(f32)
        ones = with_ones(qkv_ref[0, at, 2 * DUO :], low)
        back = [[], [], []]
        for odd in range(2):
            free = 0 if odd else HD
            mine = jnp.logical_not(low) if odd else low
            grad_den = -jnp.sum(jnp.where(mine, product, 0.0), axis=-1, keepdims=True)
            grad_one = jnp.where(mine, scaled, jnp.where(lane == free, grad_den, 0.0)).astype(bf16)
            query_feat = fq_ref[0, at, odd * FEAT : (odd + 1) * FEAT]
            key_feat = fk_ref[0, at, odd * FEAT : (odd + 1) * FEAT]
            one = ones[odd]
            after = suffix_ref[odd]
            edge = after[free : free + 1, :]
            rest = edge - edge.astype(bf16).astype(f32)
            after_low = jnp.where(state_row == free + 1, rest, after).astype(bf16)
            before_low = prefix_ref[0, tile, odd]
            weights_t = jnp.where(anti, dot_nt(key_feat, query_feat), 0.0).astype(bf16)
            grad_w = jnp.where(causal, dot_nt(grad_one, one), 0.0).astype(bf16)
            grad_wt = jnp.where(anti, dot_nt(one, grad_one), 0.0).astype(bf16)
            grad_fq = dot_nn(grad_w, key_feat) + dot_nn(grad_one, before_low)
            grad_fk = dot_nn(grad_wt, query_feat) + dot_nn(one, after_low)
            back[2].append(dot_nn(weights_t, grad_one) + dot_nt(key_feat, after_low))
            suffix_ref[odd] = after + dot_tn(grad_one, query_feat)
            grad_pq = (grad_fq * query_feat.astype(f32)).astype(bf16)
            grad_pk = (grad_fk * key_feat.astype(f32)).astype(bf16)
            back[0].append(dot_nt(grad_pq, wide_ref[odd]))
            back[1].append(dot_nt(grad_pk, wide_ref[odd]))
        for part in range(2):
            top = jnp.where(low, back[part][0], back[part][1])
            bottom = pltpu.roll(jnp.where(low, back[part][1], back[part][0]), HD, 1)
            values = qkv_ref[0, at, part * DUO : (part + 1) * DUO].astype(f32)
            store(tile, part, top * feat_scale - bottom * (feat_scale * feat_scale) * values)
        store(tile, 2, jnp.where(low, back[2][0], back[2][1]))


def pair_lanes(pair):
    return pl.ds(pl.multiple_of(pair * CHUNK, CHUNK), CHUNK)


def store_into(dqkv_ref, pair, block):
    def store(tile, part, value):
        rows = pl.ds(pl.multiple_of(block * BLOCK + tile * TILE, TILE), TILE)
        lanes = pl.ds(pl.multiple_of(pair * CHUNK + part * DUO, DUO), DUO)
        dqkv_ref[rows, lanes] = value.astype(bf16)

    return store


def input_gradient(i, x_ref, dqkv_ref, weight_ref, gain, dmid_ref):
    rows = pl.ds(pl.multiple_of(i * TILE, TILE), TILE)
    grad_normed = dot_nt(dqkv_ref[rows, :], weight_ref[...])
    unit, inverse = normalise(x_ref[rows, :].astype(f32))
    dmid_ref[rows, :] = dmid_ref[rows, :] + normalise_back(grad_normed, gain, unit, inverse)
    return rows


def backward_local_kernel(
    starts_ref, normed_ref, qkv_ref, fq_ref, fk_ref, o_ref, rden_ref, do_ref, prefix_ref, omega_ref, gain_ref,
    x_ref, dmid_in_ref, weight_ref,
    gin_ref, gw_ref,
    suffix_ref, wide_ref, dqkv_ref, rowsn_ref,
):
    pair, step = pl.program_id(0), pl.program_id(1)
    blocks = pl.num_programs(1)
    block = blocks - 1 - step

    @pl.when(step == 0)
    def _():
        ones_projection(omega_ref, wide_ref)

    @pl.when(pair == 0)
    def _():
        rowsn_ref[block_rows(block), :] = normed_ref[...]

    backward_step(
        block, blocks, starts_ref, qkv_ref, fq_ref, fk_ref, o_ref, rden_ref, do_ref, prefix_ref, wide_ref,
        suffix_ref, store_into(dqkv_ref, pair, block),
    )

    @pl.when(step == blocks - 1)
    def _():
        gw_ref[...] = dot_tn(rowsn_ref[...], dqkv_ref[:, pair_lanes(pair)]).astype(bf16)

    @pl.when(jnp.logical_and(step == blocks - 1, pair == PAIRS - 1))
    def _():
        gin_ref[...] = dmid_in_ref[...]

        @pl.loop(0, blocks * TILES_BLOCK)
        def _(i):
            input_gradient(i, x_ref, dqkv_ref, weight_ref, gain_ref[0:1, :], gin_ref)


def eye_row(column):
    row = lax.broadcasted_iota(jnp.int32, (16, 16), 0)
    lane = lax.broadcasted_iota(jnp.int32, (16, 16), 1)
    return jnp.sum(jnp.where(row == lane, column, 0.0), axis=0, keepdims=True)


def row_squares(value):
    return jnp.sum(value * value, axis=-1, keepdims=True).sum(axis=0, keepdims=True)


def backward_kernel(
    starts_ref, normed_ref, qkv_ref, fq_ref, fk_ref, o_ref, rden_ref, do_ref, prefix_ref, omega_ref, gain_ref,
    wq_ref, wu_ref, own_gain_ref, x_ref, dmid_ref, weight_ref, go_ref, gu_ref, gd_ref,
    gin_ref, ro_ref, ru_ref, rd_ref, rq_ref, rg_ref, norm_ref,
    suffix_ref, wide_ref, dqkv_ref, rowsn_ref, gq_ref,
    rows_ref, held_ref,
    po_ref, pu_ref, pd_ref, pq_ref, so_ref, su_ref, sd_ref, sq_ref, bo_ref, bu_ref, bd_ref, bq_ref,
    last_ref, near_ref, send, recv, local, last_send, last_recv, near_send, near_recv,
):
    pair, inner_step = pl.program_id(0), pl.program_id(1)
    blocks = pl.num_programs(1)
    block = blocks - 1 - inner_step
    step = pair * blocks + inner_step
    at = place()
    dp, z, core = at["dp"], at["z"], at["core"]
    grads = [go_ref] + halves(gu_ref, gd_ref) + [gq_ref.at[i] for i in range(PAIRS)]

    def each(out, up, down, pairs):
        return [out, up.at[0], up.at[1], down.at[0], down.at[1]] + [pairs.at[i] for i in range(PAIRS)]

    parts = each(po_ref, pu_ref, pd_ref, pq_ref)
    sums = each(so_ref, su_ref, sd_ref, sq_ref)
    boxes = each(bo_ref, bu_ref, bd_ref, bq_ref)
    results = [ro_ref, ru_ref.at[:, : FF // 2], ru_ref.at[:, FF // 2 :], rd_ref.at[:32], rd_ref.at[32:]]
    results += [rq_ref.at[i] for i in range(PAIRS)]
    others = all_devices(at)

    def copy(w, k):
        return scatter_copy(at, grads[w], parts[w], sums[w], boxes[w], send.at[w], recv.at[w], k)

    def keep(w):
        return pltpu.make_async_copy(grads[w].at[:, :, core], parts[w], local.at[w])

    def late(i):
        src = (x_ref, dmid_ref, weight_ref)[i]
        dst = (rows_ref, gin_ref, held_ref)[i]
        return pltpu.make_async_copy(src, dst, local.at[5 + i])

    def stages(plan):
        for w, stage in plan:
            if w < 5:
                if stage == 0:
                    keep(w).start()
                if stage == 1:
                    keep(w).wait()
                mine = lambda index, w=w: parts[w][index]
            else:
                mine = lambda index, w=w: gq_ref[w - 5, index, :, core]
            scatter_stage(at, functools.partial(copy, w), mine, parts[w], sums[w], boxes[w], stage)
            if stage == 4:
                results[w][...] = scatter_total(at, parts[w], boxes[w])

    @pl.when(step == 0)
    def _():
        greet(others)
        for i in range(3):
            late(i).start()

    @pl.when(step == 1)
    def _():
        greeted(others)

    for when, plan in SCATTER_PLAN.items():

        @pl.when(step == when)
        def _(plan=plan):
            stages(plan)

    @pl.when(inner_step == 0)
    def _():
        ones_projection(omega_ref, wide_ref)

    @pl.when(pair == 0)
    def _():
        rowsn_ref[block_rows(block), :] = normed_ref[...]

    backward_step(
        block, blocks, starts_ref, qkv_ref, fq_ref, fk_ref, o_ref, rden_ref, do_ref, prefix_ref, wide_ref,
        suffix_ref, store_into(dqkv_ref, pair, block),
    )

    for i in range(PAIRS):

        @pl.when(step == (i + 1) * blocks - 1)
        def _(i=i):
            grad = dot_tn(rowsn_ref[...], dqkv_ref[:, i * CHUNK : (i + 1) * CHUNK]).astype(bf16)
            gq_ref[i] = grad.reshape(4, 4, 2, 16, CHUNK)
            stages([(5 + i, 0)])

    @pl.when(step == PAIRS * blocks - 1)
    def _():
        for i in range(3):
            late(i).wait()
        tiles = blocks * TILES_BLOCK

        def inputs_part(first, last):
            @pl.loop(first * tiles // 8, last * tiles // 8)
            def _(i):
                input_gradient(i, rows_ref, dqkv_ref, held_ref, gain_ref[0:1, :], gin_ref)

        def last(i):
            return direct_copy(at, parts[8], last_ref, last_send, last_recv, i)

        stages([(4, 3), (6, 3), (7, 3)])
        inputs_part(0, 1)
        copy(8, 0).wait_recv()
        for i in range(4):
            index = (dp + i) % 4
            parts[8][index] = add_low(gq_ref[3, index, :, core], sums[8][index])
            for j in range(4):
                if i + j:
                    last(4 * i + j).start()
        inputs_part(1, 5)
        stages([(1, 4), (2, 4), (3, 4), (5, 4), (4, 4), (6, 4), (7, 4)])
        inputs_part(5, 8)
        early = row_squares(ro_ref[...]) + row_squares(ru_ref[...]) + row_squares(rd_ref[...])
        for i in range(PAIRS - 1):
            early = early + row_squares(rq_ref[i])
        up_low = wu_ref[...].astype(bf16).astype(f32)
        gain_low = own_gain_ref[...].astype(bf16).astype(f32)
        second = eye_row(jnp.sum(ru_ref[...] * up_low, axis=-1, keepdims=True)) / gain_low[1:2, :]
        total = parts[8][dp, z].astype(f32)
        for i in range(1, 16):
            last(i).wait_recv()
            total = total + last_ref[i - 1].astype(f32)
        rq_ref[3] = total
        first = jnp.zeros((16, 1), f32)
        for i in range(PAIRS):
            for part in range(3):
                low_w = wq_ref[:, part * D + i * DUO : part * D + (i + 1) * DUO].astype(bf16).astype(f32)
                first = first + jnp.sum(
                    rq_ref[i, :, part * DUO : (part + 1) * DUO] * low_w, axis=-1, keepdims=True
                )
        first = eye_row(first) / gain_low[0:1, :]
        rg_ref[0:1, :] = first
        rg_ref[1:2, :] = second
        squares = early + row_squares(rq_ref[PAIRS - 1]) + row_squares(first) + row_squares(second)
        mine = near_ref.at[at["flat"]]
        mine[...] = jnp.broadcast_to(squares, (8, 128))

        def near(i):
            return pltpu.make_async_remote_copy(
                src_ref=mine, dst_ref=mine, send_sem=near_send.at[i], recv_sem=near_recv.at[i],
                device_id=others[i], device_id_type=MESH,
            )

        for i in range(31):
            near(i).start()
        for i in range(31):
            near(i).wait_recv()
        group = near_ref[0]
        for i in range(1, 32):
            group = group + near_ref[i]
        norm_ref[...] = group

        for i in range(31):
            near(i).wait_send()
        for i in range(1, 16):
            last(i).wait_send()
        copy(8, 0).wait_send()
        for w in range(8):
            for k in range(7):
                copy(w, k).wait_send()


def update_kernel(
    count_ref, total_ref, rq_ref, ro_ref, ru_ref, rd_ref, rg_ref,
    wq_ref, wo_ref, wu_ref, wd_ref, wg_ref, mq_ref, mo_ref, mu_ref, md_ref, mg_ref,
    vq_ref, vo_ref, vu_ref, vd_ref, vg_ref, gin_ref, out_ref,
    norm_ref, gq_ref, nvq_ref, nwq_ref, go_ref, nvo_ref, nwo_ref, gu_ref, nvu_ref, nwu_ref,
    gd_ref, nvd_ref, nwd_ref, gg_ref, nvg_ref, nwg_ref, gin_out_ref, out_out_ref, sem,
):
    quarter = gin_ref.shape[0] // 4
    moves = []
    for i in range(4):
        rows = pl.ds(i * quarter, quarter)
        for j, (src, dst) in enumerate(((gin_ref, gin_out_ref), (out_ref, out_out_ref))):
            moves.append(pltpu.make_async_copy(src.at[rows], dst.at[rows], sem.at[j, i]))
    for move in moves:
        move.start()
    update_weights(
        count_ref, total_ref, rq_ref, ro_ref, ru_ref, rd_ref, rg_ref,
        wq_ref, wo_ref, wu_ref, wd_ref, wg_ref, mq_ref, mo_ref, mu_ref, md_ref, mg_ref,
        vq_ref, vo_ref, vu_ref, vd_ref, vg_ref,
        norm_ref, gq_ref, nvq_ref, nwq_ref, go_ref, nvo_ref, nwo_ref, gu_ref, nvu_ref, nwu_ref,
        gd_ref, nvd_ref, nwd_ref, gg_ref, nvg_ref, nwg_ref,
    )
    for move in moves:
        move.wait()


def update_weights(
    count_ref, total_ref, rq_ref, ro_ref, ru_ref, rd_ref, rg_ref,
    wq_ref, wo_ref, wu_ref, wd_ref, wg_ref, mq_ref, mo_ref, mu_ref, md_ref, mg_ref,
    vq_ref, vo_ref, vu_ref, vd_ref, vg_ref,
    norm_ref, gq_ref, nvq_ref, nwq_ref, go_ref, nvo_ref, nwo_ref, gu_ref, nvu_ref, nwu_ref,
    gd_ref, nvd_ref, nwd_ref, gg_ref, nvg_ref, nwg_ref,
):
    norm = jnp.sqrt(total_ref[0:1, 0:1])
    norm_ref[...] = norm
    factor = jnp.minimum(1.0, clip_level / norm)
    count = jnp.full((1, 1), count_ref[0], jnp.int32).astype(f32)
    first_fix = 1.0 - jnp.exp2(count * math.log2(beta_first))
    second_fix = 1.0 - jnp.exp2(count * math.log2(beta_second))

    def update(grad, at, weight, first, second, rate, outs):
        clipped = grad * factor
        first_new = beta_first * first[at] + (1.0 - beta_first) * clipped
        second_new = beta_second * second[at] + (1.0 - beta_second) * clipped * clipped
        direction = first_new / first_fix / (jnp.sqrt(second_new / second_fix) + adam_eps)
        outs[0][at] = clipped
        outs[1][at] = second_new
        outs[2][at] = weight[at] - rate * (direction + decay_weight * weight[at])

    for part in range(3):
        for i in range(PAIRS):
            at = (slice(None), slice(part * D + i * DUO, part * D + (i + 1) * DUO))
            grad = rq_ref[i, :, part * DUO : (part + 1) * DUO]
            update(grad, at, wq_ref, mq_ref, vq_ref, rate_matrix, (gq_ref, nvq_ref, nwq_ref))
    update(ro_ref[...], ..., wo_ref, mo_ref, vo_ref, rate_matrix, (go_ref, nvo_ref, nwo_ref))
    update(ru_ref[...], ..., wu_ref, mu_ref, vu_ref, rate_matrix, (gu_ref, nvu_ref, nwu_ref))
    update(rd_ref[...], ..., wd_ref, md_ref, vd_ref, rate_matrix, (gd_ref, nvd_ref, nwd_ref))
    update(rg_ref[...], ..., wg_ref, mg_ref, vg_ref, rate_gain, (gg_ref, nvg_ref, nwg_ref))


ROWS = {"pair": 16, "out": 16, "up": 16, "down": 64}
COLS = {"pair": CHUNK, "out": D, "up": FF, "down": D}
LATE = ("out", "up", "down")
smem = pl.BlockSpec(memory_space=pltpu.SMEM)
hbm = pl.BlockSpec(memory_space=pl.ANY)
vmem = pl.BlockSpec(memory_space=pltpu.VMEM)


def shaped(shape, dtype):
    return jax.ShapeDtypeStruct(shape, dtype)


def params(collective_id=None, mib=63):
    if collective_id is None:
        return pltpu.CompilerParams(vmem_limit_bytes=mib << 20)
    return pltpu.CompilerParams(vmem_limit_bytes=mib << 20, collective_id=collective_id, has_side_effects=True)


def whole(shape):
    return pl.BlockSpec(shape, lambda *_: (0,) * len(shape), pipeline_mode=pl.Buffered(1))


def whole_out(shape):
    return pl.BlockSpec(shape, lambda *_: (0,) * len(shape))


def five(name):
    return (4, 4, 2, ROWS[name], COLS[name])


def forward_outs(tokens):
    tiles = tokens // TILE
    specs = [
        pl.BlockSpec((1, BLOCK, CHUNK), lambda p, b: (p, b, 0)),
        pl.BlockSpec((1, BLOCK, 2 * FEAT), lambda p, b: (p, b, 0)),
        pl.BlockSpec((1, BLOCK, 2 * FEAT), lambda p, b: (p, b, 0)),
        pl.BlockSpec((BLOCK, DUO), lambda p, b: (b, p)),
        pl.BlockSpec((1, BLOCK, DUO), lambda p, b: (p, b, 0)),
        pl.BlockSpec((1, TILES_BLOCK, 2, DUO, FEAT), lambda p, b: (p, b, 0, 0, 0)),
        whole_out((tokens, D)),
    ]
    shapes = [
        shaped((PAIRS, tokens, CHUNK), bf16),
        shaped((PAIRS, tokens, 2 * FEAT), bf16),
        shaped((PAIRS, tokens, 2 * FEAT), bf16),
        shaped((tokens, D), bf16),
        shaped((PAIRS, tokens, DUO), f32),
        shaped((PAIRS, tiles, 2, DUO, FEAT), bf16),
        shaped((tokens, D), bf16),
    ]
    scratch = [pltpu.VMEM((2, DUO, FEAT), f32), pltpu.VMEM((DUO, 2 * FEAT), bf16)]
    return specs, shapes, scratch


pair_omega = pl.BlockSpec((2, HD, FEAT), lambda p, b: (p, 0, 0))
pair_weight = pl.BlockSpec((D, CHUNK), lambda p, b: (0, p))


def forward_local(starts, lens, x, weight, gains, omega):
    tokens = x.shape[0]
    specs, shapes, scratch = forward_outs(tokens)
    return pl.pallas_call(
        forward_local_kernel,
        grid=(PAIRS, tokens // BLOCK),
        in_specs=[smem, smem, whole((tokens, D)), pair_weight, whole((8, D)), pair_omega],
        out_specs=specs,
        out_shape=shapes,
        scratch_shapes=scratch,
        compiler_params=params(),
    )(starts, lens, x, weight, gains, omega)


def forward(count, starts, lens, x, omega, wq, wo, wu, wd, gains, cot):
    tokens = x.shape[0]
    blocks = tokens // BLOCK
    steps = PAIRS * blocks
    specs, shapes, scratch = forward_outs(tokens)

    def early(index_map):
        return lambda i: index_map(
            jnp.minimum(i // blocks, PAIRS - 1), jnp.where(i < steps, i % blocks, blocks - 1)
        )

    specs = [pl.BlockSpec(spec.block_shape, early(spec.index_map)) for spec in specs]
    weight = pl.BlockSpec(pair_weight.block_shape, early(pair_weight.index_map))
    heads = pl.BlockSpec(pair_omega.block_shape, early(pair_omega.index_map))
    rows = pl.BlockSpec((FF_BLOCK, D), lambda i: (jnp.maximum(i - steps, 0), 0))
    return pl.pallas_call(
        forward_kernel,
        grid=(steps + tokens // FF_BLOCK,),
        in_specs=[smem, smem, smem, hbm, heads] + [whole(array.shape) for array in (wq, wo, wu, wd, gains)] + [rows],
        out_specs=specs + [weight, whole_out((8, D)), vmem, rows, rows, hbm, hbm, hbm],
        out_shape=shapes
        + [shaped((D, WIDE), bf16), shaped((8, D), f32)]
        + [pltpu.VMEM((tokens, D), bf16), shaped((tokens, D), f32), shaped((tokens, D), f32)]
        + [shaped(five(name), bf16) for name in LATE],
        scratch_shapes=scratch
        + [
            pltpu.VMEM((tokens, D), bf16),
            pltpu.VMEM((tokens, D), f32),
            pltpu.VMEM((tokens, D), bf16),
            pltpu.VMEM((4, 4, 2, 16, CHUNK + EXTRA), bf16),
            pltpu.VMEM((PAIRS - 1, *five("pair")), bf16),
        ]
        + [pltpu.VMEM(five(name), bf16) for name in LATE]
        + [pltpu.VMEM((8, EXTRA), f32)]
        + feed_forward_scratch()
        + [
            pltpu.SemaphoreType.DMA((9, 10)),
            pltpu.SemaphoreType.DMA((9, 10)),
            pltpu.SemaphoreType.DMA((3,)),
        ],
        compiler_params=params(0, FORWARD_MIB),
    )(count, starts, lens, x, omega, wq, wo, wu, wd, gains, cot)


def feed_forward_scratch():
    return [
        pltpu.VMEM((D, D), f32), pltpu.VMEM((D, FF), f32), pltpu.VMEM((FF, D), f32),
        pltpu.VMEM((FF_BLOCK, D), bf16), pltpu.VMEM((D, FF_BLOCK), bf16), pltpu.VMEM((FF_BLOCK, D), bf16),
    ]


def feed_forward_local(lens, x, o, cot, wo, wu, wd, gains):
    tokens = x.shape[0]
    rows = pl.BlockSpec((FF_BLOCK, D), lambda i: (i, 0))
    return pl.pallas_call(
        feed_forward_local_kernel,
        grid=(tokens // FF_BLOCK,),
        in_specs=[smem, rows, rows, rows, whole((D, D)), whole((D, FF)), whole((FF, D)), whole((8, D))],
        out_specs=[rows, rows, rows, whole_out((D, D)), whole_out((D, FF)), whole_out((FF, D))],
        out_shape=[
            shaped((tokens, D), bf16),
            shaped((tokens, D), f32),
            shaped((tokens, D), f32),
            shaped((D, D), bf16),
            shaped((D, FF), bf16),
            shaped((FF, D), bf16),
        ],
        scratch_shapes=feed_forward_scratch(),
        compiler_params=params(),
    )(lens, x, o, cot, wo, wu, wd, gains)


def backward_ins(blocks):
    last = blocks - 1
    return [
        smem,
        pl.BlockSpec((BLOCK, D), lambda p, b: (jnp.where(p == 0, last - b, 0), 0)),
        pl.BlockSpec((1, BLOCK, CHUNK), lambda p, b: (p, last - b, 0)),
        pl.BlockSpec((1, BLOCK, 2 * FEAT), lambda p, b: (p, last - b, 0)),
        pl.BlockSpec((1, BLOCK, 2 * FEAT), lambda p, b: (p, last - b, 0)),
        pl.BlockSpec((BLOCK, DUO), lambda p, b: (last - b, p)),
        pl.BlockSpec((1, BLOCK, DUO), lambda p, b: (p, last - b, 0)),
        pl.BlockSpec((BLOCK, DUO), lambda p, b: (last - b, p)),
        pl.BlockSpec((1, TILES_BLOCK, 2, DUO, FEAT), lambda p, b: (p, last - b, 0, 0, 0)),
        pair_omega,
        whole((8, D)),
    ]


def backward_scratch(tokens):
    return [
        pltpu.VMEM((2, DUO, FEAT), f32),
        pltpu.VMEM((2, DUO, FEAT), bf16),
        pltpu.VMEM((tokens, WIDE), bf16),
        pltpu.VMEM((tokens, D), bf16),
    ]


def backward_local(args, x, dmid, weight):
    tokens = x.shape[0]
    return pl.pallas_call(
        backward_local_kernel,
        grid=(PAIRS, tokens // BLOCK),
        in_specs=backward_ins(tokens // BLOCK) + [whole((tokens, D)), whole((tokens, D)), whole((D, WIDE))],
        out_specs=[whole_out((tokens, D)), pair_weight],
        out_shape=[shaped((tokens, D), f32), shaped((D, WIDE), bf16)],
        scratch_shapes=backward_scratch(tokens),
        compiler_params=params(),
    )(*args, x, dmid, weight)


def backward(args, wq, wu, gains, x, dmid, weight, grads):
    tokens = x.shape[0]
    half = [(4, 4, 16, D), (2, 4, 4, 16, FF // 2), (2, 4, 4, 32, D), (PAIRS, 4, 4, 16, CHUNK)]
    dma = pltpu.SemaphoreType.DMA
    return pl.pallas_call(
        backward_kernel,
        grid=(PAIRS, tokens // BLOCK),
        in_specs=backward_ins(tokens // BLOCK) + [whole(wq.shape), whole(wu.shape), whole(gains.shape)] + [hbm] * 6,
        out_specs=[vmem] * 7,
        out_shape=[pltpu.VMEM((tokens, D), f32)]
        + [pltpu.VMEM((ROWS[name], COLS[name]), f32) for name in LATE]
        + [pltpu.VMEM((PAIRS, 16, CHUNK), f32), pltpu.VMEM((2, 16), f32), pltpu.VMEM((8, 128), f32)],
        scratch_shapes=backward_scratch(tokens)
        + [pltpu.VMEM((PAIRS, *five("pair")), bf16)]
        + [pltpu.VMEM((tokens, D), bf16), pltpu.VMEM((D, WIDE), bf16)]
        + [pltpu.VMEM(shape, bf16) for shape in half] * 3
        + [pltpu.VMEM((15, 16, CHUNK), bf16), pltpu.VMEM((32, 8, 128), f32)]
        + [dma((9, 7)), dma((9, 7)), dma((8,)), dma((15,)), dma((15,)), dma((31,)), dma((31,))],
        compiler_params=params(1, BACKWARD_MIB),
    )(*args, wq, wu, gains, x, dmid, weight, *grads)


def update_all(count, total, grads, weights, firsts, seconds, grad_inputs, out_rows):
    shapes = [shaped((1, 1), f32)]
    for weight in weights:
        shapes += [shaped(weight.shape, f32)] * 3
    return pl.pallas_call(
        update_kernel,
        in_specs=[smem] + [vmem] * 23,
        out_specs=[vmem] * 16 + [hbm, hbm],
        out_shape=shapes + [shaped(grad_inputs.shape, f32), shaped(out_rows.shape, bf16)],
        scratch_shapes=[pltpu.SemaphoreType.DMA((2, 4))],
        compiler_params=params(mib=UPDATE_MIB),
    )(count, total, *grads, *weights, *firsts, *seconds, grad_inputs, out_rows)


def to_pairs(weight):
    split = weight.reshape(weight.shape[0], 3, PAIRS, DUO)
    return jnp.swapaxes(split, 1, 2).reshape(weight.shape)


def from_pairs(weight):
    split = weight.reshape(weight.shape[0], PAIRS, 3, DUO)
    return jnp.swapaxes(split, 1, 2).reshape(weight.shape)


def on_device(
    sizes, inputs, cotangent, feature_omega, seg_start, seg_len, step_count,
    w_qkv, w_out, w_up, w_down, gains,
    m_qkv, m_out, m_up, m_down, m_gains,
    v_qkv, v_out, v_up, v_down, v_gains,
):
    weights = (w_qkv, w_out, w_up, w_down, gains)
    firsts = (m_qkv, m_out, m_up, m_down, m_gains)
    seconds = (v_qkv, v_out, v_up, v_down, v_gains)
    if sizes == (4, 8):
        count = step_count.reshape(1)
        (qkv, fq, fk, attended, rden, prefix, normed, qkv_full, gain_full, out_rows, dmid, grad_attended,
         *grads) = forward(count, seg_start, seg_len, inputs, feature_omega, *weights, cotangent)
        grad_inputs, r_out, r_up, r_down, r_qkv, r_gains, total = backward(
            (seg_start, normed, qkv, fq, fk, attended, rden, grad_attended, prefix, feature_omega, gain_full),
            w_qkv, w_up, gains, inputs, dmid, qkv_full, grads,
        )
        norm, *updated, grad_inputs, out_rows = update_all(
            count, total, (r_qkv, r_out, r_up, r_down, r_gains), weights, firsts, seconds, grad_inputs, out_rows
        )
        return (out_rows, grad_inputs, norm.reshape(()), *updated)

    def gather(piece, axis=0):
        return lax.all_gather(piece.astype(bf16), AXES, axis=axis, tiled=True)

    qkv_full, out_full, up_full, down_full = (gather(piece) for piece in weights[:4])
    qkv_full = to_pairs(qkv_full)
    gain_full = jnp.pad(gather(gains, 1).astype(f32), ((0, 6), (0, 0)))
    qkv, fq, fk, attended, rden, prefix, normed = forward_local(
        seg_start, seg_len, inputs, qkv_full, gain_full, feature_omega
    )
    out_rows, dmid, grad_attended, grad_out, grad_up, grad_down = feed_forward_local(
        seg_len, inputs, attended, cotangent, out_full, up_full, down_full, gain_full
    )
    grad_inputs, grad_qkv = backward_local(
        (seg_start, normed, qkv, fq, fk, attended, rden, grad_attended, prefix, feature_omega, gain_full),
        inputs, dmid, qkv_full,
    )

    def scatter(piece):
        return lax.psum_scatter(piece.astype(f32), AXES, scatter_dimension=0, tiled=True)

    reduced = [scatter(piece) for piece in (from_pairs(grad_qkv), grad_out, grad_up, grad_down)]
    low = [weight.astype(bf16).astype(f32) for weight in weights]
    first = jnp.sum(reduced[0] * low[0], axis=1) / low[4][0]
    second = jnp.sum(reduced[2] * low[2], axis=1) / low[4][1]
    reduced.append(jnp.stack([first, second], axis=0))
    grad_norm = jnp.sqrt(lax.psum(sum(jnp.sum(piece * piece) for piece in reduced), AXES))
    factor = jnp.minimum(1.0, clip_level / grad_norm)
    count = step_count.astype(f32)
    first_fix = 1.0 - jnp.power(beta_first, count)
    second_fix = 1.0 - jnp.power(beta_second, count)
    updated = []
    rates = (rate_matrix,) * 4 + (rate_gain,)
    for weight, first, second, gradient, rate in zip(weights, firsts, seconds, reduced, rates):
        clipped = gradient * factor
        first_new = beta_first * first + (1.0 - beta_first) * clipped
        second_new = beta_second * second + (1.0 - beta_second) * clipped * clipped
        direction = first_new / first_fix / (jnp.sqrt(second_new / second_fix) + adam_eps)
        updated += [clipped, second_new, weight - rate * (direction + decay_weight * weight)]
    return (out_rows, grad_inputs, grad_norm, *updated)


def solution(mesh):
    return jax.shard_map(
        functools.partial(on_device, tuple(mesh.shape[name] for name in AXES)),
        mesh=mesh,
        in_specs=(
            P(("dp", "fsdp"), None),
            P(("dp", "fsdp"), None),
            P(),
            P(("dp", "fsdp")),
            P(("dp", "fsdp")),
            P(),
            P(("dp", "fsdp"), None),
            P(("dp", "fsdp"), None),
            P(("dp", "fsdp"), None),
            P(("dp", "fsdp"), None),
            P(None, ("dp", "fsdp")),
            P(("dp", "fsdp"), None),
            P(("dp", "fsdp"), None),
            P(("dp", "fsdp"), None),
            P(("dp", "fsdp"), None),
            P(None, ("dp", "fsdp")),
            P(("dp", "fsdp"), None),
            P(("dp", "fsdp"), None),
            P(("dp", "fsdp"), None),
            P(("dp", "fsdp"), None),
            P(None, ("dp", "fsdp")),
        ),
        out_specs=(
            P(("dp", "fsdp"), None),
            P(("dp", "fsdp"), None),
            P(),
            P(("dp", "fsdp"), None),
            P(("dp", "fsdp"), None),
            P(("dp", "fsdp"), None),
            P(("dp", "fsdp"), None),
            P(("dp", "fsdp"), None),
            P(("dp", "fsdp"), None),
            P(("dp", "fsdp"), None),
            P(("dp", "fsdp"), None),
            P(("dp", "fsdp"), None),
            P(("dp", "fsdp"), None),
            P(("dp", "fsdp"), None),
            P(("dp", "fsdp"), None),
            P(None, ("dp", "fsdp")),
            P(None, ("dp", "fsdp")),
            P(None, ("dp", "fsdp")),
        ),
        check_vma=False,
    )
```

```python
import functools
import math

import jax
import jax.numpy as jnp
from jax import lax
from jax.experimental import pallas as pl
from jax.experimental.pallas import tpu as pltpu
from jax.sharding import PartitionSpec as P

D = 512
HEADS = 8
HD = 64
FEAT = 256
FF = 2048
SEG = 1024
TILE = 256
PAIRS = HEADS // 2
DUO = 2 * HD
BLOCK = 1024
TILES_BLOCK = BLOCK // TILE
FORWARD_MIB = 61
BACKWARD_MIB = 52
UPDATE_MIB = 20
FF_BLOCK = 1024
FF_PART = 512
FF_CHUNK = 512
WIDE = 3 * D
CHUNK = 3 * DUO
EXTRA = 128
AXES = ("dp", "fsdp")

norm_eps = 1e-05
clip_level = 1.0
rate_matrix = 0.03
rate_gain = 0.4
beta_first = 0.9
beta_second = 0.95
adam_eps = 1e-08
decay_weight = 0.1

feat_scale = HD ** (-0.25)
log2_e = math.log2(math.e)
f32 = jnp.float32
bf16 = jnp.bfloat16
MESH = pl.DeviceIdType.MESH


def dot_nn(a, b):
    return lax.dot_general(a, b, (((1,), (0,)), ((), ())), preferred_element_type=f32)


def dot_nt(a, b):
    return lax.dot_general(a, b, (((1,), (1,)), ((), ())), preferred_element_type=f32)


def dot_tn(a, b):
    return lax.dot_general(a, b, (((0,), (0,)), ((), ())), preferred_element_type=f32)


def normalise(rows):
    centred = rows - jnp.mean(rows, axis=-1, keepdims=True)
    spread = jnp.mean(centred * centred, axis=-1, keepdims=True)
    inverse = lax.rsqrt(spread + norm_eps)
    return centred * inverse, inverse


def normalise_back(grad, gain, unit, inverse):
    scaled = grad * gain
    first = jnp.mean(scaled, axis=-1, keepdims=True)
    second = jnp.mean(scaled * unit, axis=-1, keepdims=True)
    return inverse * (scaled - first - unit * second)


def lane_masks(rows):
    lane = lax.broadcasted_iota(jnp.int32, (rows, DUO), 1)
    return lane, lane < HD


def causal_masks():
    row = lax.broadcasted_iota(jnp.int32, (TILE, TILE), 0)
    col = lax.broadcasted_iota(jnp.int32, (TILE, TILE), 1)
    return row >= col, row <= col


def with_ones(value_pair, low):
    wide = value_pair.astype(f32)
    return (
        jnp.where(low, wide, 1.0).astype(bf16),
        jnp.where(low, 1.0, wide).astype(bf16),
    )


def place():
    dp, inner = lax.axis_index("dp"), lax.axis_index("fsdp")
    z, core = inner // 2, inner % 2
    y, x = dp // 2, dp % 2
    across = y * 2 + (1 - x)
    along = (1 - y) * 2 + x
    return {
        "dp": dp, "z": z, "core": core, "flat": dp * 8 + inner,
        "first": core * along + (1 - core) * across,
        "second": core * across + (1 - core) * along,
        "diag": (1 - y) * 2 + (1 - x),
    }


def greet(devices):
    barrier = pltpu.get_barrier_semaphore()
    for device in devices:
        pl.semaphore_signal(barrier, inc=1, device_id=device, device_id_type=MESH)


def greeted(devices):
    pl.semaphore_wait(pltpu.get_barrier_semaphore(), len(devices))


def near_devices(at):
    devices = [{"fsdp": (at["z"] + i) % 4 * 2 + at["core"]} for i in range(1, 4)]
    devices += [{"fsdp": at["z"] * 2 + 1 - at["core"]}]
    devices += [{"dp": at["first"]}, {"dp": at["second"]}]
    return devices


def halves(up, down):
    return [up.at[..., i * (FF // 2) : (i + 1) * (FF // 2)] for i in range(2)] + [
        down.at[:, :, :, i * 32 : (i + 1) * 32, :] for i in range(2)
    ]


def gather_copy(at, own, full, send, recv, k):
    dp, z, core = at["dp"], at["z"], at["core"]
    sibling = {"fsdp": z * 2 + 1 - core}
    if k < 3:
        src, dst, device = own, full.at[dp, z, core], {"fsdp": (z + 1 + k) % 4 * 2 + core}
    else:
        which = {3: "dp", 4: "dp", 5: "dp", 6: "first", 7: "first", 8: "second", 9: "diag"}[k]
        src = dst = full.at[at[which], :, core]
        device = {4: {"dp": at["first"]}, 5: {"dp": at["second"]}, 6: {"dp": at["second"]}}.get(k, sibling)
    return pltpu.make_async_remote_copy(
        src_ref=src, dst_ref=dst, send_sem=send.at[k], recv_sem=recv.at[k],
        device_id=device, device_id_type=MESH,
    )


def gather_stage(copy, stage):
    if stage == 0:
        for k in range(3):
            copy(k).start()
    elif stage == 1:
        for k in range(3):
            copy(k).wait_recv()
        for k in (4, 5, 3):
            copy(k).start()
    elif stage == 2:
        copy(4).wait_recv()
        copy(6).start()
        copy(7).start()
        copy(5).wait_recv()
        copy(8).start()
    elif stage == 3:
        copy(6).wait_recv()
        copy(9).start()
    else:
        for k in (3, 7, 8, 9):
            copy(k).wait_recv()


GATHER_START = (
    [(0, 0), (1, 0), (2, 0), (3, 0)],
    [(0, 1), (5, 0), (6, 0), (7, 0), (8, 0), (4, 0)],
    [(0, 2), (1, 1), (2, 1), (3, 1), (0, 3), (0, 4), (1, 2), (5, 1)],
)
GATHER_PLAN = {
    1: [(6, 1), (1, 3), (2, 2), (3, 2)],
    2: [(1, 4), (7, 1), (5, 2), (8, 1)],
    3: [(6, 2), (4, 1), (2, 3), (3, 3)],
    4: [(2, 4), (7, 2)],
    5: [(8, 2), (5, 3)],
    6: [(3, 4), (4, 2), (6, 3), (5, 4)],
    7: [(7, 3), (8, 3), (4, 3), (6, 4)],
    8: [(4, 4), (7, 4), (8, 4)],
}


def scatter_copy(at, grad, part, sums, boxes, send, recv, k):
    z, core = at["z"], at["core"]
    if k == 0:
        src, dst, device = grad.at[:, :, 1 - core], sums, {"fsdp": z * 2 + 1 - core}
    elif k == 1:
        src, dst, device = part.at[at["diag"]], boxes.at[0], {"dp": at["second"]}
    elif k == 2:
        src, dst, device = part.at[at["second"]], boxes.at[1], {"dp": at["second"]}
    elif k == 3:
        src, dst, device = part.at[at["first"]], boxes.at[2], {"dp": at["first"]}
    else:
        there = (z + k - 3) % 4
        src, dst, device = part.at[at["dp"], there], boxes.at[3, k - 4], {"fsdp": there * 2 + core}
    return pltpu.make_async_remote_copy(
        src_ref=src, dst_ref=dst, send_sem=send.at[k], recv_sem=recv.at[k],
        device_id=device, device_id_type=MESH,
    )


def direct_copy(at, part, boxes, send, recv, i):
    dp, z = (at["dp"] + i // 4) % 4, (at["z"] + i % 4) % 4
    return pltpu.make_async_remote_copy(
        src_ref=part.at[dp, z], dst_ref=boxes.at[i - 1], send_sem=send.at[i - 1], recv_sem=recv.at[i - 1],
        device_id={"dp": dp, "fsdp": z * 2 + at["core"]}, device_id_type=MESH,
    )


def all_devices(at):
    inner = at["z"] * 2 + at["core"]
    return [{"dp": (at["dp"] + i // 8) % 4, "fsdp": (inner + i % 8) % 8} for i in range(1, 32)]


def add_low(left, right):
    return left + right


def scatter_stage(at, copy, mine, part, sums, boxes, stage):
    dp = at["dp"]
    if stage == 0:
        copy(0).start()
    elif stage == 1:
        copy(0).wait_recv()
        for name in ("diag", "second", "first", "dp"):
            part[at[name]] = add_low(mine(at[name]), sums[at[name]])
            if name == "diag":
                copy(1).start()
            if name == "second":
                copy(2).start()
    elif stage == 2:
        copy(1).wait_recv()
        part[at["first"]] = add_low(part[at["first"]], boxes[0])
        copy(3).start()
    elif stage == 3:
        copy(2).wait_recv()
        part[dp] = add_low(part[dp], boxes[1])
        copy(3).wait_recv()
        part[dp] = add_low(part[dp], boxes[2])
        for k in (4, 5, 6):
            copy(k).start()
    else:
        for k in (4, 5, 6):
            copy(k).wait_recv()


def scatter_total(at, part, boxes):
    total = part[at["dp"], at["z"]].astype(f32)
    for i in range(3):
        total = total + boxes[3, i].astype(f32)
    return total


SCATTER_PLAN = {
    0: [(0, 0), (1, 0), (2, 0), (3, 0), (4, 0)],
    1: [(0, 1), (1, 1), (2, 1)],
    2: [(3, 1), (0, 2)],
    3: [(5, 1), (1, 2), (2, 2), (4, 1)],
    4: [(3, 2), (0, 3)],
    5: [(5, 2), (6, 1), (4, 2), (1, 3), (2, 3)],
    6: [(7, 1), (3, 3), (5, 3)],
    7: [(6, 2), (4, 3), (7, 2), (0, 4), (1, 4)],
}


def spread_projection(omega_ref, wide_ref):
    wide_ref[...] = jnp.zeros_like(wide_ref)
    wide_ref[:HD, :FEAT] = omega_ref[0]
    wide_ref[HD:, FEAT:] = omega_ref[1]


def ones_projection(omega_ref, wide_ref):
    wide_ref[...] = jnp.ones_like(wide_ref)
    for odd in range(2):
        wide_ref[odd, odd * HD : (odd + 1) * HD, :] = omega_ref[odd]


def forward_step(
    block, starts_ref, lens_ref, normed, weight, wide_ref,
    qkv_ref, fq_ref, fk_ref, att_ref, o_ref, rden_ref, prefix_ref, state_ref,
):
    per_seg = SEG // BLOCK

    @pl.when(block % per_seg == 0)
    def _():
        begins = jnp.logical_or(block == 0, starts_ref[block // per_seg] != 0)
        state_ref[...] = jnp.where(begins, 0.0, state_ref[...])

    qkv_ref[0] = dot_nn(normed, weight).astype(bf16)
    position = lax.broadcasted_iota(jnp.int32, (BLOCK, 1), 0) + (block % per_seg) * BLOCK
    valid = (position < lens_ref[block // per_seg]).astype(f32)
    _, low = lane_masks(TILE)
    causal, _ = causal_masks()
    states = [state_ref[odd] for odd in range(2)]
    cuts = [slice(tile * TILE, (tile + 1) * TILE) for tile in range(TILES_BLOCK)]
    made, mixed = {}, {}

    def features(tile):
        at = cuts[tile]
        feats = []
        for part, feat_ref in enumerate((fq_ref, fk_ref)):
            rows = qkv_ref[0, at, part * DUO : (part + 1) * DUO]
            wide = rows.astype(f32)
            square = wide * wide
            proj = dot_nn(rows, wide_ref[...])
            for odd in range(2):
                total = jnp.sum(
                    jnp.where(low, 0.0, square) if odd else jnp.where(low, square, 0.0), axis=-1, keepdims=True
                )
                value = jnp.exp2(
                    proj[:, odd * FEAT : (odd + 1) * FEAT] * (feat_scale * log2_e)
                    - total * (0.5 * feat_scale * feat_scale * log2_e)
                )
                if part:
                    value = value * valid[at]
                value = value.astype(bf16)
                feat_ref[0, at, odd * FEAT : (odd + 1) * FEAT] = value
                feats.append(value)
        made[tile] = feats, with_ones(qkv_ref[0, at, 2 * DUO :], low)

    def scores(tile):
        feats, ones = made[tile]
        weights = [
            jnp.where(causal, dot_nt(feats[odd], feats[2 + odd]), 0.0).astype(bf16) for odd in range(2)
        ]
        for odd in range(2):
            att_ref[0, cuts[tile], odd * TILE : (odd + 1) * TILE] = weights[odd]
        sums = [dot_nn(ones[odd].T, feats[2 + odd]) for odd in range(2)]
        mixed[tile] = weights, sums

    def finish(tile):
        at = cuts[tile]
        (feats, ones), (weights, sums) = made[tile], mixed[tile]
        both = []
        for odd in range(2):
            before_low = states[odd].astype(bf16)
            prefix_ref[0, tile, odd] = before_low
            both.append(dot_nn(weights[odd], ones[odd]) + dot_nt(feats[odd], before_low))
            states[odd] = states[odd] + sums[odd]
        top = jnp.where(low, both[0], both[1])
        bottom = pltpu.roll(jnp.where(low, both[1], both[0]), HD, 1)
        o_ref[at, :] = (top / bottom).astype(bf16)
        rden_ref[0, at, :] = 1.0 / bottom

    for step in range(TILES_BLOCK + 2):
        if step < TILES_BLOCK:
            features(step)
        if 1 <= step <= TILES_BLOCK:
            scores(step - 1)
        if step >= 2:
            finish(step - 2)
    for odd in range(2):
        state_ref[odd] = states[odd]


def block_rows(block):
    return pl.ds(pl.multiple_of(block * BLOCK, BLOCK), BLOCK)


ATTENTION_STEPS = 8


def forward_local_kernel(
    starts_ref, lens_ref, x_ref, w_ref, gain_ref, omega_ref,
    qkv_ref, fq_ref, fk_ref, att_ref, o_ref, rden_ref, prefix_ref, normed_ref, state_ref, wide_ref,
):
    pair, block = pl.program_id(0), pl.program_id(1)
    rows = block_rows(block)

    @pl.when(pair == 0)
    def _():
        unit, _ = normalise(x_ref[rows, :].astype(f32))
        normed_ref[rows, :] = (unit * gain_ref[0:1, :]).astype(bf16)

    @pl.when(block == 0)
    def _():
        spread_projection(omega_ref, wide_ref)

    forward_step(
        block, starts_ref, lens_ref, normed_ref[rows, :], w_ref[...], wide_ref,
        qkv_ref, fq_ref, fk_ref, att_ref, o_ref, rden_ref, prefix_ref, state_ref,
    )


def forward_kernel(
    count_ref, starts_ref, lens_ref, x_ref, omega_ref, wq_ref, wo_ref, wu_ref, wd_ref, gains_ref, cot_ref,
    qkv_ref, fq_ref, fk_ref, att_ref, o_ref, rden_ref, prefix_ref, normed_ref, wpair_ref, gain_ref,
    out_ref, dmid_ref, do_ref, gwo_ref, gwu_ref, gwd_ref,
    state_ref, wide_ref, rows_ref, unit_ref, attended_ref,
    head_ref, held_ref, heldo_ref, heldu_ref, heldd_ref, pad_ref,
    awo_ref, awu_ref, awd_ref, norm_ref, normt_ref, dy_ref, send, recv, local,
):
    step = pl.program_id(0)
    blocks = ATTENTION_STEPS // PAIRS
    pair, block = step // blocks, step % blocks
    at = place()
    dp, z, core = at["dp"], at["z"], at["core"]
    full = [head_ref, held_ref.at[0], held_ref.at[1], held_ref.at[2], heldo_ref] + halves(heldu_ref, heldd_ref)
    own = [array.at[dp, z, core] for array in full]
    partners = near_devices(at)

    def copy(w, k):
        return gather_copy(at, own[w], full[w], send.at[w], recv.at[w], k)

    def leave(w):
        src = (heldo_ref, heldu_ref, heldd_ref)[w]
        return pltpu.make_async_copy(src, (gwo_ref, gwu_ref, gwd_ref)[w], local.at[w])

    def fetch():
        return pltpu.make_async_copy(x_ref, rows_ref, local.at[0])

    def stages(plan):
        for w, stage in plan:
            gather_stage(functools.partial(copy, w), stage)

    @pl.when(step == 0)
    def _():
        greet(partners)
        fetch().start()
        pad_ref[...] = jnp.zeros_like(pad_ref)
        pad_ref[0:2, 0:16] = gains_ref[...]
        flat = pad_ref[...]
        turned = flat
        for i in range(1, 8):
            turned = jnp.where(at["flat"] % 8 == i, pltpu.roll(flat, 16 * i, 1), turned)
        row = lax.broadcasted_iota(jnp.int32, (16, EXTRA), 0)
        band = at["flat"] // 8
        placed = jnp.where(row == band, turned[0:1, :], 0.0) + jnp.where(row == band + 4, turned[1:2, :], 0.0)
        for part in range(3):
            for i in range(PAIRS):
                piece = wq_ref[:, part * D + i * DUO : part * D + (i + 1) * DUO].astype(bf16)
                if i == 0:
                    head_ref[dp, z, core, :, part * DUO : (part + 1) * DUO] = piece
                else:
                    held_ref[i - 1, dp, z, core, :, part * DUO : (part + 1) * DUO] = piece
        head_ref[dp, z, core, :, CHUNK:] = placed.astype(bf16)
        greeted(partners)
        stages(GATHER_START[0])
        heldo_ref[dp, z, core] = wo_ref[...].astype(bf16)
        heldu_ref[dp, z, core] = wu_ref[...].astype(bf16)
        heldd_ref[dp, z, core] = wd_ref[...].astype(bf16)
        stages(GATHER_START[1])
        fetch().wait()

        @pl.loop(0, blocks)
        def _(i):
            unit_ref[block_rows(i), :] = normalise(rows_ref[block_rows(i), :].astype(f32))[0]

        stages(GATHER_START[2])
        packed = head_ref[..., CHUNK:].astype(f32)
        total = jnp.sum(packed.reshape(32, 16, EXTRA), axis=0)
        gain_ref[...] = jnp.zeros_like(gain_ref)
        for i in range(2):
            for j in range(4):
                gain_ref[i : i + 1, EXTRA * j : EXTRA * (j + 1)] = total[4 * i + j : 4 * i + j + 1, :]

    for when, plan in GATHER_PLAN.items():

        @pl.when(step == when)
        def _(plan=plan):
            stages(plan)

    for i in range(PAIRS):

        @pl.when(step == i * blocks)
        def _(i=i):
            piece = held_ref[i - 1] if i else head_ref[..., :CHUNK]
            wpair_ref[...] = piece.reshape(D, CHUNK)
            spread_projection(omega_ref, wide_ref)

    @pl.when(step < ATTENTION_STEPS)
    def _():
        rows = block_rows(block)

        @pl.when(pair == 0)
        def _():
            normed_ref[rows, :] = (unit_ref[rows, :] * gain_ref[0:1, :]).astype(bf16)

        forward_step(
            block, starts_ref, lens_ref, normed_ref[rows, :], wpair_ref[...], wide_ref,
            qkv_ref, fq_ref, fk_ref, att_ref, o_ref, rden_ref, prefix_ref, state_ref,
        )
        attended_ref[rows, pl.ds(pl.multiple_of(pair * DUO, DUO), DUO)] = o_ref[...]

    @pl.when(step >= ATTENTION_STEPS)
    def _():
        late = step - ATTENTION_STEPS
        rows = pl.ds(pl.multiple_of(late * FF_BLOCK, FF_BLOCK), FF_BLOCK)

        feed_forward_step(
            late, lens_ref, rows_ref[rows, :], attended_ref[rows, :], cot_ref[...],
            lambda: heldo_ref[...].reshape(D, D),
            lambda c: heldu_ref[..., c * FF_CHUNK : (c + 1) * FF_CHUNK].reshape(D, FF_CHUNK),
            lambda c: heldd_ref[c].reshape(FF_CHUNK, D), gain_ref[1:2, :],
            out_ref.at[rows], dmid_ref, do_ref, awo_ref, awu_ref, awd_ref, norm_ref, normt_ref, dy_ref,
        )

    @pl.when(step == pl.num_programs(0) - 1)
    def _():
        for w in range(9):
            for k in range(10):
                copy(w, k).wait_send()
        heldo_ref[...] = awo_ref[...].astype(bf16).reshape(heldo_ref.shape)
        leave(0).start()
        heldu_ref[...] = awu_ref[...].astype(bf16).reshape(heldu_ref.shape)
        leave(1).start()
        heldd_ref[...] = awd_ref[...].astype(bf16).reshape(heldd_ref.shape)
        leave(2).start()
        for w in range(3):
            leave(w).wait()


def normal_parts(hidden):
    inner = 0.5 + 0.5 * lax.erf(hidden * (0.5**0.5))
    return inner, jnp.exp2(hidden * hidden * (-0.5 * log2_e)) * (1.0 / math.sqrt(2.0 * math.pi))


def feed_forward_step(
    step, lens_ref, x, attended, cot, wo, wu, wd, gain,
    out_ref, dmid_ref, do_ref, awo_ref, awu_ref, awd_ref, norm_ref, normt_ref, dy_ref,
):
    @pl.when(step == 0)
    def _():
        awo_ref[...] = jnp.zeros_like(awo_ref)
        awu_ref[...] = jnp.zeros_like(awu_ref)
        awd_ref[...] = jnp.zeros_like(awd_ref)

    per_seg = SEG // FF_BLOCK
    halves_at = [slice(i * FF_PART, (i + 1) * FF_PART) for i in range(FF_BLOCK // FF_PART)]
    kept = {}

    def before(i):
        at = halves_at[i]
        position = lax.broadcasted_iota(jnp.int32, (FF_PART, 1), 0) + (step % per_seg) * FF_BLOCK + i * FF_PART
        valid = (position < lens_ref[step // per_seg]).astype(f32)
        dy_ref[at, :] = (cot[at].astype(f32) * valid).astype(bf16)
        middle = x[at].astype(f32) + dot_nn(attended[at], wo())
        unit, inverse = normalise(middle)
        normed = (unit * gain).astype(bf16)
        norm_ref[at, :] = normed
        normt_ref[:, at] = normed.T
        kept[i] = middle, unit, inverse

    def chunks(i):
        at = halves_at[i]
        total, unit, inverse = kept[i]
        back = 0.0
        for index in range(FF // FF_CHUNK):
            cut = slice(index * FF_CHUNK, (index + 1) * FF_CHUNK)
            up, down = wu(index), wd(index)
            hidden = dot_nn(norm_ref[at, :], up)
            inner, bell = normal_parts(hidden)
            active = (hidden * inner).astype(bf16)
            slope = inner + hidden * bell
            total = total + dot_nn(active, down)
            grad_hidden = (slope * dot_nt(dy_ref[at, :], down)).astype(bf16)
            awd_ref[cut, :] += dot_tn(active, dy_ref[at, :])
            awu_ref[:, cut] += dot_nn(normt_ref[:, at], grad_hidden)
            back = back + dot_nt(grad_hidden, up)
        out_ref[at, :] = total.astype(bf16)
        kept[i] = back, unit, inverse

    def after(i):
        at = halves_at[i]
        back, unit, inverse = kept[i]
        grad_middle = dy_ref[at, :].astype(f32) + normalise_back(back, gain, unit, inverse)
        dmid_ref[at, :] = grad_middle
        branch = grad_middle.astype(bf16)
        awo_ref[...] += dot_tn(attended[at], branch)
        do_ref[at, :] = dot_nt(branch, wo())

    before(0)
    for i in range(len(halves_at)):
        if i + 1 < len(halves_at):
            before(i + 1)
        chunks(i)
        if i:
            after(i - 1)
    after(len(halves_at) - 1)


def feed_forward_local_kernel(
    lens_ref, x_ref, o_ref, cot_ref, wo_ref, wu_ref, wd_ref, gain_ref,
    out_ref, dmid_ref, do_ref, gwo_ref, gwu_ref, gwd_ref,
    awo_ref, awu_ref, awd_ref, norm_ref, normt_ref, dy_ref,
):
    def chunk(index):
        return slice(index * FF_CHUNK, (index + 1) * FF_CHUNK)

    step = pl.program_id(0)
    feed_forward_step(
        step, lens_ref, x_ref[...], o_ref[...], cot_ref[...],
        lambda: wo_ref[...], lambda c: wu_ref[:, chunk(c)], lambda c: wd_ref[chunk(c), :], gain_ref[1:2, :],
        out_ref, dmid_ref, do_ref, awo_ref, awu_ref, awd_ref, norm_ref, normt_ref, dy_ref,
    )

    @pl.when(step == pl.num_programs(0) - 1)
    def _():
        gwo_ref[...] = awo_ref[...].astype(bf16)
        gwu_ref[...] = awu_ref[...].astype(bf16)
        gwd_ref[...] = awd_ref[...].astype(bf16)


def backward_step(
    block, blocks, starts_ref, qkv_ref, fq_ref, fk_ref, att_ref, o_ref, rden_ref, do_ref, prefix_ref, wide_ref,
    suffix_ref, store,
):
    per_seg = SEG // BLOCK

    @pl.when(block % per_seg == per_seg - 1)
    def _():
        after = jnp.minimum(block // per_seg + 1, blocks // per_seg - 1)
        ends = jnp.logical_or(block == blocks - 1, starts_ref[after] != 0)
        suffix_ref[...] = jnp.where(ends, 0.0, suffix_ref[...])

    lane, low = lane_masks(TILE)
    causal, anti = causal_masks()
    state_row = lax.broadcasted_iota(jnp.int32, (DUO, FEAT), 0)
    for tile in reversed(range(TILES_BLOCK)):
        at = slice(tile * TILE, (tile + 1) * TILE)
        scaled = do_ref[at, :] * rden_ref[0, at, :]
        product = scaled * o_ref[at, :].astype(f32)
        scaled = scaled.astype(bf16).astype(f32)
        ones = with_ones(qkv_ref[0, at, 2 * DUO :], low)
        back = [[], [], []]
        for odd in range(2):
            free = 0 if odd else HD
            mine = jnp.logical_not(low) if odd else low
            grad_den = -jnp.sum(jnp.where(mine, product, 0.0), axis=-1, keepdims=True)
            grad_one = jnp.where(mine, scaled, jnp.where(lane == free, grad_den, 0.0)).astype(bf16)
            query_feat = fq_ref[0, at, odd * FEAT : (odd + 1) * FEAT]
            key_feat = fk_ref[0, at, odd * FEAT : (odd + 1) * FEAT]
            one = ones[odd]
            after = suffix_ref[odd]
            edge = after[free : free + 1, :]
            rest = edge - edge.astype(bf16).astype(f32)
            after_low = jnp.where(state_row == free + 1, rest, after).astype(bf16)
            before_low = prefix_ref[0, tile, odd]
            weights = att_ref[0, at, odd * TILE : (odd + 1) * TILE]
            grad_w = jnp.where(causal, dot_nt(grad_one, one), 0.0).astype(bf16)
            grad_wt = jnp.where(anti, dot_nt(one, grad_one), 0.0).astype(bf16)
            grad_fq = dot_nn(grad_w, key_feat) + dot_nn(grad_one, before_low)
            grad_fk = dot_nn(grad_wt, query_feat) + dot_nn(one, after_low)
            back[2].append(dot_tn(weights, grad_one) + dot_nt(key_feat, after_low))
            suffix_ref[odd] = after + dot_tn(grad_one, query_feat)
            grad_pq = (grad_fq * query_feat.astype(f32)).astype(bf16)
            grad_pk = (grad_fk * key_feat.astype(f32)).astype(bf16)
            back[0].append(dot_nt(grad_pq, wide_ref[odd]))
            back[1].append(dot_nt(grad_pk, wide_ref[odd]))
        for part in range(2):
            top = jnp.where(low, back[part][0], back[part][1])
            bottom = pltpu.roll(jnp.where(low, back[part][1], back[part][0]), HD, 1)
            values = qkv_ref[0, at, part * DUO : (part + 1) * DUO].astype(f32)
            store(tile, part, top * feat_scale - bottom * (feat_scale * feat_scale) * values)
        store(tile, 2, jnp.where(low, back[2][0], back[2][1]))


def pair_lanes(pair):
    return pl.ds(pl.multiple_of(pair * CHUNK, CHUNK), CHUNK)


def store_into(dqkv_ref, pair, block):
    def store(tile, part, value):
        rows = pl.ds(pl.multiple_of(block * BLOCK + tile * TILE, TILE), TILE)
        lanes = pl.ds(pl.multiple_of(pair * CHUNK + part * DUO, DUO), DUO)
        dqkv_ref[rows, lanes] = value.astype(bf16)

    return store


def input_gradient(i, x_ref, dqkv_ref, weight_ref, gain, dmid_ref):
    rows = pl.ds(pl.multiple_of(i * TILE, TILE), TILE)
    grad_normed = dot_nt(dqkv_ref[rows, :], weight_ref[...])
    unit, inverse = normalise(x_ref[rows, :].astype(f32))
    dmid_ref[rows, :] = dmid_ref[rows, :] + normalise_back(grad_normed, gain, unit, inverse)
    return rows


def backward_local_kernel(
    starts_ref, normed_ref, qkv_ref, fq_ref, fk_ref, att_ref, o_ref, rden_ref, do_ref, prefix_ref, omega_ref, gain_ref,
    x_ref, dmid_in_ref, weight_ref,
    gin_ref, gw_ref,
    suffix_ref, wide_ref, dqkv_ref, rowsn_ref,
):
    pair, step = pl.program_id(0), pl.program_id(1)
    blocks = pl.num_programs(1)
    block = blocks - 1 - step

    @pl.when(step == 0)
    def _():
        ones_projection(omega_ref, wide_ref)

    @pl.when(pair == 0)
    def _():
        rowsn_ref[block_rows(block), :] = normed_ref[...]

    backward_step(
        block, blocks, starts_ref, qkv_ref, fq_ref, fk_ref, att_ref, o_ref, rden_ref, do_ref, prefix_ref, wide_ref,
        suffix_ref, store_into(dqkv_ref, pair, block),
    )

    @pl.when(step == blocks - 1)
    def _():
        gw_ref[...] = dot_tn(rowsn_ref[...], dqkv_ref[:, pair_lanes(pair)]).astype(bf16)

    @pl.when(jnp.logical_and(step == blocks - 1, pair == PAIRS - 1))
    def _():
        gin_ref[...] = dmid_in_ref[...]

        @pl.loop(0, blocks * TILES_BLOCK)
        def _(i):
            input_gradient(i, x_ref, dqkv_ref, weight_ref, gain_ref[0:1, :], gin_ref)


def eye_row(column):
    row = lax.broadcasted_iota(jnp.int32, (16, 16), 0)
    lane = lax.broadcasted_iota(jnp.int32, (16, 16), 1)
    return jnp.sum(jnp.where(row == lane, column, 0.0), axis=0, keepdims=True)


def row_squares(value):
    return jnp.sum(value * value, axis=-1, keepdims=True).sum(axis=0, keepdims=True)


def backward_kernel(
    starts_ref, normed_ref, qkv_ref, fq_ref, fk_ref, att_ref, o_ref, rden_ref, do_ref, prefix_ref, omega_ref, gain_ref,
    wq_ref, wu_ref, own_gain_ref, x_ref, dmid_ref, weight_ref, go_ref, gu_ref, gd_ref,
    gin_ref, ro_ref, ru_ref, rd_ref, rq_ref, rg_ref, norm_ref,
    suffix_ref, wide_ref, dqkv_ref, rowsn_ref, gq_ref,
    rows_ref, held_ref,
    po_ref, pu_ref, pd_ref, pq_ref, so_ref, su_ref, sd_ref, sq_ref, bo_ref, bu_ref, bd_ref, bq_ref,
    last_ref, near_ref, send, recv, local, last_send, last_recv, near_send, near_recv,
):
    pair, inner_step = pl.program_id(0), pl.program_id(1)
    blocks = pl.num_programs(1)
    block = blocks - 1 - inner_step
    step = pair * blocks + inner_step
    at = place()
    dp, z, core = at["dp"], at["z"], at["core"]
    grads = [go_ref] + halves(gu_ref, gd_ref) + [gq_ref.at[i] for i in range(PAIRS)]

    def each(out, up, down, pairs):
        return [out, up.at[0], up.at[1], down.at[0], down.at[1]] + [pairs.at[i] for i in range(PAIRS)]

    parts = each(po_ref, pu_ref, pd_ref, pq_ref)
    sums = each(so_ref, su_ref, sd_ref, sq_ref)
    boxes = each(bo_ref, bu_ref, bd_ref, bq_ref)
    results = [ro_ref, ru_ref.at[:, : FF // 2], ru_ref.at[:, FF // 2 :], rd_ref.at[:32], rd_ref.at[32:]]
    results += [rq_ref.at[i] for i in range(PAIRS)]
    others = all_devices(at)

    def copy(w, k):
        return scatter_copy(at, grads[w], parts[w], sums[w], boxes[w], send.at[w], recv.at[w], k)

    def keep(w):
        return pltpu.make_async_copy(grads[w].at[:, :, core], parts[w], local.at[w])

    def late(i):
        src = (x_ref, dmid_ref, weight_ref)[i]
        dst = (rows_ref, gin_ref, held_ref)[i]
        return pltpu.make_async_copy(src, dst, local.at[5 + i])

    def stages(plan):
        for w, stage in plan:
            if w < 5:
                if stage == 0:
                    keep(w).start()
                if stage == 1:
                    keep(w).wait()
                mine = lambda index, w=w: parts[w][index]
            else:
                mine = lambda index, w=w: gq_ref[w - 5, index, :, core]
            scatter_stage(at, functools.partial(copy, w), mine, parts[w], sums[w], boxes[w], stage)
            if stage == 4:
                results[w][...] = scatter_total(at, parts[w], boxes[w])

    @pl.when(step == 0)
    def _():
        greet(others)
        for i in range(3):
            late(i).start()

    @pl.when(step == 0)
    def _():
        greeted(others)

    for when, plan in SCATTER_PLAN.items():

        @pl.when(step == when)
        def _(plan=plan):
            stages(plan)

    @pl.when(inner_step == 0)
    def _():
        ones_projection(omega_ref, wide_ref)

    @pl.when(pair == 0)
    def _():
        rowsn_ref[block_rows(block), :] = normed_ref[...]

    backward_step(
        block, blocks, starts_ref, qkv_ref, fq_ref, fk_ref, att_ref, o_ref, rden_ref, do_ref, prefix_ref, wide_ref,
        suffix_ref, store_into(dqkv_ref, pair, block),
    )

    for i in range(PAIRS):

        @pl.when(step == (i + 1) * blocks - 1)
        def _(i=i):
            grad = dot_tn(rowsn_ref[...], dqkv_ref[:, i * CHUNK : (i + 1) * CHUNK]).astype(bf16)
            gq_ref[i] = grad.reshape(4, 4, 2, 16, CHUNK)
            stages([(5 + i, 0)])

    @pl.when(step == PAIRS * blocks - 1)
    def _():
        for i in range(3):
            late(i).wait()
        tiles = blocks * TILES_BLOCK

        def inputs_part(first, last):
            @pl.loop(first * tiles // 8, last * tiles // 8)
            def _(i):
                input_gradient(i, rows_ref, dqkv_ref, held_ref, gain_ref[0:1, :], gin_ref)

        def last(i):
            return direct_copy(at, parts[8], last_ref, last_send, last_recv, i)

        stages([(6, 3), (7, 3)])
        inputs_part(0, 1)
        copy(8, 0).wait_recv()
        for i in range(4):
            index = (dp + i) % 4
            parts[8][index] = add_low(gq_ref[3, index, :, core], sums[8][index])
            for j in range(4):
                if i + j:
                    last(4 * i + j).start()
        inputs_part(1, 5)
        stages([(2, 4), (3, 4), (5, 4), (4, 4), (6, 4), (7, 4)])
        inputs_part(5, 8)
        early = row_squares(ro_ref[...]) + row_squares(ru_ref[...]) + row_squares(rd_ref[...])
        for i in range(PAIRS - 1):
            early = early + row_squares(rq_ref[i])
        up_low = wu_ref[...].astype(bf16).astype(f32)
        gain_low = own_gain_ref[...].astype(bf16).astype(f32)
        second = eye_row(jnp.sum(ru_ref[...] * up_low, axis=-1, keepdims=True)) / gain_low[1:2, :]
        total = parts[8][dp, z].astype(f32)
        for i in range(1, 16):
            last(i).wait_recv()
            total = total + last_ref[i - 1].astype(f32)
        rq_ref[3] = total
        first = jnp.zeros((16, 1), f32)
        for i in range(PAIRS):
            for part in range(3):
                low_w = wq_ref[:, part * D + i * DUO : part * D + (i + 1) * DUO].astype(bf16).astype(f32)
                first = first + jnp.sum(
                    rq_ref[i, :, part * DUO : (part + 1) * DUO] * low_w, axis=-1, keepdims=True
                )
        first = eye_row(first) / gain_low[0:1, :]
        rg_ref[0:1, :] = first
        rg_ref[1:2, :] = second
        squares = early + row_squares(rq_ref[PAIRS - 1]) + row_squares(first) + row_squares(second)
        mine = near_ref.at[at["flat"]]
        mine[...] = jnp.broadcast_to(squares, (8, 128))

        def near(i):
            return pltpu.make_async_remote_copy(
                src_ref=mine, dst_ref=mine, send_sem=near_send.at[i], recv_sem=near_recv.at[i],
                device_id=others[i], device_id_type=MESH,
            )

        for i in range(31):
            near(i).start()
        for i in range(31):
            near(i).wait_recv()
        group = near_ref[0]
        for i in range(1, 32):
            group = group + near_ref[i]
        norm_ref[...] = group

        for i in range(31):
            near(i).wait_send()
        for i in range(1, 16):
            last(i).wait_send()
        copy(8, 0).wait_send()
        for w in range(8):
            for k in range(7):
                copy(w, k).wait_send()


def update_kernel(
    count_ref, total_ref, rq_ref, ro_ref, ru_ref, rd_ref, rg_ref,
    wq_ref, wo_ref, wu_ref, wd_ref, wg_ref, mq_ref, mo_ref, mu_ref, md_ref, mg_ref,
    vq_ref, vo_ref, vu_ref, vd_ref, vg_ref, gin_ref, out_ref,
    norm_ref, gq_ref, nvq_ref, nwq_ref, go_ref, nvo_ref, nwo_ref, gu_ref, nvu_ref, nwu_ref,
    gd_ref, nvd_ref, nwd_ref, gg_ref, nvg_ref, nwg_ref, gin_out_ref, out_out_ref, sem,
):
    pieces = 8
    height = gin_ref.shape[0] // pieces
    moves = []
    for i in range(pieces):
        rows = pl.ds(i * height, height)
        for j, (src, dst) in enumerate(((gin_ref, gin_out_ref), (out_ref, out_out_ref))):
            moves.append(pltpu.make_async_copy(src.at[rows], dst.at[rows], sem.at[j, i]))
    for move in moves:
        move.start()
    update_weights(
        count_ref, total_ref, rq_ref, ro_ref, ru_ref, rd_ref, rg_ref,
        wq_ref, wo_ref, wu_ref, wd_ref, wg_ref, mq_ref, mo_ref, mu_ref, md_ref, mg_ref,
        vq_ref, vo_ref, vu_ref, vd_ref, vg_ref,
        norm_ref, gq_ref, nvq_ref, nwq_ref, go_ref, nvo_ref, nwo_ref, gu_ref, nvu_ref, nwu_ref,
        gd_ref, nvd_ref, nwd_ref, gg_ref, nvg_ref, nwg_ref,
    )
    for move in moves:
        move.wait()


def update_weights(
    count_ref, total_ref, rq_ref, ro_ref, ru_ref, rd_ref, rg_ref,
    wq_ref, wo_ref, wu_ref, wd_ref, wg_ref, mq_ref, mo_ref, mu_ref, md_ref, mg_ref,
    vq_ref, vo_ref, vu_ref, vd_ref, vg_ref,
    norm_ref, gq_ref, nvq_ref, nwq_ref, go_ref, nvo_ref, nwo_ref, gu_ref, nvu_ref, nwu_ref,
    gd_ref, nvd_ref, nwd_ref, gg_ref, nvg_ref, nwg_ref,
):
    norm = jnp.sqrt(total_ref[0:1, 0:1])
    norm_ref[...] = norm
    factor = jnp.minimum(1.0, clip_level / norm)
    count = jnp.full((1, 1), count_ref[0], jnp.int32).astype(f32)
    first_fix = 1.0 - jnp.exp2(count * math.log2(beta_first))
    second_fix = 1.0 - jnp.exp2(count * math.log2(beta_second))

    def update(grad, at, weight, first, second, rate, outs):
        clipped = grad * factor
        first_new = beta_first * first[at] + (1.0 - beta_first) * clipped
        second_new = beta_second * second[at] + (1.0 - beta_second) * clipped * clipped
        direction = first_new / first_fix / (jnp.sqrt(second_new / second_fix) + adam_eps)
        outs[0][at] = clipped
        outs[1][at] = second_new
        outs[2][at] = weight[at] - rate * (direction + decay_weight * weight[at])

    for part in range(3):
        for i in range(PAIRS):
            at = (slice(None), slice(part * D + i * DUO, part * D + (i + 1) * DUO))
            grad = rq_ref[i, :, part * DUO : (part + 1) * DUO]
            update(grad, at, wq_ref, mq_ref, vq_ref, rate_matrix, (gq_ref, nvq_ref, nwq_ref))
    update(ro_ref[...], ..., wo_ref, mo_ref, vo_ref, rate_matrix, (go_ref, nvo_ref, nwo_ref))
    update(ru_ref[...], ..., wu_ref, mu_ref, vu_ref, rate_matrix, (gu_ref, nvu_ref, nwu_ref))
    update(rd_ref[...], ..., wd_ref, md_ref, vd_ref, rate_matrix, (gd_ref, nvd_ref, nwd_ref))
    update(rg_ref[...], ..., wg_ref, mg_ref, vg_ref, rate_gain, (gg_ref, nvg_ref, nwg_ref))


ROWS = {"pair": 16, "out": 16, "up": 16, "down": 64}
COLS = {"pair": CHUNK, "out": D, "up": FF, "down": D}
LATE = ("out", "up", "down")
smem = pl.BlockSpec(memory_space=pltpu.SMEM)
hbm = pl.BlockSpec(memory_space=pl.ANY)
vmem = pl.BlockSpec(memory_space=pltpu.VMEM)


def shaped(shape, dtype):
    return jax.ShapeDtypeStruct(shape, dtype)


def params(collective_id=None, mib=63):
    if collective_id is None:
        return pltpu.CompilerParams(vmem_limit_bytes=mib << 20)
    return pltpu.CompilerParams(vmem_limit_bytes=mib << 20, collective_id=collective_id, has_side_effects=True)


def whole(shape):
    return pl.BlockSpec(shape, lambda *_: (0,) * len(shape), pipeline_mode=pl.Buffered(1))


def whole_out(shape):
    return pl.BlockSpec(shape, lambda *_: (0,) * len(shape))


def five(name):
    return (4, 4, 2, ROWS[name], COLS[name])


def forward_outs(tokens):
    tiles = tokens // TILE
    specs = [
        pl.BlockSpec((1, BLOCK, CHUNK), lambda p, b: (p, b, 0)),
        pl.BlockSpec((1, BLOCK, 2 * FEAT), lambda p, b: (p, b, 0)),
        pl.BlockSpec((1, BLOCK, 2 * FEAT), lambda p, b: (p, b, 0)),
        pl.BlockSpec((1, BLOCK, 2 * TILE), lambda p, b: (p, b, 0)),
        pl.BlockSpec((BLOCK, DUO), lambda p, b: (b, p)),
        pl.BlockSpec((1, BLOCK, DUO), lambda p, b: (p, b, 0)),
        pl.BlockSpec((1, TILES_BLOCK, 2, DUO, FEAT), lambda p, b: (p, b, 0, 0, 0)),
        whole_out((tokens, D)),
    ]
    shapes = [
        shaped((PAIRS, tokens, CHUNK), bf16),
        shaped((PAIRS, tokens, 2 * FEAT), bf16),
        shaped((PAIRS, tokens, 2 * FEAT), bf16),
        shaped((PAIRS, tokens, 2 * TILE), bf16),
        shaped((tokens, D), bf16),
        shaped((PAIRS, tokens, DUO), f32),
        shaped((PAIRS, tiles, 2, DUO, FEAT), bf16),
        shaped((tokens, D), bf16),
    ]
    scratch = [pltpu.VMEM((2, DUO, FEAT), f32), pltpu.VMEM((DUO, 2 * FEAT), bf16)]
    return specs, shapes, scratch


pair_omega = pl.BlockSpec((2, HD, FEAT), lambda p, b: (p, 0, 0))
pair_weight = pl.BlockSpec((D, CHUNK), lambda p, b: (0, p))


def forward_local(starts, lens, x, weight, gains, omega):
    tokens = x.shape[0]
    specs, shapes, scratch = forward_outs(tokens)
    return pl.pallas_call(
        forward_local_kernel,
        grid=(PAIRS, tokens // BLOCK),
        in_specs=[smem, smem, whole((tokens, D)), pair_weight, whole((8, D)), pair_omega],
        out_specs=specs,
        out_shape=shapes,
        scratch_shapes=scratch,
        compiler_params=params(),
    )(starts, lens, x, weight, gains, omega)


def forward(count, starts, lens, x, omega, wq, wo, wu, wd, gains, cot):
    tokens = x.shape[0]
    blocks = tokens // BLOCK
    steps = PAIRS * blocks
    specs, shapes, scratch = forward_outs(tokens)

    def early(index_map):
        return lambda i: index_map(
            jnp.minimum(i // blocks, PAIRS - 1), jnp.where(i < steps, i % blocks, blocks - 1)
        )

    specs = [pl.BlockSpec(spec.block_shape, early(spec.index_map)) for spec in specs]
    weight = pl.BlockSpec(pair_weight.block_shape, early(pair_weight.index_map))
    heads = pl.BlockSpec(pair_omega.block_shape, early(pair_omega.index_map))
    rows = pl.BlockSpec((FF_BLOCK, D), lambda i: (jnp.maximum(i - steps, 0), 0))
    return pl.pallas_call(
        forward_kernel,
        grid=(steps + tokens // FF_BLOCK,),
        in_specs=[smem, smem, smem, hbm, heads] + [whole(array.shape) for array in (wq, wo, wu, wd, gains)] + [rows],
        out_specs=specs + [weight, whole_out((8, D)), vmem, rows, rows, hbm, hbm, hbm],
        out_shape=shapes
        + [shaped((D, WIDE), bf16), shaped((8, D), f32)]
        + [pltpu.VMEM((tokens, D), bf16), shaped((tokens, D), f32), shaped((tokens, D), f32)]
        + [shaped(five(name), bf16) for name in LATE],
        scratch_shapes=scratch
        + [
            pltpu.VMEM((tokens, D), bf16),
            pltpu.VMEM((tokens, D), f32),
            pltpu.VMEM((tokens, D), bf16),
            pltpu.VMEM((4, 4, 2, 16, CHUNK + EXTRA), bf16),
            pltpu.VMEM((PAIRS - 1, *five("pair")), bf16),
        ]
        + [pltpu.VMEM(five(name), bf16) for name in LATE]
        + [pltpu.VMEM((8, EXTRA), f32)]
        + feed_forward_scratch()
        + [
            pltpu.SemaphoreType.DMA((9, 10)),
            pltpu.SemaphoreType.DMA((9, 10)),
            pltpu.SemaphoreType.DMA((3,)),
        ],
        compiler_params=params(0, FORWARD_MIB),
    )(count, starts, lens, x, omega, wq, wo, wu, wd, gains, cot)


def feed_forward_scratch():
    return [
        pltpu.VMEM((D, D), f32), pltpu.VMEM((D, FF), f32), pltpu.VMEM((FF, D), f32),
        pltpu.VMEM((FF_BLOCK, D), bf16), pltpu.VMEM((D, FF_BLOCK), bf16), pltpu.VMEM((FF_BLOCK, D), bf16),
    ]


def feed_forward_local(lens, x, o, cot, wo, wu, wd, gains):
    tokens = x.shape[0]
    rows = pl.BlockSpec((FF_BLOCK, D), lambda i: (i, 0))
    return pl.pallas_call(
        feed_forward_local_kernel,
        grid=(tokens // FF_BLOCK,),
        in_specs=[smem, rows, rows, rows, whole((D, D)), whole((D, FF)), whole((FF, D)), whole((8, D))],
        out_specs=[rows, rows, rows, whole_out((D, D)), whole_out((D, FF)), whole_out((FF, D))],
        out_shape=[
            shaped((tokens, D), bf16),
            shaped((tokens, D), f32),
            shaped((tokens, D), f32),
            shaped((D, D), bf16),
            shaped((D, FF), bf16),
            shaped((FF, D), bf16),
        ],
        scratch_shapes=feed_forward_scratch(),
        compiler_params=params(),
    )(lens, x, o, cot, wo, wu, wd, gains)


def backward_ins(blocks):
    last = blocks - 1
    return [
        smem,
        pl.BlockSpec((BLOCK, D), lambda p, b: (jnp.where(p == 0, last - b, 0), 0)),
        pl.BlockSpec((1, BLOCK, CHUNK), lambda p, b: (p, last - b, 0)),
        pl.BlockSpec((1, BLOCK, 2 * FEAT), lambda p, b: (p, last - b, 0)),
        pl.BlockSpec((1, BLOCK, 2 * FEAT), lambda p, b: (p, last - b, 0)),
        pl.BlockSpec((1, BLOCK, 2 * TILE), lambda p, b: (p, last - b, 0)),
        pl.BlockSpec((BLOCK, DUO), lambda p, b: (last - b, p)),
        pl.BlockSpec((1, BLOCK, DUO), lambda p, b: (p, last - b, 0)),
        pl.BlockSpec((BLOCK, DUO), lambda p, b: (last - b, p)),
        pl.BlockSpec((1, TILES_BLOCK, 2, DUO, FEAT), lambda p, b: (p, last - b, 0, 0, 0)),
        pair_omega,
        whole((8, D)),
    ]


def backward_scratch(tokens):
    return [
        pltpu.VMEM((2, DUO, FEAT), f32),
        pltpu.VMEM((2, DUO, FEAT), bf16),
        pltpu.VMEM((tokens, WIDE), bf16),
        pltpu.VMEM((tokens, D), bf16),
    ]


def backward_local(args, x, dmid, weight):
    tokens = x.shape[0]
    return pl.pallas_call(
        backward_local_kernel,
        grid=(PAIRS, tokens // BLOCK),
        in_specs=backward_ins(tokens // BLOCK) + [whole((tokens, D)), whole((tokens, D)), whole((D, WIDE))],
        out_specs=[whole_out((tokens, D)), pair_weight],
        out_shape=[shaped((tokens, D), f32), shaped((D, WIDE), bf16)],
        scratch_shapes=backward_scratch(tokens),
        compiler_params=params(),
    )(*args, x, dmid, weight)


def backward(args, wq, wu, gains, x, dmid, weight, grads):
    tokens = x.shape[0]
    half = [(4, 4, 16, D), (2, 4, 4, 16, FF // 2), (2, 4, 4, 32, D), (PAIRS, 4, 4, 16, CHUNK)]
    dma = pltpu.SemaphoreType.DMA
    return pl.pallas_call(
        backward_kernel,
        grid=(PAIRS, tokens // BLOCK),
        in_specs=backward_ins(tokens // BLOCK) + [whole(wq.shape), whole(wu.shape), whole(gains.shape)] + [hbm] * 6,
        out_specs=[vmem] * 7,
        out_shape=[pltpu.VMEM((tokens, D), f32)]
        + [pltpu.VMEM((ROWS[name], COLS[name]), f32) for name in LATE]
        + [pltpu.VMEM((PAIRS, 16, CHUNK), f32), pltpu.VMEM((2, 16), f32), pltpu.VMEM((8, 128), f32)],
        scratch_shapes=backward_scratch(tokens)
        + [pltpu.VMEM((PAIRS, *five("pair")), bf16)]
        + [pltpu.VMEM((tokens, D), bf16), pltpu.VMEM((D, WIDE), bf16)]
        + [pltpu.VMEM(shape, bf16) for shape in half] * 3
        + [pltpu.VMEM((15, 16, CHUNK), bf16), pltpu.VMEM((32, 8, 128), f32)]
        + [dma((9, 7)), dma((9, 7)), dma((8,)), dma((15,)), dma((15,)), dma((31,)), dma((31,))],
        compiler_params=params(1, BACKWARD_MIB),
    )(*args, wq, wu, gains, x, dmid, weight, *grads)


def update_all(count, total, grads, weights, firsts, seconds, grad_inputs, out_rows):
    shapes = [shaped((1, 1), f32)]
    for weight in weights:
        shapes += [shaped(weight.shape, f32)] * 3
    return pl.pallas_call(
        update_kernel,
        in_specs=[smem] + [vmem] * 23,
        out_specs=[vmem] * 16 + [hbm, hbm],
        out_shape=shapes + [shaped(grad_inputs.shape, f32), shaped(out_rows.shape, bf16)],
        scratch_shapes=[pltpu.SemaphoreType.DMA((2, 8))],
        compiler_params=params(mib=UPDATE_MIB),
    )(count, total, *grads, *weights, *firsts, *seconds, grad_inputs, out_rows)


def to_pairs(weight):
    split = weight.reshape(weight.shape[0], 3, PAIRS, DUO)
    return jnp.swapaxes(split, 1, 2).reshape(weight.shape)


def from_pairs(weight):
    split = weight.reshape(weight.shape[0], PAIRS, 3, DUO)
    return jnp.swapaxes(split, 1, 2).reshape(weight.shape)


def on_device(
    sizes, inputs, cotangent, feature_omega, seg_start, seg_len, step_count,
    w_qkv, w_out, w_up, w_down, gains,
    m_qkv, m_out, m_up, m_down, m_gains,
    v_qkv, v_out, v_up, v_down, v_gains,
):
    weights = (w_qkv, w_out, w_up, w_down, gains)
    firsts = (m_qkv, m_out, m_up, m_down, m_gains)
    seconds = (v_qkv, v_out, v_up, v_down, v_gains)
    if sizes == (4, 8):
        count = step_count.reshape(1)
        (qkv, fq, fk, weights_kept, attended, rden, prefix, normed, qkv_full, gain_full, out_rows, dmid, grad_attended,
         *grads) = forward(count, seg_start, seg_len, inputs, feature_omega, *weights, cotangent)
        grad_inputs, r_out, r_up, r_down, r_qkv, r_gains, total = backward(
            (seg_start, normed, qkv, fq, fk, weights_kept, attended, rden, grad_attended, prefix, feature_omega, gain_full),
            w_qkv, w_up, gains, inputs, dmid, qkv_full, grads,
        )
        norm, *updated, grad_inputs, out_rows = update_all(
            count, total, (r_qkv, r_out, r_up, r_down, r_gains), weights, firsts, seconds, grad_inputs, out_rows
        )
        return (out_rows, grad_inputs, norm.reshape(()), *updated)

    def gather(piece, axis=0):
        return lax.all_gather(piece.astype(bf16), AXES, axis=axis, tiled=True)

    qkv_full, out_full, up_full, down_full = (gather(piece) for piece in weights[:4])
    qkv_full = to_pairs(qkv_full)
    gain_full = jnp.pad(gather(gains, 1).astype(f32), ((0, 6), (0, 0)))
    qkv, fq, fk, weights_kept, attended, rden, prefix, normed = forward_local(
        seg_start, seg_len, inputs, qkv_full, gain_full, feature_omega
    )
    out_rows, dmid, grad_attended, grad_out, grad_up, grad_down = feed_forward_local(
        seg_len, inputs, attended, cotangent, out_full, up_full, down_full, gain_full
    )
    grad_inputs, grad_qkv = backward_local(
        (seg_start, normed, qkv, fq, fk, weights_kept, attended, rden, grad_attended, prefix, feature_omega, gain_full),
        inputs, dmid, qkv_full,
    )

    def scatter(piece):
        return lax.psum_scatter(piece.astype(f32), AXES, scatter_dimension=0, tiled=True)

    reduced = [scatter(piece) for piece in (from_pairs(grad_qkv), grad_out, grad_up, grad_down)]
    low = [weight.astype(bf16).astype(f32) for weight in weights]
    first = jnp.sum(reduced[0] * low[0], axis=1) / low[4][0]
    second = jnp.sum(reduced[2] * low[2], axis=1) / low[4][1]
    reduced.append(jnp.stack([first, second], axis=0))
    grad_norm = jnp.sqrt(lax.psum(sum(jnp.sum(piece * piece) for piece in reduced), AXES))
    factor = jnp.minimum(1.0, clip_level / grad_norm)
    count = step_count.astype(f32)
    first_fix = 1.0 - jnp.power(beta_first, count)
    second_fix = 1.0 - jnp.power(beta_second, count)
    updated = []
    rates = (rate_matrix,) * 4 + (rate_gain,)
    for weight, first, second, gradient, rate in zip(weights, firsts, seconds, reduced, rates):
        clipped = gradient * factor
        first_new = beta_first * first + (1.0 - beta_first) * clipped
        second_new = beta_second * second + (1.0 - beta_second) * clipped * clipped
        direction = first_new / first_fix / (jnp.sqrt(second_new / second_fix) + adam_eps)
        updated += [clipped, second_new, weight - rate * (direction + decay_weight * weight)]
    return (out_rows, grad_inputs, grad_norm, *updated)


def solution(mesh):
    return jax.shard_map(
        functools.partial(on_device, tuple(mesh.shape[name] for name in AXES)),
        mesh=mesh,
        in_specs=(
            P(("dp", "fsdp"), None),
            P(("dp", "fsdp"), None),
            P(),
            P(("dp", "fsdp")),
            P(("dp", "fsdp")),
            P(),
            P(("dp", "fsdp"), None),
            P(("dp", "fsdp"), None),
            P(("dp", "fsdp"), None),
            P(("dp", "fsdp"), None),
            P(None, ("dp", "fsdp")),
            P(("dp", "fsdp"), None),
            P(("dp", "fsdp"), None),
            P(("dp", "fsdp"), None),
            P(("dp", "fsdp"), None),
            P(None, ("dp", "fsdp")),
            P(("dp", "fsdp"), None),
            P(("dp", "fsdp"), None),
            P(("dp", "fsdp"), None),
            P(("dp", "fsdp"), None),
            P(None, ("dp", "fsdp")),
        ),
        out_specs=(
            P(("dp", "fsdp"), None),
            P(("dp", "fsdp"), None),
            P(),
            P(("dp", "fsdp"), None),
            P(("dp", "fsdp"), None),
            P(("dp", "fsdp"), None),
            P(("dp", "fsdp"), None),
            P(("dp", "fsdp"), None),
            P(("dp", "fsdp"), None),
            P(("dp", "fsdp"), None),
            P(("dp", "fsdp"), None),
            P(("dp", "fsdp"), None),
            P(("dp", "fsdp"), None),
            P(("dp", "fsdp"), None),
            P(("dp", "fsdp"), None),
            P(None, ("dp", "fsdp")),
            P(None, ("dp", "fsdp")),
            P(None, ("dp", "fsdp")),
        ),
        check_vma=False,
    )
```

```python
import functools
import math

import jax
import jax.numpy as jnp
from jax import lax
from jax.experimental import pallas as pl
from jax.experimental.pallas import tpu as pltpu
from jax.sharding import PartitionSpec as P

D = 512
HEADS = 8
HD = 64
FEAT = 256
FF = 2048
SEG = 1024
TILE = 256
PAIRS = HEADS // 2
DUO = 2 * HD
BLOCK = 1024
TILES_BLOCK = BLOCK // TILE
FORWARD_MIB = 61
BACKWARD_MIB = 52
UPDATE_MIB = 20
FF_BLOCK = 1024
FF_PART = 512
FF_CHUNK = 512
WIDE = 3 * D
CHUNK = 3 * DUO
EXTRA = 128
AXES = ("dp", "fsdp")

norm_eps = 1e-05
clip_level = 1.0
rate_matrix = 0.03
rate_gain = 0.4
beta_first = 0.9
beta_second = 0.95
adam_eps = 1e-08
decay_weight = 0.1

feat_scale = HD ** (-0.25)
log2_e = math.log2(math.e)
f32 = jnp.float32
bf16 = jnp.bfloat16
MESH = pl.DeviceIdType.MESH


def dot_nn(a, b):
    return lax.dot_general(a, b, (((1,), (0,)), ((), ())), preferred_element_type=f32)


def dot_nt(a, b):
    return lax.dot_general(a, b, (((1,), (1,)), ((), ())), preferred_element_type=f32)


def dot_tn(a, b):
    return lax.dot_general(a, b, (((0,), (0,)), ((), ())), preferred_element_type=f32)


def normalise(rows):
    centred = rows - jnp.mean(rows, axis=-1, keepdims=True)
    spread = jnp.mean(centred * centred, axis=-1, keepdims=True)
    inverse = lax.rsqrt(spread + norm_eps)
    return centred * inverse, inverse


def normalise_back(grad, gain, unit, inverse):
    scaled = grad * gain
    first = jnp.mean(scaled, axis=-1, keepdims=True)
    second = jnp.mean(scaled * unit, axis=-1, keepdims=True)
    return inverse * (scaled - first - unit * second)


def lane_masks(rows):
    lane = lax.broadcasted_iota(jnp.int32, (rows, DUO), 1)
    return lane, lane < HD


def causal_masks():
    row = lax.broadcasted_iota(jnp.int32, (TILE, TILE), 0)
    col = lax.broadcasted_iota(jnp.int32, (TILE, TILE), 1)
    return row >= col, row <= col


def with_ones(value_pair, low):
    wide = value_pair.astype(f32)
    return (
        jnp.where(low, wide, 1.0).astype(bf16),
        jnp.where(low, 1.0, wide).astype(bf16),
    )


def place():
    dp, inner = lax.axis_index("dp"), lax.axis_index("fsdp")
    z, core = inner // 2, inner % 2
    y, x = dp // 2, dp % 2
    across = y * 2 + (1 - x)
    along = (1 - y) * 2 + x
    return {
        "dp": dp, "z": z, "core": core, "flat": dp * 8 + inner,
        "first": core * along + (1 - core) * across,
        "second": core * across + (1 - core) * along,
        "diag": (1 - y) * 2 + (1 - x),
    }


def greet(devices):
    barrier = pltpu.get_barrier_semaphore()
    for device in devices:
        pl.semaphore_signal(barrier, inc=1, device_id=device, device_id_type=MESH)


def greeted(devices):
    pl.semaphore_wait(pltpu.get_barrier_semaphore(), len(devices))


def near_devices(at):
    devices = [{"fsdp": (at["z"] + i) % 4 * 2 + at["core"]} for i in range(1, 4)]
    devices += [{"fsdp": at["z"] * 2 + 1 - at["core"]}]
    devices += [{"dp": at["first"]}, {"dp": at["second"]}]
    return devices


def halves(up, down):
    return [up.at[..., i * (FF // 2) : (i + 1) * (FF // 2)] for i in range(2)] + [
        down.at[:, :, :, i * 32 : (i + 1) * 32, :] for i in range(2)
    ]


def gather_copy(at, own, full, send, recv, k):
    dp, z, core = at["dp"], at["z"], at["core"]
    sibling = {"fsdp": z * 2 + 1 - core}
    if k < 3:
        src, dst, device = own, full.at[dp, z, core], {"fsdp": (z + 1 + k) % 4 * 2 + core}
    else:
        which = {3: "dp", 4: "dp", 5: "dp", 6: "first", 7: "first", 8: "second", 9: "diag"}[k]
        src = dst = full.at[at[which], :, core]
        device = {4: {"dp": at["first"]}, 5: {"dp": at["second"]}, 6: {"dp": at["second"]}}.get(k, sibling)
    return pltpu.make_async_remote_copy(
        src_ref=src, dst_ref=dst, send_sem=send.at[k], recv_sem=recv.at[k],
        device_id=device, device_id_type=MESH,
    )


def gather_stage(copy, stage):
    if stage == 0:
        for k in range(3):
            copy(k).start()
    elif stage == 1:
        for k in range(3):
            copy(k).wait_recv()
        for k in (4, 5, 3):
            copy(k).start()
    elif stage == 2:
        copy(4).wait_recv()
        copy(6).start()
        copy(7).start()
        copy(5).wait_recv()
        copy(8).start()
    elif stage == 3:
        copy(6).wait_recv()
        copy(9).start()
    else:
        for k in (3, 7, 8, 9):
            copy(k).wait_recv()


GATHER_START = (
    [(0, 0), (1, 0), (2, 0), (3, 0)],
    [(0, 1), (5, 0), (6, 0), (7, 0), (8, 0), (4, 0)],
    [(0, 2), (1, 1), (2, 1), (3, 1), (0, 3), (0, 4), (1, 2), (5, 1)],
)
GATHER_PLAN = {
    1: [(6, 1), (1, 3), (2, 2), (3, 2)],
    2: [(1, 4), (7, 1), (5, 2), (8, 1)],
    3: [(6, 2), (4, 1), (2, 3), (3, 3)],
    4: [(2, 4), (7, 2)],
    5: [(8, 2), (5, 3)],
    6: [(3, 4), (4, 2), (6, 3), (5, 4)],
    7: [(7, 3), (8, 3), (4, 3), (6, 4)],
    8: [(4, 4), (7, 4), (8, 4)],
}


def scatter_copy(at, grad, part, sums, boxes, send, recv, k):
    z, core = at["z"], at["core"]
    if k == 0:
        src, dst, device = grad.at[:, :, 1 - core], sums, {"fsdp": z * 2 + 1 - core}
    elif k == 1:
        src, dst, device = part.at[at["diag"]], boxes.at[0], {"dp": at["second"]}
    elif k == 2:
        src, dst, device = part.at[at["second"]], boxes.at[1], {"dp": at["second"]}
    elif k == 3:
        src, dst, device = part.at[at["first"]], boxes.at[2], {"dp": at["first"]}
    else:
        there = (z + k - 3) % 4
        src, dst, device = part.at[at["dp"], there], boxes.at[3, k - 4], {"fsdp": there * 2 + core}
    return pltpu.make_async_remote_copy(
        src_ref=src, dst_ref=dst, send_sem=send.at[k], recv_sem=recv.at[k],
        device_id=device, device_id_type=MESH,
    )


def direct_copy(at, part, boxes, send, recv, i):
    dp, z = (at["dp"] + i // 4) % 4, (at["z"] + i % 4) % 4
    return pltpu.make_async_remote_copy(
        src_ref=part.at[dp, z], dst_ref=boxes.at[i - 1], send_sem=send.at[i - 1], recv_sem=recv.at[i - 1],
        device_id={"dp": dp, "fsdp": z * 2 + at["core"]}, device_id_type=MESH,
    )


def all_devices(at):
    inner = at["z"] * 2 + at["core"]
    return [{"dp": (at["dp"] + i // 8) % 4, "fsdp": (inner + i % 8) % 8} for i in range(1, 32)]


def add_low(left, right):
    return left + right


def scatter_stage(at, copy, mine, part, sums, boxes, stage):
    dp = at["dp"]
    if stage == 0:
        copy(0).start()
    elif stage == 1:
        copy(0).wait_recv()
        for name in ("diag", "second", "first", "dp"):
            part[at[name]] = add_low(mine(at[name]), sums[at[name]])
            if name == "diag":
                copy(1).start()
            if name == "second":
                copy(2).start()
    elif stage == 2:
        copy(1).wait_recv()
        part[at["first"]] = add_low(part[at["first"]], boxes[0])
        copy(3).start()
    elif stage == 3:
        copy(2).wait_recv()
        part[dp] = add_low(part[dp], boxes[1])
        copy(3).wait_recv()
        part[dp] = add_low(part[dp], boxes[2])
        for k in (4, 5, 6):
            copy(k).start()
    else:
        for k in (4, 5, 6):
            copy(k).wait_recv()


def scatter_total(at, part, boxes):
    total = part[at["dp"], at["z"]].astype(f32)
    for i in range(3):
        total = total + boxes[3, i].astype(f32)
    return total


SCATTER_PLAN = {
    0: [(0, 0), (1, 0), (2, 0), (3, 0), (4, 0)],
    1: [(0, 1), (1, 1), (2, 1)],
    2: [(3, 1), (0, 2)],
    3: [(5, 1), (1, 2), (2, 2), (4, 1)],
    4: [(3, 2), (0, 3)],
    5: [(5, 2), (6, 1), (4, 2), (1, 3), (2, 3)],
    6: [(7, 1), (3, 3), (5, 3)],
    7: [(6, 2), (4, 3), (7, 2), (0, 4), (1, 4)],
}


def spread_projection(omega_ref, wide_ref):
    wide_ref[...] = jnp.zeros_like(wide_ref)
    wide_ref[:HD, :FEAT] = omega_ref[0]
    wide_ref[HD:, FEAT:] = omega_ref[1]


def ones_projection(omega_ref, wide_ref):
    wide_ref[...] = jnp.ones_like(wide_ref)
    for odd in range(2):
        wide_ref[odd, odd * HD : (odd + 1) * HD, :] = omega_ref[odd]


def forward_step(
    block, starts_ref, lens_ref, normed, weight, wide_ref,
    qkv_ref, fq_ref, fk_ref, att_ref, o_ref, rden_ref, prefix_ref, state_ref,
):
    per_seg = SEG // BLOCK

    @pl.when(block % per_seg == 0)
    def _():
        begins = jnp.logical_or(block == 0, starts_ref[block // per_seg] != 0)
        state_ref[...] = jnp.where(begins, 0.0, state_ref[...])

    qkv_ref[0] = dot_nn(normed, weight).astype(bf16)
    position = lax.broadcasted_iota(jnp.int32, (BLOCK, 1), 0) + (block % per_seg) * BLOCK
    valid = (position < lens_ref[block // per_seg]).astype(f32)
    _, low = lane_masks(TILE)
    causal, _ = causal_masks()
    states = [state_ref[odd] for odd in range(2)]
    cuts = [slice(tile * TILE, (tile + 1) * TILE) for tile in range(TILES_BLOCK)]
    made, mixed = {}, {}

    def features(tile):
        at = cuts[tile]
        feats = []
        for part, feat_ref in enumerate((fq_ref, fk_ref)):
            rows = qkv_ref[0, at, part * DUO : (part + 1) * DUO]
            wide = rows.astype(f32)
            square = wide * wide
            proj = dot_nn(rows, wide_ref[...])
            for odd in range(2):
                total = jnp.sum(
                    jnp.where(low, 0.0, square) if odd else jnp.where(low, square, 0.0), axis=-1, keepdims=True
                )
                value = jnp.exp2(
                    proj[:, odd * FEAT : (odd + 1) * FEAT] * (feat_scale * log2_e)
                    - total * (0.5 * feat_scale * feat_scale * log2_e)
                )
                if part:
                    value = value * valid[at]
                value = value.astype(bf16)
                feat_ref[0, at, odd * FEAT : (odd + 1) * FEAT] = value
                feats.append(value)
        made[tile] = feats, with_ones(qkv_ref[0, at, 2 * DUO :], low)

    def scores(tile):
        feats, ones = made[tile]
        weights = [
            jnp.where(causal, dot_nt(feats[odd], feats[2 + odd]), 0.0).astype(bf16) for odd in range(2)
        ]
        for odd in range(2):
            att_ref[0, cuts[tile], odd * TILE : (odd + 1) * TILE] = weights[odd]
        sums = [dot_nn(ones[odd].T, feats[2 + odd]) for odd in range(2)]
        mixed[tile] = weights, sums

    def finish(tile):
        at = cuts[tile]
        (feats, ones), (weights, sums) = made[tile], mixed[tile]
        both = []
        for odd in range(2):
            before_low = states[odd].astype(bf16)
            prefix_ref[0, tile, odd] = before_low
            both.append(dot_nn(weights[odd], ones[odd]) + dot_nt(feats[odd], before_low))
            states[odd] = states[odd] + sums[odd]
        top = jnp.where(low, both[0], both[1])
        bottom = pltpu.roll(jnp.where(low, both[1], both[0]), HD, 1)
        o_ref[at, :] = (top / bottom).astype(bf16)
        rden_ref[0, at, :] = 1.0 / bottom

    for step in range(TILES_BLOCK + 2):
        if step < TILES_BLOCK:
            features(step)
        if 1 <= step <= TILES_BLOCK:
            scores(step - 1)
        if step >= 2:
            finish(step - 2)
    for odd in range(2):
        state_ref[odd] = states[odd]


def block_rows(block):
    return pl.ds(pl.multiple_of(block * BLOCK, BLOCK), BLOCK)


ATTENTION_STEPS = 8


def forward_local_kernel(
    starts_ref, lens_ref, x_ref, w_ref, gain_ref, omega_ref,
    qkv_ref, fq_ref, fk_ref, att_ref, o_ref, rden_ref, prefix_ref, normed_ref, state_ref, wide_ref,
):
    pair, block = pl.program_id(0), pl.program_id(1)
    rows = block_rows(block)

    @pl.when(pair == 0)
    def _():
        unit, _ = normalise(x_ref[rows, :].astype(f32))
        normed_ref[rows, :] = (unit * gain_ref[0:1, :]).astype(bf16)

    @pl.when(block == 0)
    def _():
        spread_projection(omega_ref, wide_ref)

    forward_step(
        block, starts_ref, lens_ref, normed_ref[rows, :], w_ref[...], wide_ref,
        qkv_ref, fq_ref, fk_ref, att_ref, o_ref, rden_ref, prefix_ref, state_ref,
    )


def forward_kernel(
    count_ref, starts_ref, lens_ref, x_ref, omega_ref, wq_ref, wo_ref, wu_ref, wd_ref, gains_ref, cot_ref,
    qkv_ref, fq_ref, fk_ref, att_ref, o_ref, rden_ref, prefix_ref, normed_ref, wpair_ref, gain_ref,
    out_ref, dmid_ref, do_ref, gwo_ref, gwu_ref, gwd_ref,
    state_ref, wide_ref, rows_ref, unit_ref, attended_ref,
    head_ref, held_ref, heldo_ref, heldu_ref, heldd_ref, pad_ref,
    awo_ref, awu_ref, awd_ref, norm_ref, normt_ref, dy_ref, send, recv, local,
):
    step = pl.program_id(0)
    blocks = ATTENTION_STEPS // PAIRS
    pair, block = step // blocks, step % blocks
    at = place()
    dp, z, core = at["dp"], at["z"], at["core"]
    full = [head_ref, held_ref.at[0], held_ref.at[1], held_ref.at[2], heldo_ref] + halves(heldu_ref, heldd_ref)
    own = [array.at[dp, z, core] for array in full]
    partners = near_devices(at)

    def copy(w, k):
        return gather_copy(at, own[w], full[w], send.at[w], recv.at[w], k)

    def leave(w):
        src = (heldo_ref, heldu_ref, heldd_ref)[w]
        return pltpu.make_async_copy(src, (gwo_ref, gwu_ref, gwd_ref)[w], local.at[w])

    def fetch():
        return pltpu.make_async_copy(x_ref, rows_ref, local.at[0])

    def stages(plan):
        for w, stage in plan:
            gather_stage(functools.partial(copy, w), stage)

    @pl.when(step == 0)
    def _():
        greet(partners)
        fetch().start()
        pad_ref[...] = jnp.zeros_like(pad_ref)
        pad_ref[0:2, 0:16] = gains_ref[...]
        flat = pad_ref[...]
        turned = flat
        for i in range(1, 8):
            turned = jnp.where(at["flat"] % 8 == i, pltpu.roll(flat, 16 * i, 1), turned)
        row = lax.broadcasted_iota(jnp.int32, (16, EXTRA), 0)
        band = at["flat"] // 8
        placed = jnp.where(row == band, turned[0:1, :], 0.0) + jnp.where(row == band + 4, turned[1:2, :], 0.0)
        for part in range(3):
            for i in range(PAIRS):
                piece = wq_ref[:, part * D + i * DUO : part * D + (i + 1) * DUO].astype(bf16)
                if i == 0:
                    head_ref[dp, z, core, :, part * DUO : (part + 1) * DUO] = piece
                else:
                    held_ref[i - 1, dp, z, core, :, part * DUO : (part + 1) * DUO] = piece
        head_ref[dp, z, core, :, CHUNK:] = placed.astype(bf16)
        greeted(partners)
        stages(GATHER_START[0])
        heldo_ref[dp, z, core] = wo_ref[...].astype(bf16)
        heldu_ref[dp, z, core] = wu_ref[...].astype(bf16)
        heldd_ref[dp, z, core] = wd_ref[...].astype(bf16)
        stages(GATHER_START[1])
        fetch().wait()

        @pl.loop(0, blocks)
        def _(i):
            unit_ref[block_rows(i), :] = normalise(rows_ref[block_rows(i), :].astype(f32))[0]

        stages(GATHER_START[2])
        packed = head_ref[..., CHUNK:].astype(f32)
        total = jnp.sum(packed.reshape(32, 16, EXTRA), axis=0)
        gain_ref[...] = jnp.zeros_like(gain_ref)
        for i in range(2):
            for j in range(4):
                gain_ref[i : i + 1, EXTRA * j : EXTRA * (j + 1)] = total[4 * i + j : 4 * i + j + 1, :]

    for when, plan in GATHER_PLAN.items():

        @pl.when(step == when)
        def _(plan=plan):
            stages(plan)

    for i in range(PAIRS):

        @pl.when(step == i * blocks)
        def _(i=i):
            piece = held_ref[i - 1] if i else head_ref[..., :CHUNK]
            wpair_ref[...] = piece.reshape(D, CHUNK)
            spread_projection(omega_ref, wide_ref)

    @pl.when(step < ATTENTION_STEPS)
    def _():
        rows = block_rows(block)

        @pl.when(pair == 0)
        def _():
            normed_ref[rows, :] = (unit_ref[rows, :] * gain_ref[0:1, :]).astype(bf16)

        forward_step(
            block, starts_ref, lens_ref, normed_ref[rows, :], wpair_ref[...], wide_ref,
            qkv_ref, fq_ref, fk_ref, att_ref, o_ref, rden_ref, prefix_ref, state_ref,
        )
        attended_ref[rows, pl.ds(pl.multiple_of(pair * DUO, DUO), DUO)] = o_ref[...]

    @pl.when(step >= ATTENTION_STEPS)
    def _():
        late = step - ATTENTION_STEPS
        rows = pl.ds(pl.multiple_of(late * FF_BLOCK, FF_BLOCK), FF_BLOCK)

        feed_forward_step(
            late, lens_ref, rows_ref[rows, :], attended_ref[rows, :], cot_ref[...],
            lambda: heldo_ref[...].reshape(D, D),
            lambda c: heldu_ref[..., c * FF_CHUNK : (c + 1) * FF_CHUNK].reshape(D, FF_CHUNK),
            lambda c: heldd_ref[c].reshape(FF_CHUNK, D), gain_ref[1:2, :],
            out_ref.at[rows], dmid_ref, do_ref, awo_ref, awu_ref, awd_ref, norm_ref, normt_ref, dy_ref,
        )

    @pl.when(step == pl.num_programs(0) - 1)
    def _():
        for w in range(9):
            for k in range(10):
                copy(w, k).wait_send()
        heldo_ref[...] = awo_ref[...].astype(bf16).reshape(heldo_ref.shape)
        leave(0).start()
        heldu_ref[...] = awu_ref[...].astype(bf16).reshape(heldu_ref.shape)
        leave(1).start()
        heldd_ref[...] = awd_ref[...].astype(bf16).reshape(heldd_ref.shape)
        leave(2).start()
        for w in range(3):
            leave(w).wait()


def normal_parts(hidden):
    inner = 0.5 + 0.5 * lax.erf(hidden * (0.5**0.5))
    return inner, jnp.exp2(hidden * hidden * (-0.5 * log2_e)) * (1.0 / math.sqrt(2.0 * math.pi))


def feed_forward_step(
    step, lens_ref, x, attended, cot, wo, wu, wd, gain,
    out_ref, dmid_ref, do_ref, awo_ref, awu_ref, awd_ref, norm_ref, normt_ref, dy_ref,
):
    @pl.when(step == 0)
    def _():
        awo_ref[...] = jnp.zeros_like(awo_ref)
        awu_ref[...] = jnp.zeros_like(awu_ref)
        awd_ref[...] = jnp.zeros_like(awd_ref)

    per_seg = SEG // FF_BLOCK
    halves_at = [slice(i * FF_PART, (i + 1) * FF_PART) for i in range(FF_BLOCK // FF_PART)]
    kept = {}

    def before(i):
        at = halves_at[i]
        position = lax.broadcasted_iota(jnp.int32, (FF_PART, 1), 0) + (step % per_seg) * FF_BLOCK + i * FF_PART
        valid = (position < lens_ref[step // per_seg]).astype(f32)
        dy_ref[at, :] = (cot[at].astype(f32) * valid).astype(bf16)
        middle = x[at].astype(f32) + dot_nn(attended[at], wo())
        unit, inverse = normalise(middle)
        normed = (unit * gain).astype(bf16)
        norm_ref[at, :] = normed
        normt_ref[:, at] = normed.T
        kept[i] = middle, unit, inverse

    def chunks(i):
        at = halves_at[i]
        total, unit, inverse = kept[i]
        back = 0.0
        for index in range(FF // FF_CHUNK):
            cut = slice(index * FF_CHUNK, (index + 1) * FF_CHUNK)
            up, down = wu(index), wd(index)
            hidden = dot_nn(norm_ref[at, :], up)
            inner, bell = normal_parts(hidden)
            active = (hidden * inner).astype(bf16)
            slope = inner + hidden * bell
            total = total + dot_nn(active, down)
            grad_hidden = (slope * dot_nt(dy_ref[at, :], down)).astype(bf16)
            awd_ref[cut, :] += dot_tn(active, dy_ref[at, :])
            awu_ref[:, cut] += dot_nn(normt_ref[:, at], grad_hidden)
            back = back + dot_nt(grad_hidden, up)
        out_ref[at, :] = total.astype(bf16)
        kept[i] = back, unit, inverse

    def after(i):
        at = halves_at[i]
        back, unit, inverse = kept[i]
        grad_middle = dy_ref[at, :].astype(f32) + normalise_back(back, gain, unit, inverse)
        dmid_ref[at, :] = grad_middle
        branch = grad_middle.astype(bf16)
        awo_ref[...] += dot_tn(attended[at], branch)
        do_ref[at, :] = dot_nt(branch, wo())

    before(0)
    for i in range(len(halves_at)):
        if i + 1 < len(halves_at):
            before(i + 1)
        chunks(i)
        if i:
            after(i - 1)
    after(len(halves_at) - 1)


def feed_forward_local_kernel(
    lens_ref, x_ref, o_ref, cot_ref, wo_ref, wu_ref, wd_ref, gain_ref,
    out_ref, dmid_ref, do_ref, gwo_ref, gwu_ref, gwd_ref,
    awo_ref, awu_ref, awd_ref, norm_ref, normt_ref, dy_ref,
):
    def chunk(index):
        return slice(index * FF_CHUNK, (index + 1) * FF_CHUNK)

    step = pl.program_id(0)
    feed_forward_step(
        step, lens_ref, x_ref[...], o_ref[...], cot_ref[...],
        lambda: wo_ref[...], lambda c: wu_ref[:, chunk(c)], lambda c: wd_ref[chunk(c), :], gain_ref[1:2, :],
        out_ref, dmid_ref, do_ref, awo_ref, awu_ref, awd_ref, norm_ref, normt_ref, dy_ref,
    )

    @pl.when(step == pl.num_programs(0) - 1)
    def _():
        gwo_ref[...] = awo_ref[...].astype(bf16)
        gwu_ref[...] = awu_ref[...].astype(bf16)
        gwd_ref[...] = awd_ref[...].astype(bf16)


def backward_step(
    block, blocks, starts_ref, qkv_ref, fq_ref, fk_ref, att_ref, o_ref, rden_ref, do_ref, prefix_ref, wide_ref,
    suffix_ref, store,
):
    per_seg = SEG // BLOCK

    @pl.when(block % per_seg == per_seg - 1)
    def _():
        after = jnp.minimum(block // per_seg + 1, blocks // per_seg - 1)
        ends = jnp.logical_or(block == blocks - 1, starts_ref[after] != 0)
        suffix_ref[...] = jnp.where(ends, 0.0, suffix_ref[...])

    lane, low = lane_masks(TILE)
    causal, anti = causal_masks()
    state_row = lax.broadcasted_iota(jnp.int32, (DUO, FEAT), 0)
    for tile in reversed(range(TILES_BLOCK)):
        at = slice(tile * TILE, (tile + 1) * TILE)
        scaled = do_ref[at, :] * rden_ref[0, at, :]
        product = scaled * o_ref[at, :].astype(f32)
        scaled = scaled.astype(bf16).astype(f32)
        ones = with_ones(qkv_ref[0, at, 2 * DUO :], low)
        back = [[], [], []]
        for odd in range(2):
            free = 0 if odd else HD
            mine = jnp.logical_not(low) if odd else low
            grad_den = -jnp.sum(jnp.where(mine, product, 0.0), axis=-1, keepdims=True)
            grad_one = jnp.where(mine, scaled, jnp.where(lane == free, grad_den, 0.0)).astype(bf16)
            query_feat = fq_ref[0, at, odd * FEAT : (odd + 1) * FEAT]
            key_feat = fk_ref[0, at, odd * FEAT : (odd + 1) * FEAT]
            one = ones[odd]
            after = suffix_ref[odd]
            edge = after[free : free + 1, :]
            rest = edge - edge.astype(bf16).astype(f32)
            after_low = jnp.where(state_row == free + 1, rest, after).astype(bf16)
            before_low = prefix_ref[0, tile, odd]
            weights = att_ref[0, at, odd * TILE : (odd + 1) * TILE]
            grad_w = jnp.where(causal, dot_nt(grad_one, one), 0.0).astype(bf16)
            grad_wt = jnp.where(anti, dot_nt(one, grad_one), 0.0).astype(bf16)
            grad_fq = dot_nn(grad_w, key_feat) + dot_nn(grad_one, before_low)
            grad_fk = dot_nn(grad_wt, query_feat) + dot_nn(one, after_low)
            back[2].append(dot_tn(weights, grad_one) + dot_nt(key_feat, after_low))
            suffix_ref[odd] = after + dot_tn(grad_one, query_feat)
            grad_pq = (grad_fq * query_feat.astype(f32)).astype(bf16)
            grad_pk = (grad_fk * key_feat.astype(f32)).astype(bf16)
            back[0].append(dot_nt(grad_pq, wide_ref[odd]))
            back[1].append(dot_nt(grad_pk, wide_ref[odd]))
        for part in range(2):
            top = jnp.where(low, back[part][0], back[part][1])
            bottom = pltpu.roll(jnp.where(low, back[part][1], back[part][0]), HD, 1)
            values = qkv_ref[0, at, part * DUO : (part + 1) * DUO].astype(f32)
            store(tile, part, top * feat_scale - bottom * (feat_scale * feat_scale) * values)
        store(tile, 2, jnp.where(low, back[2][0], back[2][1]))


def pair_lanes(pair):
    return pl.ds(pl.multiple_of(pair * CHUNK, CHUNK), CHUNK)


def store_into(dqkv_ref, pair, block):
    def store(tile, part, value):
        rows = pl.ds(pl.multiple_of(block * BLOCK + tile * TILE, TILE), TILE)
        lanes = pl.ds(pl.multiple_of(pair * CHUNK + part * DUO, DUO), DUO)
        dqkv_ref[rows, lanes] = value.astype(bf16)

    return store


def input_gradient(i, x_ref, dqkv_ref, weight_ref, gain, dmid_ref):
    rows = pl.ds(pl.multiple_of(i * TILE, TILE), TILE)
    grad_normed = dot_nt(dqkv_ref[rows, :], weight_ref[...])
    unit, inverse = normalise(x_ref[rows, :].astype(f32))
    dmid_ref[rows, :] = dmid_ref[rows, :] + normalise_back(grad_normed, gain, unit, inverse)
    return rows


def backward_local_kernel(
    starts_ref, normed_ref, qkv_ref, fq_ref, fk_ref, att_ref, o_ref, rden_ref, do_ref, prefix_ref, omega_ref, gain_ref,
    x_ref, dmid_in_ref, weight_ref,
    gin_ref, gw_ref,
    suffix_ref, wide_ref, dqkv_ref, rowsn_ref,
):
    pair, step = pl.program_id(0), pl.program_id(1)
    blocks = pl.num_programs(1)
    block = blocks - 1 - step

    @pl.when(step == 0)
    def _():
        ones_projection(omega_ref, wide_ref)

    @pl.when(pair == 0)
    def _():
        rowsn_ref[block_rows(block), :] = normed_ref[...]

    backward_step(
        block, blocks, starts_ref, qkv_ref, fq_ref, fk_ref, att_ref, o_ref, rden_ref, do_ref, prefix_ref, wide_ref,
        suffix_ref, store_into(dqkv_ref, pair, block),
    )

    @pl.when(step == blocks - 1)
    def _():
        gw_ref[...] = dot_tn(rowsn_ref[...], dqkv_ref[:, pair_lanes(pair)]).astype(bf16)

    @pl.when(jnp.logical_and(step == blocks - 1, pair == PAIRS - 1))
    def _():
        gin_ref[...] = dmid_in_ref[...]

        @pl.loop(0, blocks * TILES_BLOCK)
        def _(i):
            input_gradient(i, x_ref, dqkv_ref, weight_ref, gain_ref[0:1, :], gin_ref)


def eye_row(column):
    row = lax.broadcasted_iota(jnp.int32, (16, 16), 0)
    lane = lax.broadcasted_iota(jnp.int32, (16, 16), 1)
    return jnp.sum(jnp.where(row == lane, column, 0.0), axis=0, keepdims=True)


def row_squares(value):
    return jnp.sum(value * value, axis=-1, keepdims=True).sum(axis=0, keepdims=True)


def backward_kernel(
    starts_ref, normed_ref, qkv_ref, fq_ref, fk_ref, att_ref, o_ref, rden_ref, do_ref, prefix_ref, omega_ref, gain_ref,
    wq_ref, wu_ref, own_gain_ref, x_ref, dmid_ref, weight_ref, go_ref, gu_ref, gd_ref,
    gin_ref, ro_ref, ru_ref, rd_ref, rq_ref, rg_ref, norm_ref,
    suffix_ref, wide_ref, dqkv_ref, rowsn_ref, gq_ref,
    rows_ref, held_ref,
    po_ref, pu_ref, pd_ref, pq_ref, so_ref, su_ref, sd_ref, sq_ref, bo_ref, bu_ref, bd_ref, bq_ref,
    last_ref, near_ref, send, recv, local, last_send, last_recv, near_send, near_recv,
):
    pair, inner_step = pl.program_id(0), pl.program_id(1)
    blocks = pl.num_programs(1)
    block = blocks - 1 - inner_step
    step = pair * blocks + inner_step
    at = place()
    dp, z, core = at["dp"], at["z"], at["core"]
    grads = [go_ref] + halves(gu_ref, gd_ref) + [gq_ref.at[i] for i in range(PAIRS)]

    def each(out, up, down, pairs):
        return [out, up.at[0], up.at[1], down.at[0], down.at[1]] + [pairs.at[i] for i in range(PAIRS)]

    parts = each(po_ref, pu_ref, pd_ref, pq_ref)
    sums = each(so_ref, su_ref, sd_ref, sq_ref)
    boxes = each(bo_ref, bu_ref, bd_ref, bq_ref)
    results = [ro_ref, ru_ref.at[:, : FF // 2], ru_ref.at[:, FF // 2 :], rd_ref.at[:32], rd_ref.at[32:]]
    results += [rq_ref.at[i] for i in range(PAIRS)]
    others = all_devices(at)

    def copy(w, k):
        return scatter_copy(at, grads[w], parts[w], sums[w], boxes[w], send.at[w], recv.at[w], k)

    def keep(w):
        return pltpu.make_async_copy(grads[w].at[:, :, core], parts[w], local.at[w])

    def late(i):
        src = (x_ref, dmid_ref, weight_ref)[i]
        dst = (rows_ref, gin_ref, held_ref)[i]
        return pltpu.make_async_copy(src, dst, local.at[5 + i])

    def stages(plan):
        for w, stage in plan:
            if w < 5:
                if stage == 0:
                    keep(w).start()
                if stage == 1:
                    keep(w).wait()
                mine = lambda index, w=w: parts[w][index]
            else:
                mine = lambda index, w=w: gq_ref[w - 5, index, :, core]
            scatter_stage(at, functools.partial(copy, w), mine, parts[w], sums[w], boxes[w], stage)
            if stage == 4:
                results[w][...] = scatter_total(at, parts[w], boxes[w])

    @pl.when(step == 0)
    def _():
        greet(others)

    @pl.when(step == 3)
    def _():
        for i in range(3):
            late(i).start()

    @pl.when(step == 0)
    def _():
        greeted(others)

    for when, plan in SCATTER_PLAN.items():

        @pl.when(step == when)
        def _(plan=plan):
            stages(plan)

    @pl.when(inner_step == 0)
    def _():
        ones_projection(omega_ref, wide_ref)

    @pl.when(pair == 0)
    def _():
        rowsn_ref[block_rows(block), :] = normed_ref[...]

    backward_step(
        block, blocks, starts_ref, qkv_ref, fq_ref, fk_ref, att_ref, o_ref, rden_ref, do_ref, prefix_ref, wide_ref,
        suffix_ref, store_into(dqkv_ref, pair, block),
    )

    for i in range(PAIRS):

        @pl.when(step == (i + 1) * blocks - 1)
        def _(i=i):
            grad = dot_tn(rowsn_ref[...], dqkv_ref[:, i * CHUNK : (i + 1) * CHUNK]).astype(bf16)
            gq_ref[i] = grad.reshape(4, 4, 2, 16, CHUNK)
            stages([(5 + i, 0)])

    @pl.when(step == PAIRS * blocks - 1)
    def _():
        for i in range(3):
            late(i).wait()
        tiles = blocks * TILES_BLOCK

        def inputs_part(first, last):
            @pl.loop(first * tiles // 8, last * tiles // 8)
            def _(i):
                input_gradient(i, rows_ref, dqkv_ref, held_ref, gain_ref[0:1, :], gin_ref)

        def last(i):
            return direct_copy(at, parts[8], last_ref, last_send, last_recv, i)

        stages([(6, 3), (7, 3)])
        inputs_part(0, 1)
        copy(8, 0).wait_recv()
        for i in range(4):
            index = (dp + i) % 4
            parts[8][index] = add_low(gq_ref[3, index, :, core], sums[8][index])
            for j in range(4):
                if i + j:
                    last(4 * i + j).start()
        inputs_part(1, 5)
        stages([(2, 4), (3, 4), (5, 4), (4, 4), (6, 4), (7, 4)])
        inputs_part(5, 8)
        early = row_squares(ro_ref[...]) + row_squares(ru_ref[...]) + row_squares(rd_ref[...])
        for i in range(PAIRS - 1):
            early = early + row_squares(rq_ref[i])
        up_low = wu_ref[...].astype(bf16).astype(f32)
        gain_low = own_gain_ref[...].astype(bf16).astype(f32)
        second = eye_row(jnp.sum(ru_ref[...] * up_low, axis=-1, keepdims=True)) / gain_low[1:2, :]
        total = parts[8][dp, z].astype(f32)
        for i in range(1, 16):
            last(i).wait_recv()
            total = total + last_ref[i - 1].astype(f32)
        rq_ref[3] = total
        first = jnp.zeros((16, 1), f32)
        for i in range(PAIRS):
            for part in range(3):
                low_w = wq_ref[:, part * D + i * DUO : part * D + (i + 1) * DUO].astype(bf16).astype(f32)
                first = first + jnp.sum(
                    rq_ref[i, :, part * DUO : (part + 1) * DUO] * low_w, axis=-1, keepdims=True
                )
        first = eye_row(first) / gain_low[0:1, :]
        rg_ref[0:1, :] = first
        rg_ref[1:2, :] = second
        squares = early + row_squares(rq_ref[PAIRS - 1]) + row_squares(first) + row_squares(second)
        mine = near_ref.at[at["flat"]]
        mine[...] = jnp.broadcast_to(squares, (8, 128))

        def near(i):
            return pltpu.make_async_remote_copy(
                src_ref=mine, dst_ref=mine, send_sem=near_send.at[i], recv_sem=near_recv.at[i],
                device_id=others[i], device_id_type=MESH,
            )

        for i in range(31):
            near(i).start()
        for i in range(31):
            near(i).wait_recv()
        group = near_ref[0]
        for i in range(1, 32):
            group = group + near_ref[i]
        norm_ref[...] = group

        for i in range(31):
            near(i).wait_send()
        for i in range(1, 16):
            last(i).wait_send()
        copy(8, 0).wait_send()
        for w in range(8):
            for k in range(7):
                copy(w, k).wait_send()


def update_kernel(
    count_ref, total_ref, rq_ref, ro_ref, ru_ref, rd_ref, rg_ref,
    wq_ref, wo_ref, wu_ref, wd_ref, wg_ref, mq_ref, mo_ref, mu_ref, md_ref, mg_ref,
    vq_ref, vo_ref, vu_ref, vd_ref, vg_ref, gin_ref, out_ref,
    norm_ref, gq_ref, nvq_ref, nwq_ref, go_ref, nvo_ref, nwo_ref, gu_ref, nvu_ref, nwu_ref,
    gd_ref, nvd_ref, nwd_ref, gg_ref, nvg_ref, nwg_ref, gin_out_ref, out_out_ref, sem,
):
    pieces = 4
    height = gin_ref.shape[0] // pieces
    moves = []
    for i in range(pieces):
        rows = pl.ds(i * height, height)
        for j, (src, dst) in enumerate(((gin_ref, gin_out_ref), (out_ref, out_out_ref))):
            moves.append(pltpu.make_async_copy(src.at[rows], dst.at[rows], sem.at[j, i]))
    for move in moves:
        move.start()
    update_weights(
        count_ref, total_ref, rq_ref, ro_ref, ru_ref, rd_ref, rg_ref,
        wq_ref, wo_ref, wu_ref, wd_ref, wg_ref, mq_ref, mo_ref, mu_ref, md_ref, mg_ref,
        vq_ref, vo_ref, vu_ref, vd_ref, vg_ref,
        norm_ref, gq_ref, nvq_ref, nwq_ref, go_ref, nvo_ref, nwo_ref, gu_ref, nvu_ref, nwu_ref,
        gd_ref, nvd_ref, nwd_ref, gg_ref, nvg_ref, nwg_ref,
    )
    for move in moves:
        move.wait()


def update_weights(
    count_ref, total_ref, rq_ref, ro_ref, ru_ref, rd_ref, rg_ref,
    wq_ref, wo_ref, wu_ref, wd_ref, wg_ref, mq_ref, mo_ref, mu_ref, md_ref, mg_ref,
    vq_ref, vo_ref, vu_ref, vd_ref, vg_ref,
    norm_ref, gq_ref, nvq_ref, nwq_ref, go_ref, nvo_ref, nwo_ref, gu_ref, nvu_ref, nwu_ref,
    gd_ref, nvd_ref, nwd_ref, gg_ref, nvg_ref, nwg_ref,
):
    norm = jnp.sqrt(total_ref[0:1, 0:1])
    norm_ref[...] = norm
    factor = jnp.minimum(1.0, clip_level / norm)
    count = jnp.full((1, 1), count_ref[0], jnp.int32).astype(f32)
    first_fix = 1.0 - jnp.exp2(count * math.log2(beta_first))
    second_fix = 1.0 - jnp.exp2(count * math.log2(beta_second))

    def update(grad, at, weight, first, second, rate, outs):
        clipped = grad * factor
        first_new = beta_first * first[at] + (1.0 - beta_first) * clipped
        second_new = beta_second * second[at] + (1.0 - beta_second) * clipped * clipped
        direction = first_new / first_fix / (jnp.sqrt(second_new / second_fix) + adam_eps)
        outs[0][at] = clipped
        outs[1][at] = second_new
        outs[2][at] = weight[at] - rate * (direction + decay_weight * weight[at])

    for part in range(3):
        for i in range(PAIRS):
            at = (slice(None), slice(part * D + i * DUO, part * D + (i + 1) * DUO))
            grad = rq_ref[i, :, part * DUO : (part + 1) * DUO]
            update(grad, at, wq_ref, mq_ref, vq_ref, rate_matrix, (gq_ref, nvq_ref, nwq_ref))
    update(ro_ref[...], ..., wo_ref, mo_ref, vo_ref, rate_matrix, (go_ref, nvo_ref, nwo_ref))
    update(ru_ref[...], ..., wu_ref, mu_ref, vu_ref, rate_matrix, (gu_ref, nvu_ref, nwu_ref))
    update(rd_ref[...], ..., wd_ref, md_ref, vd_ref, rate_matrix, (gd_ref, nvd_ref, nwd_ref))
    update(rg_ref[...], ..., wg_ref, mg_ref, vg_ref, rate_gain, (gg_ref, nvg_ref, nwg_ref))


ROWS = {"pair": 16, "out": 16, "up": 16, "down": 64}
COLS = {"pair": CHUNK, "out": D, "up": FF, "down": D}
LATE = ("out", "up", "down")
smem = pl.BlockSpec(memory_space=pltpu.SMEM)
hbm = pl.BlockSpec(memory_space=pl.ANY)
vmem = pl.BlockSpec(memory_space=pltpu.VMEM)


def shaped(shape, dtype):
    return jax.ShapeDtypeStruct(shape, dtype)


def params(collective_id=None, mib=63):
    if collective_id is None:
        return pltpu.CompilerParams(vmem_limit_bytes=mib << 20)
    return pltpu.CompilerParams(vmem_limit_bytes=mib << 20, collective_id=collective_id, has_side_effects=True)


def whole(shape):
    return pl.BlockSpec(shape, lambda *_: (0,) * len(shape), pipeline_mode=pl.Buffered(1))


def whole_out(shape):
    return pl.BlockSpec(shape, lambda *_: (0,) * len(shape))


def five(name):
    return (4, 4, 2, ROWS[name], COLS[name])


def forward_outs(tokens):
    tiles = tokens // TILE
    specs = [
        pl.BlockSpec((1, BLOCK, CHUNK), lambda p, b: (p, b, 0)),
        pl.BlockSpec((1, BLOCK, 2 * FEAT), lambda p, b: (p, b, 0)),
        pl.BlockSpec((1, BLOCK, 2 * FEAT), lambda p, b: (p, b, 0)),
        pl.BlockSpec((1, BLOCK, 2 * TILE), lambda p, b: (p, b, 0)),
        pl.BlockSpec((BLOCK, DUO), lambda p, b: (b, p)),
        pl.BlockSpec((1, BLOCK, DUO), lambda p, b: (p, b, 0)),
        pl.BlockSpec((1, TILES_BLOCK, 2, DUO, FEAT), lambda p, b: (p, b, 0, 0, 0)),
        whole_out((tokens, D)),
    ]
    shapes = [
        shaped((PAIRS, tokens, CHUNK), bf16),
        shaped((PAIRS, tokens, 2 * FEAT), bf16),
        shaped((PAIRS, tokens, 2 * FEAT), bf16),
        shaped((PAIRS, tokens, 2 * TILE), bf16),
        shaped((tokens, D), bf16),
        shaped((PAIRS, tokens, DUO), f32),
        shaped((PAIRS, tiles, 2, DUO, FEAT), bf16),
        shaped((tokens, D), bf16),
    ]
    scratch = [pltpu.VMEM((2, DUO, FEAT), f32), pltpu.VMEM((DUO, 2 * FEAT), bf16)]
    return specs, shapes, scratch


pair_omega = pl.BlockSpec((2, HD, FEAT), lambda p, b: (p, 0, 0))
pair_weight = pl.BlockSpec((D, CHUNK), lambda p, b: (0, p))


def forward_local(starts, lens, x, weight, gains, omega):
    tokens = x.shape[0]
    specs, shapes, scratch = forward_outs(tokens)
    return pl.pallas_call(
        forward_local_kernel,
        grid=(PAIRS, tokens // BLOCK),
        in_specs=[smem, smem, whole((tokens, D)), pair_weight, whole((8, D)), pair_omega],
        out_specs=specs,
        out_shape=shapes,
        scratch_shapes=scratch,
        compiler_params=params(),
    )(starts, lens, x, weight, gains, omega)


def forward(count, starts, lens, x, omega, wq, wo, wu, wd, gains, cot):
    tokens = x.shape[0]
    blocks = tokens // BLOCK
    steps = PAIRS * blocks
    specs, shapes, scratch = forward_outs(tokens)

    def early(index_map):
        return lambda i: index_map(
            jnp.minimum(i // blocks, PAIRS - 1), jnp.where(i < steps, i % blocks, blocks - 1)
        )

    specs = [pl.BlockSpec(spec.block_shape, early(spec.index_map)) for spec in specs]
    weight = pl.BlockSpec(pair_weight.block_shape, early(pair_weight.index_map))
    heads = pl.BlockSpec(pair_omega.block_shape, early(pair_omega.index_map))
    rows = pl.BlockSpec((FF_BLOCK, D), lambda i: (jnp.maximum(i - steps, 0), 0))
    return pl.pallas_call(
        forward_kernel,
        grid=(steps + tokens // FF_BLOCK,),
        in_specs=[smem, smem, smem, hbm, heads] + [whole(array.shape) for array in (wq, wo, wu, wd, gains)] + [rows],
        out_specs=specs + [weight, whole_out((8, D)), vmem, rows, rows, hbm, hbm, hbm],
        out_shape=shapes
        + [shaped((D, WIDE), bf16), shaped((8, D), f32)]
        + [pltpu.VMEM((tokens, D), bf16), shaped((tokens, D), f32), shaped((tokens, D), f32)]
        + [shaped(five(name), bf16) for name in LATE],
        scratch_shapes=scratch
        + [
            pltpu.VMEM((tokens, D), bf16),
            pltpu.VMEM((tokens, D), f32),
            pltpu.VMEM((tokens, D), bf16),
            pltpu.VMEM((4, 4, 2, 16, CHUNK + EXTRA), bf16),
            pltpu.VMEM((PAIRS - 1, *five("pair")), bf16),
        ]
        + [pltpu.VMEM(five(name), bf16) for name in LATE]
        + [pltpu.VMEM((8, EXTRA), f32)]
        + feed_forward_scratch()
        + [
            pltpu.SemaphoreType.DMA((9, 10)),
            pltpu.SemaphoreType.DMA((9, 10)),
            pltpu.SemaphoreType.DMA((3,)),
        ],
        compiler_params=params(0, FORWARD_MIB),
    )(count, starts, lens, x, omega, wq, wo, wu, wd, gains, cot)


def feed_forward_scratch():
    return [
        pltpu.VMEM((D, D), f32), pltpu.VMEM((D, FF), f32), pltpu.VMEM((FF, D), f32),
        pltpu.VMEM((FF_BLOCK, D), bf16), pltpu.VMEM((D, FF_BLOCK), bf16), pltpu.VMEM((FF_BLOCK, D), bf16),
    ]


def feed_forward_local(lens, x, o, cot, wo, wu, wd, gains):
    tokens = x.shape[0]
    rows = pl.BlockSpec((FF_BLOCK, D), lambda i: (i, 0))
    return pl.pallas_call(
        feed_forward_local_kernel,
        grid=(tokens // FF_BLOCK,),
        in_specs=[smem, rows, rows, rows, whole((D, D)), whole((D, FF)), whole((FF, D)), whole((8, D))],
        out_specs=[rows, rows, rows, whole_out((D, D)), whole_out((D, FF)), whole_out((FF, D))],
        out_shape=[
            shaped((tokens, D), bf16),
            shaped((tokens, D), f32),
            shaped((tokens, D), f32),
            shaped((D, D), bf16),
            shaped((D, FF), bf16),
            shaped((FF, D), bf16),
        ],
        scratch_shapes=feed_forward_scratch(),
        compiler_params=params(),
    )(lens, x, o, cot, wo, wu, wd, gains)


def backward_ins(blocks):
    last = blocks - 1
    return [
        smem,
        pl.BlockSpec((BLOCK, D), lambda p, b: (jnp.where(p == 0, last - b, 0), 0)),
        pl.BlockSpec((1, BLOCK, CHUNK), lambda p, b: (p, last - b, 0)),
        pl.BlockSpec((1, BLOCK, 2 * FEAT), lambda p, b: (p, last - b, 0)),
        pl.BlockSpec((1, BLOCK, 2 * FEAT), lambda p, b: (p, last - b, 0)),
        pl.BlockSpec((1, BLOCK, 2 * TILE), lambda p, b: (p, last - b, 0)),
        pl.BlockSpec((BLOCK, DUO), lambda p, b: (last - b, p)),
        pl.BlockSpec((1, BLOCK, DUO), lambda p, b: (p, last - b, 0)),
        pl.BlockSpec((BLOCK, DUO), lambda p, b: (last - b, p)),
        pl.BlockSpec((1, TILES_BLOCK, 2, DUO, FEAT), lambda p, b: (p, last - b, 0, 0, 0)),
        pair_omega,
        whole((8, D)),
    ]


def backward_scratch(tokens):
    return [
        pltpu.VMEM((2, DUO, FEAT), f32),
        pltpu.VMEM((2, DUO, FEAT), bf16),
        pltpu.VMEM((tokens, WIDE), bf16),
        pltpu.VMEM((tokens, D), bf16),
    ]


def backward_local(args, x, dmid, weight):
    tokens = x.shape[0]
    return pl.pallas_call(
        backward_local_kernel,
        grid=(PAIRS, tokens // BLOCK),
        in_specs=backward_ins(tokens // BLOCK) + [whole((tokens, D)), whole((tokens, D)), whole((D, WIDE))],
        out_specs=[whole_out((tokens, D)), pair_weight],
        out_shape=[shaped((tokens, D), f32), shaped((D, WIDE), bf16)],
        scratch_shapes=backward_scratch(tokens),
        compiler_params=params(),
    )(*args, x, dmid, weight)


def backward(args, wq, wu, gains, x, dmid, weight, grads):
    tokens = x.shape[0]
    half = [(4, 4, 16, D), (2, 4, 4, 16, FF // 2), (2, 4, 4, 32, D), (PAIRS, 4, 4, 16, CHUNK)]
    dma = pltpu.SemaphoreType.DMA
    return pl.pallas_call(
        backward_kernel,
        grid=(PAIRS, tokens // BLOCK),
        in_specs=backward_ins(tokens // BLOCK) + [whole(wq.shape), whole(wu.shape), whole(gains.shape)] + [hbm] * 6,
        out_specs=[vmem] * 7,
        out_shape=[pltpu.VMEM((tokens, D), f32)]
        + [pltpu.VMEM((ROWS[name], COLS[name]), f32) for name in LATE]
        + [pltpu.VMEM((PAIRS, 16, CHUNK), f32), pltpu.VMEM((2, 16), f32), pltpu.VMEM((8, 128), f32)],
        scratch_shapes=backward_scratch(tokens)
        + [pltpu.VMEM((PAIRS, *five("pair")), bf16)]
        + [pltpu.VMEM((tokens, D), bf16), pltpu.VMEM((D, WIDE), bf16)]
        + [pltpu.VMEM(shape, bf16) for shape in half] * 3
        + [pltpu.VMEM((15, 16, CHUNK), bf16), pltpu.VMEM((32, 8, 128), f32)]
        + [dma((9, 7)), dma((9, 7)), dma((8,)), dma((15,)), dma((15,)), dma((31,)), dma((31,))],
        compiler_params=params(1, BACKWARD_MIB),
    )(*args, wq, wu, gains, x, dmid, weight, *grads)


def update_all(count, total, grads, weights, firsts, seconds, grad_inputs, out_rows):
    shapes = [shaped((1, 1), f32)]
    for weight in weights:
        shapes += [shaped(weight.shape, f32)] * 3
    return pl.pallas_call(
        update_kernel,
        in_specs=[smem] + [vmem] * 23,
        out_specs=[vmem] * 16 + [hbm, hbm],
        out_shape=shapes + [shaped(grad_inputs.shape, f32), shaped(out_rows.shape, bf16)],
        scratch_shapes=[pltpu.SemaphoreType.DMA((2, 4))],
        compiler_params=params(mib=UPDATE_MIB),
    )(count, total, *grads, *weights, *firsts, *seconds, grad_inputs, out_rows)


def to_pairs(weight):
    split = weight.reshape(weight.shape[0], 3, PAIRS, DUO)
    return jnp.swapaxes(split, 1, 2).reshape(weight.shape)


def from_pairs(weight):
    split = weight.reshape(weight.shape[0], PAIRS, 3, DUO)
    return jnp.swapaxes(split, 1, 2).reshape(weight.shape)


def on_device(
    sizes, inputs, cotangent, feature_omega, seg_start, seg_len, step_count,
    w_qkv, w_out, w_up, w_down, gains,
    m_qkv, m_out, m_up, m_down, m_gains,
    v_qkv, v_out, v_up, v_down, v_gains,
):
    weights = (w_qkv, w_out, w_up, w_down, gains)
    firsts = (m_qkv, m_out, m_up, m_down, m_gains)
    seconds = (v_qkv, v_out, v_up, v_down, v_gains)
    if sizes == (4, 8):
        count = step_count.reshape(1)
        (qkv, fq, fk, weights_kept, attended, rden, prefix, normed, qkv_full, gain_full, out_rows, dmid, grad_attended,
         *grads) = forward(count, seg_start, seg_len, inputs, feature_omega, *weights, cotangent)
        grad_inputs, r_out, r_up, r_down, r_qkv, r_gains, total = backward(
            (seg_start, normed, qkv, fq, fk, weights_kept, attended, rden, grad_attended, prefix, feature_omega, gain_full),
            w_qkv, w_up, gains, inputs, dmid, qkv_full, grads,
        )
        norm, *updated, grad_inputs, out_rows = update_all(
            count, total, (r_qkv, r_out, r_up, r_down, r_gains), weights, firsts, seconds, grad_inputs, out_rows
        )
        return (out_rows, grad_inputs, norm.reshape(()), *updated)

    def gather(piece, axis=0):
        return lax.all_gather(piece.astype(bf16), AXES, axis=axis, tiled=True)

    qkv_full, out_full, up_full, down_full = (gather(piece) for piece in weights[:4])
    qkv_full = to_pairs(qkv_full)
    gain_full = jnp.pad(gather(gains, 1).astype(f32), ((0, 6), (0, 0)))
    qkv, fq, fk, weights_kept, attended, rden, prefix, normed = forward_local(
        seg_start, seg_len, inputs, qkv_full, gain_full, feature_omega
    )
    out_rows, dmid, grad_attended, grad_out, grad_up, grad_down = feed_forward_local(
        seg_len, inputs, attended, cotangent, out_full, up_full, down_full, gain_full
    )
    grad_inputs, grad_qkv = backward_local(
        (seg_start, normed, qkv, fq, fk, weights_kept, attended, rden, grad_attended, prefix, feature_omega, gain_full),
        inputs, dmid, qkv_full,
    )

    def scatter(piece):
        return lax.psum_scatter(piece.astype(f32), AXES, scatter_dimension=0, tiled=True)

    reduced = [scatter(piece) for piece in (from_pairs(grad_qkv), grad_out, grad_up, grad_down)]
    low = [weight.astype(bf16).astype(f32) for weight in weights]
    first = jnp.sum(reduced[0] * low[0], axis=1) / low[4][0]
    second = jnp.sum(reduced[2] * low[2], axis=1) / low[4][1]
    reduced.append(jnp.stack([first, second], axis=0))
    grad_norm = jnp.sqrt(lax.psum(sum(jnp.sum(piece * piece) for piece in reduced), AXES))
    factor = jnp.minimum(1.0, clip_level / grad_norm)
    count = step_count.astype(f32)
    first_fix = 1.0 - jnp.power(beta_first, count)
    second_fix = 1.0 - jnp.power(beta_second, count)
    updated = []
    rates = (rate_matrix,) * 4 + (rate_gain,)
    for weight, first, second, gradient, rate in zip(weights, firsts, seconds, reduced, rates):
        clipped = gradient * factor
        first_new = beta_first * first + (1.0 - beta_first) * clipped
        second_new = beta_second * second + (1.0 - beta_second) * clipped * clipped
        direction = first_new / first_fix / (jnp.sqrt(second_new / second_fix) + adam_eps)
        updated += [clipped, second_new, weight - rate * (direction + decay_weight * weight)]
    return (out_rows, grad_inputs, grad_norm, *updated)


def solution(mesh):
    return jax.shard_map(
        functools.partial(on_device, tuple(mesh.shape[name] for name in AXES)),
        mesh=mesh,
        in_specs=(
            P(("dp", "fsdp"), None),
            P(("dp", "fsdp"), None),
            P(),
            P(("dp", "fsdp")),
            P(("dp", "fsdp")),
            P(),
            P(("dp", "fsdp"), None),
            P(("dp", "fsdp"), None),
            P(("dp", "fsdp"), None),
            P(("dp", "fsdp"), None),
            P(None, ("dp", "fsdp")),
            P(("dp", "fsdp"), None),
            P(("dp", "fsdp"), None),
            P(("dp", "fsdp"), None),
            P(("dp", "fsdp"), None),
            P(None, ("dp", "fsdp")),
            P(("dp", "fsdp"), None),
            P(("dp", "fsdp"), None),
            P(("dp", "fsdp"), None),
            P(("dp", "fsdp"), None),
            P(None, ("dp", "fsdp")),
        ),
        out_specs=(
            P(("dp", "fsdp"), None),
            P(("dp", "fsdp"), None),
            P(),
            P(("dp", "fsdp"), None),
            P(("dp", "fsdp"), None),
            P(("dp", "fsdp"), None),
            P(("dp", "fsdp"), None),
            P(("dp", "fsdp"), None),
            P(("dp", "fsdp"), None),
            P(("dp", "fsdp"), None),
            P(("dp", "fsdp"), None),
            P(("dp", "fsdp"), None),
            P(("dp", "fsdp"), None),
            P(("dp", "fsdp"), None),
            P(("dp", "fsdp"), None),
            P(None, ("dp", "fsdp")),
            P(None, ("dp", "fsdp")),
            P(None, ("dp", "fsdp")),
        ),
        check_vma=False,
    )
```
